256 devices in a mesh: row: 8 (over y, core), col: 32 (over x, z).
Axes of the slice: x: 4, y: 4, z: 8, core: 2. Of those that a mesh axis runs over, the one named last changes fastest.
Arguments:
- eigvecs: float32 [1024, 100352], P('col', 'row'), may hold values from -6 to 6
- span_vectors: float32 [2, 64, 4, 128], P(None, 'row'), may hold values from -6 to 6
- span_offsets: int32 [2, 64], P(None, 'row'), may hold values from 0 to 12543, as said below
- panels: bfloat16 [2, 256, 100352], P(None, 'col', 'row'), may hold values from -0.01894036 to 0.01894036
Outputs:
- back_vectors: float32 [1024, 100352], P('col', 'row')
The draws below stay inside these ranges and needn't reach their ends.
Inputs may be any that keep to these rules, and one draw needn't show every extreme that they name: `span_offsets`: each block starts within the rows of its index of row and ends at most 128 rows after them, and inside the matrix; on every index of row but the last the last block of each sweep reaches into the next index's rows.
All inputs are finite; a program needn't handle non-finite values.
Results may differ from the reference program's by a relative error of at most 0.0075.
Values may be sent and summed in bfloat16 or wider, within the bound.
A program may use at most 128 MiB of HBM per device.

```python
import jax
import jax.numpy as jnp
from jax import lax

K = 1024
ROWS_DEV = 12544
N = 100352
BAND = 128
REFL = 4
SPANS_DEV = 8
SPANS = 64
SWEEPS = 2
WIDTH = 256
PANELS = 2
N_ROW = 8


def draw_span_offsets(key, part):
    key_base, key_last = jax.random.split(key, 2)
    offsets_all = jax.random.randint(key_base, (SWEEPS, N_ROW, SPANS_DEV), 0, ROWS_DEV - BAND + 1)
    last_span = jax.random.randint(key_last, (SWEEPS, N_ROW), ROWS_DEV - 3 * BAND // 4, ROWS_DEV - BAND // 4 + 1)
    device_ids = jnp.arange(N_ROW)[None, :]
    last_span = jnp.where(device_ids < N_ROW - 1, last_span, ROWS_DEV - BAND)
    offsets_all = offsets_all.at[:, :, SPANS_DEV - 1].set(last_span)
    return offsets_all.reshape(SWEEPS, N_ROW * SPANS_DEV).astype(jnp.int32)


def draw_panels(key, part):
    key_own = jax.random.fold_in(key, 17)
    own = jax.random.truncated_normal(key_own, -4.0, 4.0, (PANELS, WIDTH, N), jnp.float32)
    scaled = own * float(N) ** (-0.5)
    limit = 6.0 * float(N) ** (-0.5)
    return jnp.clip(scaled, -limit, limit).astype(jnp.bfloat16)


def levels(own_key, extent, cuts, least, high):
    def one(axis_at, shards_of):
        heights = jax.random.uniform(jax.random.fold_in(jax.random.fold_in(own_key, 6), axis_at), (shards_of,), jnp.float32, least / len(cuts), high / len(cuts))
        return jnp.repeat(jnp.exp(heights), extent[axis_at] // shards_of).reshape((-1,) + (1,) * (len(extent) - axis_at - 1))

    loudness = one(*cuts[0])
    for cut in cuts[1:]:
        loudness = loudness * one(*cut)
    return loudness


def centred(rng, shape, width, reach, cuts=(), held_as=jnp.bfloat16):
    factor_of = levels(rng, shape, cuts, -0.22, 0.18) if cuts else 1.0
    values = jax.random.normal(rng, shape, jnp.float32) * width * factor_of
    return jnp.minimum(jnp.maximum(values, -reach), reach).astype(held_as)


def setup_inputs(seed: int = 0) -> dict:
    streams_of = jax.random.split(jax.random.key(seed), 5)
    return {
        "eigvecs": centred(streams_of[0], (K, N), 1.0, 6.0, ((0, 32), (1, 8)), jnp.float32),
        "span_vectors": centred(streams_of[1], (SWEEPS, SPANS, REFL, BAND), 1.0, 6.0, ((1, 8),), jnp.float32),
        "span_offsets": draw_span_offsets(jax.random.fold_in(streams_of[4], 71), 0),
        "panels": draw_panels(jax.random.fold_in(streams_of[4], 71), 0),
    }


PRECISE = lax.Precision.HIGHEST
CONTRACT_LAST = (((1,), (1,)), ((), ()))
CONTRACT_FIRST = (((0,), (0,)), ((), ()))

def wy_matrix(gram_mat):
    return jnp.triu(gram_mat, 1) + 0.5 * jnp.diag(jnp.diag(gram_mat))

def apply_span(window, vectors):
    gram_mat = jnp.dot(vectors, vectors.T, precision=PRECISE)
    inner = jnp.dot(vectors, window.T, precision=PRECISE)
    coeffs = lax.linalg.triangular_solve(wy_matrix(gram_mat), inner, left_side=True, lower=False)
    return window - jnp.dot(coeffs.T, vectors, precision=PRECISE)

def reference(eigvecs, span_vectors, span_offsets, panels):
    eigen = eigvecs
    for sweep_at in range(SWEEPS):
        vectors = span_vectors[sweep_at]
        offsets = span_offsets[sweep_at]

        def advance(span_at, state, vectors=vectors, offsets=offsets):
            begin_at = (span_at // SPANS_DEV * ROWS_DEV + offsets[span_at]).astype(jnp.int32)
            window = lax.dynamic_slice_in_dim(state, begin_at, BAND, 1)
            return lax.dynamic_update_slice_in_dim(state, apply_span(window, vectors[span_at]), begin_at, 1)
        eigen = lax.fori_loop(0, SPANS, advance, eigen)
    for panel_at in range(PANELS):
        reflect = panels[panel_at]
        gram_mat = lax.dot_general(reflect.astype(jnp.float32), reflect.astype(jnp.float32), CONTRACT_LAST, preferred_element_type=jnp.float32)
        inner = lax.dot_general(reflect.astype(jnp.float32), eigen.astype(jnp.bfloat16).astype(jnp.float32), CONTRACT_LAST, preferred_element_type=jnp.float32)
        coeffs = lax.linalg.triangular_solve(wy_matrix(gram_mat), inner, left_side=True, lower=False)
        eigen = eigen - lax.dot_general(coeffs.astype(jnp.bfloat16).astype(jnp.float32), reflect.astype(jnp.float32), CONTRACT_FIRST, preferred_element_type=jnp.float32)
    return eigen
```

```python
import functools

import jax
import jax.numpy as jnp
from jax import lax
from jax.experimental import pallas as pl
from jax.experimental.pallas import tpu as pltpu
from jax.sharding import Mesh
from jax.sharding import PartitionSpec as P

LANE = 128
BLOCK = 128
NX = 4
NZ = 8
F32 = jnp.float32
BF16 = jnp.bfloat16
HI = lax.Precision.HIGHEST
NT = (((1,), (1,)), ((), ()))
NN = (((1,), (0,)), ((), ()))


def dot_hi(a, b, dims=NN):
    return lax.dot_general(a, b, dims, precision=HI, preferred_element_type=F32)


def halves(a):
    top = a.astype(BF16)
    return top, (a - top.astype(F32)).astype(BF16)


def dot3(a, b):
    a_top, a_low = halves(a)
    b_top, b_low = halves(b)
    d = functools.partial(lax.dot_general, dimension_numbers=NN, preferred_element_type=F32)
    return d(a_top, b_top) + (d(a_top, b_low) + d(a_low, b_top))


def solve_wy(gram, right, unit):
    order = gram.shape[0]
    p = lax.broadcasted_iota(jnp.int32, gram.shape, 0)
    q = lax.broadcasted_iota(jnp.int32, gram.shape, 1)
    on_diag = p == q
    same = (p // unit) == (q // unit)
    keep = (same & (p > q)) | (jnp.logical_not(same) & (p < q))
    picked = jnp.where(on_diag, gram, 0.0)
    down = 2.0 / jnp.sum(picked, axis=1, keepdims=True)
    across = 2.0 / jnp.sum(picked, axis=0, keepdims=True)
    strict = jnp.where(keep, gram * down, 0.0)
    bp = lax.broadcasted_iota(jnp.int32, (BLOCK, BLOCK), 0)
    bq = lax.broadcasted_iota(jnp.int32, (BLOCK, BLOCK), 1)
    count = order // BLOCK
    tiles = [strict[t * BLOCK : (t + 1) * BLOCK, t * BLOCK : (t + 1) * BLOCK] for t in range(count)]
    eye = (bp == bq).astype(F32)
    inverse = [eye - jnp.where(bp // 2 == bq // 2, tile, 0.0) for tile in tiles]
    size = 2
    while size < BLOCK:
        joined = (bp // (2 * size) == bq // (2 * size)) & (bp // size != bq // size)
        middle = [jnp.where(joined, tile, 0.0) for tile in tiles]
        left = [dot3(inverse[t], middle[t]) for t in range(count)]
        inverse = [inverse[t] - dot3(left[t], inverse[t]) for t in range(count)]
        size *= 2
    per = max(1, unit // BLOCK)
    sequence = [base + k for base in range(0, count, per) for k in reversed(range(per))]
    found = [None] * count
    done = []
    for t in sequence:
        value = right[:, t * BLOCK : (t + 1) * BLOCK]
        for u in done:
            value = value - dot3(found[u], strict[u * BLOCK : (u + 1) * BLOCK, t * BLOCK : (t + 1) * BLOCK])
        found[t] = dot3(value, inverse[t])
        done.append(t)
    return jnp.concatenate(found, axis=1) * across


def span_products(tiles_dev, own_tile, vectors, shift, tile_down, tile_across, own, own_shift, prev, prev_shift,
                  prev_over, eigen, gram_ref, own_ref, prev_ref, inner_ref, windows):
    def placed(values, amount):
        wide = jnp.concatenate([values, jnp.zeros_like(values)], axis=1)
        for bit in range(7):
            wide = jnp.where(((amount >> bit) & 1) == 1, pltpu.roll(wide, 1 << bit, 1), wide)
        return wide

    wide = placed(vectors[...], shift[...])
    low, high = wide[:, :LANE], wide[:, LANE:]
    down, across = tile_down[...], tile_across[...]
    level = dot_hi(wide, wide, NT)
    after = dot_hi(high, low, NT)
    before = dot_hi(low, high, NT)
    gram_ref[...] = jnp.where(
        down == across,
        level,
        jnp.where(across == down + 1, after, jnp.where(across == down - 1, before, 0.0)),
    )
    own_wide = placed(own[...], own_shift[...])
    own_ref[...] = own_wide
    prev_high = jnp.where(prev_over[...] == 1, placed(prev[...], prev_shift[...])[:, LANE:], 0.0)
    prev_ref[...] = prev_high
    rows = eigen.shape[0]
    count = own_tile.shape[0]
    for c in range(count):
        at = own_tile[c]
        inside = jnp.where(at + 1 < tiles_dev, 1.0, 0.0).astype(F32)
        then = jnp.minimum(at + 1, tiles_dev - 1)
        windows[c * rows : (c + 1) * rows, :LANE] = eigen[:, pl.ds(pl.multiple_of(at * LANE, LANE), LANE)]
        windows[c * rows : (c + 1) * rows, LANE:] = (
            eigen[:, pl.ds(pl.multiple_of(then * LANE, LANE), LANE)] * inside
        )
    table = dot_hi(windows[...], own_wide, NT)
    width = own_wide.shape[0]
    place = lax.broadcasted_iota(jnp.int32, (rows, width), 1) // (width // count)
    total = jnp.zeros((rows, width), F32)
    for c in range(count):
        total = total + jnp.where(place == c, table[c * rows : (c + 1) * rows], 0.0)
    behind = dot_hi(eigen[:, :LANE], prev_high, NT)
    inner_ref[...] = jnp.concatenate([total, behind], axis=1)


def span_coeffs(unit, gram, right, coeffs):
    coeffs[...] = solve_wy(gram[...], right[...], unit)


def span_apply(tiles_dev, own_tile, eigen, own_wide, prev_high, own_coeffs, prev_coeffs, out, rounded):
    rows, cols = eigen.shape
    count = own_tile.shape[0]
    width = own_wide.shape[0]
    out[...] = eigen[...]
    mine = own_coeffs[...]
    place = lax.broadcasted_iota(jnp.int32, (rows, width), 1) // (width // count)
    spread = jnp.concatenate([jnp.where(place == c, mine, 0.0) for c in range(count)], axis=0)
    change = dot_hi(spread, own_wide[...])
    out[:, :LANE] = out[:, :LANE] - dot_hi(prev_coeffs[...], prev_high[...])
    for c in range(count):
        at = own_tile[c]
        inside = jnp.where(at + 1 < tiles_dev, 1.0, 0.0).astype(F32)
        then = jnp.minimum(at + 1, tiles_dev - 1)
        first = pl.ds(pl.multiple_of(at * LANE, LANE), LANE)
        second = pl.ds(pl.multiple_of(then * LANE, LANE), LANE)
        out[:, first] = out[:, first] - change[c * rows : (c + 1) * rows, :LANE]
        out[:, second] = out[:, second] - change[c * rows : (c + 1) * rows, LANE:] * inside
    rounded[:, :cols] = out[...].astype(BF16)
    rounded[:, cols:] = jnp.zeros((rows, rounded.shape[1] - cols), BF16)


def panel_coeffs(unit, gram, right, coeffs):
    coeffs[...] = solve_wy(gram[...].astype(F32), right[...].astype(F32), unit).astype(BF16)


def sent_to_all(x, axis):
    peers = lax.psum(1, axis)
    return lax.all_to_all(jnp.broadcast_to(x[None], (peers, *x.shape)), axis, 0, 0, tiled=True)


def call(kernel, outs, smem, *args, scratch=(), cost=2_000_000_000):
    specs = [pl.BlockSpec(memory_space=pltpu.SMEM)] * smem
    specs += [pl.BlockSpec(memory_space=pltpu.VMEM)] * (len(args) - smem)
    return pl.pallas_call(
        kernel,
        out_shape=[jax.ShapeDtypeStruct(s, d) for s, d in outs],
        in_specs=specs,
        out_specs=[pl.BlockSpec(memory_space=pltpu.VMEM)] * len(outs),
        scratch_shapes=list(scratch),
        compiler_params=pltpu.CompilerParams(vmem_limit_bytes=40 * 1024 * 1024),
        cost_estimate=pl.CostEstimate(flops=cost, bytes_accessed=4_000_000, transcendentals=0),
    )(*args)


def local(eigvecs, span_vectors, span_offsets, panels):
    rows, cols = eigvecs.shape
    sweeps, spans_dev, refl, band = span_vectors.shape
    n_row = lax.psum(1, "row")
    row = lax.axis_index("row")
    tiles_dev = cols // LANE
    part = -(-tiles_dev // NX) * LANE
    full = part * NX
    n_panel, refl_dev, _ = panels.shape
    width = refl_dev * NX * NZ
    every = n_panel * width

    padded = jnp.pad(panels, ((0, 0), (0, 0), (0, full - cols)))
    cut = padded.reshape(n_panel, refl_dev, NX, part).transpose(2, 0, 1, 3)
    block = lax.all_to_all(cut, "cx", 0, 0, tiled=True)
    up = [(k, (k + 1) % NZ) for k in range(NZ)]
    down = [(k, (k - 1) % NZ) for k in range(NZ)]
    blocks = {0: block}
    forward = backward = block
    for step in range(1, NZ // 2 + 1):
        forward = lax.ppermute(forward, "cz", up)
        blocks[step] = forward
        if step < NZ - step:
            backward = lax.ppermute(backward, "cz", down)
            blocks[NZ - step] = backward

    per_dev = sweeps * spans_dev * refl
    flat_off = span_offsets.reshape(1, sweeps * spans_dev).astype(F32)
    note = jnp.pad(flat_off, ((0, 7), (0, band - sweeps * spans_dev)))
    pack = jnp.concatenate([span_vectors.reshape(per_dev, band), note], axis=0)
    packs = sent_to_all(pack, "row").reshape(n_row, per_dev + 8, band)
    by_row = packs[:, :per_dev]
    half = spans_dev * refl
    vectors = by_row.reshape(n_row, sweeps, half, band).transpose(1, 0, 2, 3).reshape(-1, band)
    offs = packs[:, per_dev, : sweeps * spans_dev].astype(jnp.int32)
    tile_dev = jnp.repeat(offs // LANE, refl, axis=1)
    shift_dev = jnp.repeat(offs % LANE, refl, axis=1)

    def swept(x):
        return x.reshape(n_row, sweeps, half).transpose(1, 0, 2).reshape(-1)

    tile_all = swept(tile_dev + jnp.arange(n_row, dtype=jnp.int32)[:, None] * tiles_dev)
    shift_all = swept(shift_dev)
    prev_row = jnp.maximum(row - 1, 0)
    own = span_vectors.reshape(per_dev, band)
    own_tile = span_offsets.reshape(-1) // LANE
    own_shift = jnp.repeat(span_offsets.reshape(-1) % LANE, refl)[:, None]
    prev = lax.dynamic_index_in_dim(by_row, prev_row, 0, keepdims=False)
    prev_shift = lax.dynamic_index_in_dim(shift_dev, prev_row, 0, keepdims=False)[:, None]
    prev_tile = lax.dynamic_index_in_dim(tile_dev, prev_row, 0, keepdims=False)[:, None]
    prev_over = ((prev_tile == tiles_dev - 1) & (row > 0)).astype(jnp.int32)
    total = n_row * per_dev
    gram, own_wide, prev_high, inner = call(
        functools.partial(span_products, tiles_dev),
        [((total, total), F32), ((per_dev, 2 * LANE), F32), ((per_dev, LANE), F32), ((rows, 2 * per_dev), F32)],
        1,
        own_tile, vectors, shift_all[:, None], tile_all[:, None], tile_all[None, :], own, own_shift, prev,
        prev_shift, prev_over, eigvecs,
        scratch=[pltpu.VMEM((sweeps * spans_dev * rows, 2 * LANE), F32)],
    )
    inners = sent_to_all(inner, "row").reshape(n_row, rows, 2, sweeps, half)
    sums = inners[:, :, 0] + jnp.pad(inners[1:, :, 1], ((0, 1), (0, 0), (0, 0), (0, 0)))
    right = sums.transpose(1, 2, 0, 3).reshape(rows, total)
    (coeffs,) = call(functools.partial(span_coeffs, refl), [((rows, total), F32)], 0, gram, right)
    by_sweep = coeffs.reshape(rows, sweeps, n_row, half)
    own_coeffs = lax.dynamic_index_in_dim(by_sweep, row, 2, keepdims=False).reshape(rows, per_dev)
    prev_coeffs = lax.dynamic_index_in_dim(by_sweep, prev_row, 2, keepdims=False).reshape(rows, per_dev)
    eigen, rounded = call(
        functools.partial(span_apply, tiles_dev),
        [((rows, cols), F32), ((rows, full), BF16)],
        1,
        own_tile, eigvecs, own_wide, prev_high, own_coeffs, prev_coeffs,
    )

    traded = lax.all_to_all(rounded.reshape(rows, NX, part).transpose(1, 0, 2), "cx", 0, 0, tiled=True)
    traded = traded.reshape(NX * rows, part)
    at_z = lax.axis_index("cz")
    gathered = jnp.zeros((n_panel, NX, NZ, refl_dev, part), BF16)
    for step in range(NZ):
        piece = blocks[step].transpose(1, 0, 2, 3)[:, :, None]
        gathered = lax.dynamic_update_slice(gathered, piece, (0, 0, (at_z - step) % NZ, 0, 0))
    reflect = gathered.reshape(every, part)
    gram_mat = lax.dot_general(reflect, reflect, NT, preferred_element_type=F32)
    inner_mat = lax.dot_general(traded, reflect, NT, preferred_element_type=F32)
    group = n_row * NX
    piece_rows = every // group
    sending = jnp.concatenate(
        [
            gram_mat.astype(BF16).reshape(group, piece_rows, every),
            inner_mat.astype(BF16).reshape(group, piece_rows, -1),
        ],
        axis=2,
    )
    arrived = lax.all_to_all(sending, ("row", "cx"), 0, 0, tiled=True)
    added = jnp.sum(arrived.astype(F32), axis=0).astype(BF16)
    whole = sent_to_all(added, ("row", "cx"))
    gram_sum = whole[:, :, :every].reshape(every, every)
    inner_sum = whole[:, :, every:].reshape(NX * rows, every)
    (coeffs_mat,) = call(
        functools.partial(panel_coeffs, width), [((NX * rows, every), BF16)], 0, gram_sum, inner_sum
    )
    update = lax.dot_general(coeffs_mat, reflect, NN, preferred_element_type=F32).astype(BF16)
    home = lax.all_to_all(update.reshape(NX, rows, part), "cx", 0, 0, tiled=True)
    home = home.transpose(1, 0, 2).reshape(rows, full)[:, :cols]
    return eigen - home.astype(F32)


def solution(mesh):
    finer = Mesh(mesh.devices.reshape(mesh.shape["row"], NX, NZ), ("row", "cx", "cz"))
    col = ("cx", "cz")
    placed = (P(col, "row"), P(None, "row", None, None), P(None, "row"), P(None, col, "row"))
    return jax.shard_map(local, mesh=finer, in_specs=placed, out_specs=P(col, "row"), check_vma=False)
```

```python
import functools

import jax
import jax.numpy as jnp
from jax import lax
from jax.experimental import pallas as pl
from jax.experimental.pallas import tpu as pltpu
from jax.sharding import Mesh
from jax.sharding import PartitionSpec as P

LANE = 128
BLOCK = 128
NX = 4
NZ = 8
F32 = jnp.float32
BF16 = jnp.bfloat16
HI = lax.Precision.HIGHEST
NT = (((1,), (1,)), ((), ()))
NN = (((1,), (0,)), ((), ()))


def dot_hi(a, b, dims=NN):
    return lax.dot_general(a, b, dims, precision=HI, preferred_element_type=F32)


def halves(a):
    top = a.astype(BF16)
    return top, (a - top.astype(F32)).astype(BF16)


def dot3(a, b):
    a_top, a_low = halves(a)
    b_top, b_low = halves(b)
    d = functools.partial(lax.dot_general, dimension_numbers=NN, preferred_element_type=F32)
    return d(a_top, b_top) + (d(a_top, b_low) + d(a_low, b_top))


def solve_wy(gram, right, unit):
    order = gram.shape[0]
    p = lax.broadcasted_iota(jnp.int32, gram.shape, 0)
    q = lax.broadcasted_iota(jnp.int32, gram.shape, 1)
    on_diag = p == q
    same = (p // unit) == (q // unit)
    keep = (same & (p > q)) | (jnp.logical_not(same) & (p < q))
    picked = jnp.where(on_diag, gram, 0.0)
    down = 2.0 / jnp.sum(picked, axis=1, keepdims=True)
    across = 2.0 / jnp.sum(picked, axis=0, keepdims=True)
    strict = jnp.where(keep, gram * down, 0.0)
    bp = lax.broadcasted_iota(jnp.int32, (BLOCK, BLOCK), 0)
    bq = lax.broadcasted_iota(jnp.int32, (BLOCK, BLOCK), 1)
    count = order // BLOCK
    tiles = [strict[t * BLOCK : (t + 1) * BLOCK, t * BLOCK : (t + 1) * BLOCK] for t in range(count)]
    eye = (bp == bq).astype(F32)
    inverse = [eye - jnp.where(bp // 2 == bq // 2, tile, 0.0) for tile in tiles]
    size = 2
    while size < BLOCK:
        joined = (bp // (2 * size) == bq // (2 * size)) & (bp // size != bq // size)
        middle = [jnp.where(joined, tile, 0.0) for tile in tiles]
        left = [dot3(inverse[t], middle[t]) for t in range(count)]
        inverse = [inverse[t] - dot3(left[t], inverse[t]) for t in range(count)]
        size *= 2
    per = max(1, unit // BLOCK)
    sequence = [base + k for base in range(0, count, per) for k in reversed(range(per))]
    found = [None] * count
    done = []
    for t in sequence:
        value = right[:, t * BLOCK : (t + 1) * BLOCK]
        for u in done:
            value = value - dot3(found[u], strict[u * BLOCK : (u + 1) * BLOCK, t * BLOCK : (t + 1) * BLOCK])
        found[t] = dot3(value, inverse[t])
        done.append(t)
    return jnp.concatenate(found, axis=1) * across


def span_products(tiles_dev, own_tile, vectors, shift, tile_down, tile_across, own, own_shift, prev, prev_shift,
                  prev_over, eigen, gram_ref, own_ref, prev_ref, inner_ref, windows):
    def placed(values, amount):
        wide = jnp.concatenate([values, jnp.zeros_like(values)], axis=1)
        for bit in range(7):
            wide = jnp.where(((amount >> bit) & 1) == 1, pltpu.roll(wide, 1 << bit, 1), wide)
        return wide

    wide = placed(vectors[...], shift[...])
    low, high = wide[:, :LANE], wide[:, LANE:]
    down, across = tile_down[...], tile_across[...]
    level = dot_hi(wide, wide, NT)
    after = dot_hi(high, low, NT)
    before = dot_hi(low, high, NT)
    gram_ref[...] = jnp.where(
        down == across,
        level,
        jnp.where(across == down + 1, after, jnp.where(across == down - 1, before, 0.0)),
    )
    own_wide = placed(own[...], own_shift[...])
    own_ref[...] = own_wide
    prev_high = jnp.where(prev_over[...] == 1, placed(prev[...], prev_shift[...])[:, LANE:], 0.0)
    prev_ref[...] = prev_high
    rows = eigen.shape[0]
    count = own_tile.shape[0]
    for c in range(count):
        at = own_tile[c]
        inside = jnp.where(at + 1 < tiles_dev, 1.0, 0.0).astype(F32)
        then = jnp.minimum(at + 1, tiles_dev - 1)
        windows[c * rows : (c + 1) * rows, :LANE] = eigen[:, pl.ds(pl.multiple_of(at * LANE, LANE), LANE)]
        windows[c * rows : (c + 1) * rows, LANE:] = (
            eigen[:, pl.ds(pl.multiple_of(then * LANE, LANE), LANE)] * inside
        )
    table = dot_hi(windows[...], own_wide, NT)
    width = own_wide.shape[0]
    place = lax.broadcasted_iota(jnp.int32, (rows, width), 1) // (width // count)
    total = jnp.zeros((rows, width), F32)
    for c in range(count):
        total = total + jnp.where(place == c, table[c * rows : (c + 1) * rows], 0.0)
    behind = dot_hi(eigen[:, :LANE], prev_high, NT)
    inner_ref[...] = jnp.concatenate([total, behind], axis=1)


def span_coeffs(unit, gram, right, coeffs):
    coeffs[...] = solve_wy(gram[...], right[...], unit)


def span_apply(tiles_dev, own_tile, eigen, own_wide, prev_high, own_coeffs, prev_coeffs, out, rounded):
    rows, cols = eigen.shape
    count = own_tile.shape[0]
    width = own_wide.shape[0]
    out[...] = eigen[...]
    mine = own_coeffs[...]
    place = lax.broadcasted_iota(jnp.int32, (rows, width), 1) // (width // count)
    spread = jnp.concatenate([jnp.where(place == c, mine, 0.0) for c in range(count)], axis=0)
    change = dot_hi(spread, own_wide[...])
    out[:, :LANE] = out[:, :LANE] - dot_hi(prev_coeffs[...], prev_high[...])
    for c in range(count):
        at = own_tile[c]
        inside = jnp.where(at + 1 < tiles_dev, 1.0, 0.0).astype(F32)
        then = jnp.minimum(at + 1, tiles_dev - 1)
        first = pl.ds(pl.multiple_of(at * LANE, LANE), LANE)
        second = pl.ds(pl.multiple_of(then * LANE, LANE), LANE)
        out[:, first] = out[:, first] - change[c * rows : (c + 1) * rows, :LANE]
        out[:, second] = out[:, second] - change[c * rows : (c + 1) * rows, LANE:] * inside
    rounded[:, :cols] = out[...].astype(BF16)
    rounded[:, cols:] = jnp.zeros((rows, rounded.shape[1] - cols), BF16)


GRAM_TILES = ((0, 0), (0, 2), (0, 3), (1, 0), (1, 1), (1, 2), (1, 3), (2, 2), (3, 2), (3, 3))


def tile_inverses(tiles):
    bp = lax.broadcasted_iota(jnp.int32, (BLOCK, BLOCK), 0)
    bq = lax.broadcasted_iota(jnp.int32, (BLOCK, BLOCK), 1)
    eye = (bp == bq).astype(F32)
    inverse = [eye - jnp.where(bp // 2 == bq // 2, tile, 0.0) for tile in tiles]
    size = 2
    while size < BLOCK:
        joined = (bp // (2 * size) == bq // (2 * size)) & (bp // size != bq // size)
        left = [dot3(inv, jnp.where(joined, tile, 0.0)) for inv, tile in zip(inverse, tiles)]
        inverse = [inv - dot3(lhs, inv) for inv, lhs in zip(inverse, left)]
        size *= 2
    return inverse


def panel_kernel(traded, reflect, home, acc_top, acc_low, work, slots, whole, change, send_rs, recv_rs, send_ag,
                 recv_ag, send_x, recv_x, own_x):
    row, cx = lax.axis_index("row"), lax.axis_index("cx")
    n_row = lax.axis_size("row")
    peers = n_row * NX
    me = row * NX + cx
    owners = work.shape[0]
    rows = traded.shape[0]
    part = reflect.shape[1]

    def device(place):
        return {"row": place // NX, "cx": place % NX}

    barrier = pltpu.get_barrier_semaphore()
    for k in range(1, peers):
        pl.semaphore_signal(
            barrier, inc=1, device_id=device((me + k) % peers), device_id_type=pl.DeviceIdType.MESH
        )

    acc_top[...] = jnp.zeros_like(acc_top)
    acc_low[...] = jnp.zeros_like(acc_low)
    chunk = 5 * LANE

    def product(step, carry):
        at = pl.ds(pl.multiple_of(step * chunk, LANE), chunk)
        low = reflect[2 * BLOCK :, at]
        both = reflect[:, at]
        top = jnp.concatenate([traded[:, at], reflect[: 2 * BLOCK, at]], axis=0)
        acc_top[...] += lax.dot_general(top, both, NT, preferred_element_type=F32)
        acc_low[...] += lax.dot_general(low, low, NT, preferred_element_type=F32)
        return carry

    lax.fori_loop(0, part // chunk, product, 0)
    half = BLOCK // 2

    def put(place, value):
        rounded = value.astype(BF16)
        work[2 * place] = rounded[:half]
        work[2 * place + 1] = rounded[half:]

    for place, (u, t) in enumerate(GRAM_TILES):
        if u < 2:
            put(place, acc_top[(1 + u) * BLOCK : (2 + u) * BLOCK, t * BLOCK : (t + 1) * BLOCK])
        else:
            put(place, acc_low[(u - 2) * BLOCK : (u - 1) * BLOCK, (t - 2) * BLOCK : (t - 1) * BLOCK])
    for t in range(4):
        put(len(GRAM_TILES) + t, acc_top[:rows, t * BLOCK : (t + 1) * BLOCK])

    pl.semaphore_wait(barrier, peers - 1)

    def scatter(k):
        target = (me + k) % peers
        return target, pltpu.make_async_remote_copy(
            src_ref=work.at[lax.rem(target, owners)],
            dst_ref=slots.at[k - 1],
            send_sem=send_rs.at[k - 1],
            recv_sem=recv_rs.at[k - 1],
            device_id=device(target),
            device_id_type=pl.DeviceIdType.MESH,
        )

    def gather(k):
        return pltpu.make_async_remote_copy(
            src_ref=whole.at[lax.rem(me, owners)],
            dst_ref=whole.at[lax.rem(me, owners)],
            send_sem=send_ag.at[k - 1],
            recv_sem=recv_ag.at[k - 1],
            device_id=device((me + k) % peers),
            device_id_type=pl.DeviceIdType.MESH,
        )

    def arrival(k):
        source = lax.rem((me + peers - k) % peers, owners)
        return pltpu.make_async_remote_copy(
            src_ref=whole.at[source],
            dst_ref=whole.at[source],
            send_sem=send_ag.at[k - 1],
            recv_sem=recv_ag.at[k - 1],
            device_id=device((me + k) % peers),
            device_id_type=pl.DeviceIdType.MESH,
        )

    for k in range(1, peers):
        target, copy = scatter(k)
        pl.when(target < owners)(copy.start)

    @pl.when(me < owners)
    def _():
        total = work[lax.rem(me, owners)].astype(F32)
        for k in range(1, peers):
            scatter(k)[1].wait_recv()
            total = total + slots[k - 1].astype(F32)
        whole[lax.rem(me, owners)] = total.astype(BF16)
        for k in range(1, peers):
            gather(k).start()

    for k in range(1, peers):
        source = (me + peers - k) % peers
        pl.when(source < owners)(arrival(k).wait_recv)

    for k in range(1, peers):
        target, copy = scatter(k)
        pl.when(target < owners)(copy.wait_send)

    @pl.when(me < owners)
    def _():
        for k in range(1, peers):
            gather(k).wait_send()

    def got(place):
        return jnp.concatenate([whole[2 * place].astype(F32), whole[2 * place + 1].astype(F32)], axis=0)

    gram = {key: got(place) for place, key in enumerate(GRAM_TILES)}
    bp = lax.broadcasted_iota(jnp.int32, (BLOCK, BLOCK), 0)
    bq = lax.broadcasted_iota(jnp.int32, (BLOCK, BLOCK), 1)
    picked = [jnp.where(bp == bq, gram[t, t], 0.0) for t in range(4)]
    down = [2.0 / jnp.sum(p, axis=1, keepdims=True) for p in picked]
    across = [2.0 / jnp.sum(p, axis=0, keepdims=True) for p in picked]
    strict = {(u, t): gram[u, t] * down[u] for u, t in GRAM_TILES}
    for t in range(4):
        strict[t, t] = jnp.where(bp > bq, strict[t, t], 0.0)
    inverse = tile_inverses([strict[t, t] for t in range(4)])
    found = {}
    for t in (1, 0, 3, 2):
        value = got(len(GRAM_TILES) + t)
        for u in tuple(found):
            value = value - dot3(found[u], strict[u, t])
        found[t] = dot3(value, inverse[t])
    coeffs = jnp.concatenate([(found[t] * across[t]).astype(BF16) for t in range(4)], axis=1)

    def update(step, carry):
        at = pl.ds(pl.multiple_of(step * chunk, LANE), chunk)
        value = jnp.dot(coeffs, reflect[:, at], preferred_element_type=F32).astype(BF16)
        for k in range(NX):
            change[k, :, at] = value[k * (rows // NX) : (k + 1) * (rows // NX)]
        return carry

    lax.fori_loop(0, part // chunk, update, 0)

    def back(k):
        target = (cx + k) % NX
        return pltpu.make_async_remote_copy(
            src_ref=change.at[target],
            dst_ref=home.at[cx],
            send_sem=send_x.at[k - 1],
            recv_sem=recv_x.at[k - 1],
            device_id={"cx": target},
            device_id_type=pl.DeviceIdType.MESH,
        )

    def back_arrival(k):
        source = (cx + NX - k) % NX
        return pltpu.make_async_remote_copy(
            src_ref=change.at[source],
            dst_ref=home.at[source],
            send_sem=send_x.at[k - 1],
            recv_sem=recv_x.at[k - 1],
            device_id={"cx": source},
            device_id_type=pl.DeviceIdType.MESH,
        )

    for k in range(1, NX):
        back(k).start()
    keep = pltpu.make_async_copy(change.at[cx], home.at[cx], own_x)
    keep.start()
    keep.wait()
    for k in range(1, NX):
        back(k).wait_send()
        back_arrival(k).wait_recv()


def panel_step(traded, reflect, n_row):
    rows, part = traded.shape
    peers = n_row * NX
    owners = 2 * (len(GRAM_TILES) + 4)
    half = BLOCK // 2
    dma = pltpu.SemaphoreType.DMA
    return pl.pallas_call(
        panel_kernel,
        out_shape=jax.ShapeDtypeStruct((NX, rows // NX, part), BF16),
        in_specs=[pl.BlockSpec(memory_space=pltpu.VMEM)] * 2,
        out_specs=pl.BlockSpec(memory_space=pltpu.VMEM),
        scratch_shapes=[
            pltpu.VMEM((rows + 2 * BLOCK, 4 * BLOCK), F32),
            pltpu.VMEM((2 * BLOCK, 2 * BLOCK), F32),
            pltpu.VMEM((owners, half, BLOCK), BF16),
            pltpu.VMEM((peers - 1, half, BLOCK), BF16),
            pltpu.VMEM((owners, half, BLOCK), BF16),
            pltpu.VMEM((NX, rows // NX, part), BF16),
            dma((peers - 1,)),
            dma((peers - 1,)),
            dma((peers - 1,)),
            dma((peers - 1,)),
            dma((NX - 1,)),
            dma((NX - 1,)),
            dma(()),
        ],
        compiler_params=pltpu.CompilerParams(
            collective_id=0, has_side_effects=True, vmem_limit_bytes=40 * 1024 * 1024
        ),
        cost_estimate=pl.CostEstimate(flops=20_000_000_000, bytes_accessed=4_000_000, transcendentals=0),
    )(traded, reflect)


def sent_to_all(x, axis):
    peers = lax.psum(1, axis)
    return lax.all_to_all(jnp.broadcast_to(x[None], (peers, *x.shape)), axis, 0, 0, tiled=True)


def call(kernel, outs, smem, *args, scratch=(), cost=2_000_000_000):
    specs = [pl.BlockSpec(memory_space=pltpu.SMEM)] * smem
    specs += [pl.BlockSpec(memory_space=pltpu.VMEM)] * (len(args) - smem)
    return pl.pallas_call(
        kernel,
        out_shape=[jax.ShapeDtypeStruct(s, d) for s, d in outs],
        in_specs=specs,
        out_specs=[pl.BlockSpec(memory_space=pltpu.VMEM)] * len(outs),
        scratch_shapes=list(scratch),
        compiler_params=pltpu.CompilerParams(vmem_limit_bytes=40 * 1024 * 1024),
        cost_estimate=pl.CostEstimate(flops=cost, bytes_accessed=4_000_000, transcendentals=0),
    )(*args)


def local(eigvecs, span_vectors, span_offsets, panels):
    rows, cols = eigvecs.shape
    sweeps, spans_dev, refl, band = span_vectors.shape
    n_row = lax.psum(1, "row")
    row = lax.axis_index("row")
    tiles_dev = cols // LANE
    part = -(-tiles_dev // NX) * LANE
    full = part * NX
    n_panel, refl_dev, _ = panels.shape
    width = refl_dev * NX * NZ
    every = n_panel * width

    padded = jnp.pad(panels, ((0, 0), (0, 0), (0, full - cols)))
    cut = padded.reshape(n_panel, refl_dev, NX, part).transpose(2, 0, 1, 3)
    block = lax.all_to_all(cut, "cx", 0, 0, tiled=True)
    up = [(k, (k + 1) % NZ) for k in range(NZ)]
    down = [(k, (k - 1) % NZ) for k in range(NZ)]
    blocks = {0: block}
    forward = backward = block
    for step in range(1, NZ // 2 + 1):
        forward = lax.ppermute(forward, "cz", up)
        blocks[step] = forward
        if step < NZ - step:
            backward = lax.ppermute(backward, "cz", down)
            blocks[NZ - step] = backward

    per_dev = sweeps * spans_dev * refl
    flat_off = span_offsets.reshape(1, sweeps * spans_dev).astype(F32)
    note = jnp.pad(flat_off, ((0, 7), (0, band - sweeps * spans_dev)))
    pack = jnp.concatenate([span_vectors.reshape(per_dev, band), note], axis=0)
    packs = sent_to_all(pack, "row").reshape(n_row, per_dev + 8, band)
    by_row = packs[:, :per_dev]
    half = spans_dev * refl
    vectors = by_row.reshape(n_row, sweeps, half, band).transpose(1, 0, 2, 3).reshape(-1, band)
    offs = packs[:, per_dev, : sweeps * spans_dev].astype(jnp.int32)
    tile_dev = jnp.repeat(offs // LANE, refl, axis=1)
    shift_dev = jnp.repeat(offs % LANE, refl, axis=1)

    def swept(x):
        return x.reshape(n_row, sweeps, half).transpose(1, 0, 2).reshape(-1)

    tile_all = swept(tile_dev + jnp.arange(n_row, dtype=jnp.int32)[:, None] * tiles_dev)
    shift_all = swept(shift_dev)
    prev_row = jnp.maximum(row - 1, 0)
    own = span_vectors.reshape(per_dev, band)
    own_tile = span_offsets.reshape(-1) // LANE
    own_shift = jnp.repeat(span_offsets.reshape(-1) % LANE, refl)[:, None]
    prev = lax.dynamic_index_in_dim(by_row, prev_row, 0, keepdims=False)
    prev_shift = lax.dynamic_index_in_dim(shift_dev, prev_row, 0, keepdims=False)[:, None]
    prev_tile = lax.dynamic_index_in_dim(tile_dev, prev_row, 0, keepdims=False)[:, None]
    prev_over = ((prev_tile == tiles_dev - 1) & (row > 0)).astype(jnp.int32)
    total = n_row * per_dev
    gram, own_wide, prev_high, inner = call(
        functools.partial(span_products, tiles_dev),
        [((total, total), F32), ((per_dev, 2 * LANE), F32), ((per_dev, LANE), F32), ((rows, 2 * per_dev), F32)],
        1,
        own_tile, vectors, shift_all[:, None], tile_all[:, None], tile_all[None, :], own, own_shift, prev,
        prev_shift, prev_over, eigvecs,
        scratch=[pltpu.VMEM((sweeps * spans_dev * rows, 2 * LANE), F32)],
    )
    inners = sent_to_all(inner, "row").reshape(n_row, rows, 2, sweeps, half)
    sums = inners[:, :, 0] + jnp.pad(inners[1:, :, 1], ((0, 1), (0, 0), (0, 0), (0, 0)))
    right = sums.transpose(1, 2, 0, 3).reshape(rows, total)
    (coeffs,) = call(functools.partial(span_coeffs, refl), [((rows, total), F32)], 0, gram, right)
    by_sweep = coeffs.reshape(rows, sweeps, n_row, half)
    own_coeffs = lax.dynamic_index_in_dim(by_sweep, row, 2, keepdims=False).reshape(rows, per_dev)
    prev_coeffs = lax.dynamic_index_in_dim(by_sweep, prev_row, 2, keepdims=False).reshape(rows, per_dev)
    eigen, rounded = call(
        functools.partial(span_apply, tiles_dev),
        [((rows, cols), F32), ((rows, full), BF16)],
        1,
        own_tile, eigvecs, own_wide, prev_high, own_coeffs, prev_coeffs,
    )

    traded = lax.all_to_all(rounded.reshape(rows, NX, part).transpose(1, 0, 2), "cx", 0, 0, tiled=True)
    traded = traded.reshape(NX * rows, part)
    at_z = lax.axis_index("cz")
    gathered = jnp.zeros((n_panel, NX, NZ, refl_dev, part), BF16)
    for step in range(NZ):
        piece = blocks[step].transpose(1, 0, 2, 3)[:, :, None]
        gathered = lax.dynamic_update_slice(gathered, piece, (0, 0, (at_z - step) % NZ, 0, 0))
    reflect = gathered.reshape(every, part)
    home = panel_step(traded, reflect, n_row)
    home = home.transpose(1, 0, 2).reshape(rows, full)[:, :cols]
    return eigen - home.astype(F32)


def solution(mesh):
    finer = Mesh(mesh.devices.reshape(mesh.shape["row"], NX, NZ), ("row", "cx", "cz"))
    col = ("cx", "cz")
    placed = (P(col, "row"), P(None, "row", None, None), P(None, "row"), P(None, col, "row"))
    return jax.shard_map(local, mesh=finer, in_specs=placed, out_specs=P(col, "row"), check_vma=False)
```

```python
import functools

import jax
import jax.numpy as jnp
from jax import lax
from jax.experimental import pallas as pl
from jax.experimental.pallas import tpu as pltpu
from jax.sharding import Mesh
from jax.sharding import PartitionSpec as P

LANE = 128
BLOCK = 128
NX = 4
NZ = 8
F32 = jnp.float32
BF16 = jnp.bfloat16
NT = (((1,), (1,)), ((), ()))
NN = (((1,), (0,)), ((), ()))


def halves(a):
    top = a.astype(BF16)
    return top, (a - top.astype(F32)).astype(BF16)


def dot3(a, b):
    a_top, a_low = halves(a)
    b_top, b_low = halves(b)
    d = functools.partial(lax.dot_general, dimension_numbers=NN, preferred_element_type=F32)
    return d(a_top, b_top) + (d(a_top, b_low) + d(a_low, b_top))


GRAM_TILES = ((0, 0), (0, 2), (0, 3), (1, 0), (1, 1), (1, 2), (1, 3), (2, 2), (3, 2), (3, 3))


def tile_inverses(tiles):
    bp = lax.broadcasted_iota(jnp.int32, (BLOCK, BLOCK), 0)
    bq = lax.broadcasted_iota(jnp.int32, (BLOCK, BLOCK), 1)
    eye = (bp == bq).astype(F32)
    inverse = [eye - jnp.where(bp // 2 == bq // 2, tile, 0.0) for tile in tiles]
    size = 2
    while size < BLOCK:
        joined = (bp // (2 * size) == bq // (2 * size)) & (bp // size != bq // size)
        left = [dot3(inv, jnp.where(joined, tile, 0.0)) for inv, tile in zip(inverse, tiles)]
        inverse = [inv - dot3(lhs, inv) for inv, lhs in zip(inverse, left)]
        size *= 2
    return inverse


def panel_kernel(traded, reflect, home, acc_top, acc_low, work, slots, whole, change, send_rs, recv_rs, send_ag,
                 recv_ag, send_x, recv_x, own_x):
    row, cx = lax.axis_index("row"), lax.axis_index("cx")
    n_row = lax.axis_size("row")
    peers = n_row * NX
    me = row * NX + cx
    owners = work.shape[0]
    rows = traded.shape[0]
    part = reflect.shape[1]

    def device(place):
        return {"row": place // NX, "cx": place % NX}

    barrier = pltpu.get_barrier_semaphore()
    for k in range(1, peers):
        pl.semaphore_signal(
            barrier, inc=1, device_id=device((me + k) % peers), device_id_type=pl.DeviceIdType.MESH
        )

    acc_top[...] = jnp.zeros_like(acc_top)
    acc_low[...] = jnp.zeros_like(acc_low)
    chunk = 5 * LANE

    def product(step, carry):
        at = pl.ds(pl.multiple_of(step * chunk, LANE), chunk)
        low = reflect[2 * BLOCK :, at]
        both = reflect[:, at]
        top = jnp.concatenate([traded[:, at], reflect[: 2 * BLOCK, at]], axis=0)
        acc_top[...] += lax.dot_general(top, both, NT, preferred_element_type=F32)
        acc_low[...] += lax.dot_general(low, low, NT, preferred_element_type=F32)
        return carry

    lax.fori_loop(0, part // chunk, product, 0)
    half = BLOCK // 2

    def put(place, value):
        rounded = value.astype(BF16)
        work[2 * place] = rounded[:half]
        work[2 * place + 1] = rounded[half:]

    for place, (u, t) in enumerate(GRAM_TILES):
        if u < 2:
            put(place, acc_top[(1 + u) * BLOCK : (2 + u) * BLOCK, t * BLOCK : (t + 1) * BLOCK])
        else:
            put(place, acc_low[(u - 2) * BLOCK : (u - 1) * BLOCK, (t - 2) * BLOCK : (t - 1) * BLOCK])
    for t in range(4):
        put(len(GRAM_TILES) + t, acc_top[:rows, t * BLOCK : (t + 1) * BLOCK])

    pl.semaphore_wait(barrier, peers - 1)

    def scatter(k):
        target = (me + k) % peers
        return target, pltpu.make_async_remote_copy(
            src_ref=work.at[lax.rem(target, owners)],
            dst_ref=slots.at[k - 1],
            send_sem=send_rs.at[k - 1],
            recv_sem=recv_rs.at[k - 1],
            device_id=device(target),
            device_id_type=pl.DeviceIdType.MESH,
        )

    def gather(k):
        return pltpu.make_async_remote_copy(
            src_ref=whole.at[lax.rem(me, owners)],
            dst_ref=whole.at[lax.rem(me, owners)],
            send_sem=send_ag.at[k - 1],
            recv_sem=recv_ag.at[k - 1],
            device_id=device((me + k) % peers),
            device_id_type=pl.DeviceIdType.MESH,
        )

    def arrival(k):
        source = lax.rem((me + peers - k) % peers, owners)
        return pltpu.make_async_remote_copy(
            src_ref=whole.at[source],
            dst_ref=whole.at[source],
            send_sem=send_ag.at[k - 1],
            recv_sem=recv_ag.at[k - 1],
            device_id=device((me + k) % peers),
            device_id_type=pl.DeviceIdType.MESH,
        )

    for k in range(1, peers):
        target, copy = scatter(k)
        pl.when(target < owners)(copy.start)

    @pl.when(me < owners)
    def _():
        total = work[lax.rem(me, owners)].astype(F32)
        for k in range(1, peers):
            scatter(k)[1].wait_recv()
            total = total + slots[k - 1].astype(F32)
        whole[lax.rem(me, owners)] = total.astype(BF16)
        for k in range(1, peers):
            gather(k).start()

    for k in range(1, peers):
        source = (me + peers - k) % peers
        pl.when(source < owners)(arrival(k).wait_recv)

    for k in range(1, peers):
        target, copy = scatter(k)
        pl.when(target < owners)(copy.wait_send)

    @pl.when(me < owners)
    def _():
        for k in range(1, peers):
            gather(k).wait_send()

    def got(place):
        return jnp.concatenate([whole[2 * place].astype(F32), whole[2 * place + 1].astype(F32)], axis=0)

    gram = {key: got(place) for place, key in enumerate(GRAM_TILES)}
    bp = lax.broadcasted_iota(jnp.int32, (BLOCK, BLOCK), 0)
    bq = lax.broadcasted_iota(jnp.int32, (BLOCK, BLOCK), 1)
    picked = [jnp.where(bp == bq, gram[t, t], 0.0) for t in range(4)]
    down = [2.0 / jnp.sum(p, axis=1, keepdims=True) for p in picked]
    across = [2.0 / jnp.sum(p, axis=0, keepdims=True) for p in picked]
    strict = {(u, t): gram[u, t] * down[u] for u, t in GRAM_TILES}
    for t in range(4):
        strict[t, t] = jnp.where(bp > bq, strict[t, t], 0.0)
    inverse = tile_inverses([strict[t, t] for t in range(4)])
    found = {}
    for t in (1, 0, 3, 2):
        value = got(len(GRAM_TILES) + t)
        for u in tuple(found):
            value = value - dot3(found[u], strict[u, t])
        found[t] = dot3(value, inverse[t])
    coeffs = jnp.concatenate([(found[t] * across[t]).astype(BF16) for t in range(4)], axis=1)

    def update(step, carry):
        at = pl.ds(pl.multiple_of(step * chunk, LANE), chunk)
        value = jnp.dot(coeffs, reflect[:, at], preferred_element_type=F32).astype(BF16)
        for k in range(NX):
            change[k, :, at] = value[k * (rows // NX) : (k + 1) * (rows // NX)]
        return carry

    lax.fori_loop(0, part // chunk, update, 0)

    def back(k):
        target = (cx + k) % NX
        return pltpu.make_async_remote_copy(
            src_ref=change.at[target],
            dst_ref=home.at[cx],
            send_sem=send_x.at[k - 1],
            recv_sem=recv_x.at[k - 1],
            device_id={"cx": target},
            device_id_type=pl.DeviceIdType.MESH,
        )

    def back_arrival(k):
        source = (cx + NX - k) % NX
        return pltpu.make_async_remote_copy(
            src_ref=change.at[source],
            dst_ref=home.at[source],
            send_sem=send_x.at[k - 1],
            recv_sem=recv_x.at[k - 1],
            device_id={"cx": source},
            device_id_type=pl.DeviceIdType.MESH,
        )

    for k in range(1, NX):
        back(k).start()
    keep = pltpu.make_async_copy(change.at[cx], home.at[cx], own_x)
    keep.start()
    keep.wait()
    for k in range(1, NX):
        back(k).wait_send()
        back_arrival(k).wait_recv()


def panel_step(traded, reflect, n_row):
    rows, part = traded.shape
    peers = n_row * NX
    owners = 2 * (len(GRAM_TILES) + 4)
    half = BLOCK // 2
    dma = pltpu.SemaphoreType.DMA
    return pl.pallas_call(
        panel_kernel,
        out_shape=jax.ShapeDtypeStruct((NX, rows // NX, part), BF16),
        in_specs=[pl.BlockSpec(memory_space=pltpu.VMEM)] * 2,
        out_specs=pl.BlockSpec(memory_space=pltpu.VMEM),
        scratch_shapes=[
            pltpu.VMEM((rows + 2 * BLOCK, 4 * BLOCK), F32),
            pltpu.VMEM((2 * BLOCK, 2 * BLOCK), F32),
            pltpu.VMEM((owners, half, BLOCK), BF16),
            pltpu.VMEM((peers - 1, half, BLOCK), BF16),
            pltpu.VMEM((owners, half, BLOCK), BF16),
            pltpu.VMEM((NX, rows // NX, part), BF16),
            dma((peers - 1,)),
            dma((peers - 1,)),
            dma((peers - 1,)),
            dma((peers - 1,)),
            dma((NX - 1,)),
            dma((NX - 1,)),
            dma(()),
        ],
        compiler_params=pltpu.CompilerParams(
            collective_id=0, has_side_effects=True, vmem_limit_bytes=40 * 1024 * 1024
        ),
        cost_estimate=pl.CostEstimate(flops=20_000_000_000, bytes_accessed=4_000_000, transcendentals=0),
    )(traded, reflect)


def spread_dot(coeffs_top, coeffs_both, top, low):
    rows = coeffs_top.shape[0]
    d = functools.partial(lax.dot_general, dimension_numbers=NN, preferred_element_type=F32)
    first = d(coeffs_both, top)
    return first[:rows] + first[rows:] + d(coeffs_top, low)


def dot3_nt(a, b):
    a_top, a_low = halves(a)
    b_top, b_low = halves(b)
    d = functools.partial(lax.dot_general, dimension_numbers=NT, preferred_element_type=F32)
    return d(a_top, b_top) + (d(a_top, b_low) + d(a_low, b_top))


def span_kernel(offs, vectors, windows, eigen, cut, gathered, traded, kept, packs, inners, wide, tile_of, outgoing,
                send_a, recv_a, send_p, recv_p, send_w, recv_w, send_f, recv_f, send_b, recv_b, send_x, recv_x, own_sem):
    row, cx, cz = lax.axis_index("row"), lax.axis_index("cx"), lax.axis_index("cz")
    n_row = lax.axis_size("row")
    rows, cols = eigen.shape
    tiles_dev = cols // LANE
    part = cut.shape[3]
    per_dev = vectors.shape[0]
    half = per_dev // 2
    refl = 4
    spans = half // refl
    per_tile = BLOCK // half
    mesh = pl.DeviceIdType.MESH

    barrier = pltpu.get_barrier_semaphore()
    for k in range(1, n_row):
        pl.semaphore_signal(barrier, inc=1, device_id={"row": (row + k) % n_row}, device_id_type=mesh)
    for k in range(1, NX):
        pl.semaphore_signal(barrier, inc=1, device_id={"cx": (cx + k) % NX}, device_id_type=mesh)
    for k in (1, NZ - 1):
        pl.semaphore_signal(barrier, inc=1, device_id={"cz": (cz + k) % NZ}, device_id_type=mesh)

    lane8 = lax.broadcasted_iota(jnp.int32, (8, LANE), 1)
    line8 = lax.broadcasted_iota(jnp.int32, (8, LANE), 0)
    meta = jnp.zeros((8, LANE), F32)
    for s in range(2):
        for b in range(spans):
            at = offs[s * spans + b]
            place = (row % per_tile) * half + b * refl
            mine = (lane8 >= place) & (lane8 < place + refl)
            line = s * 2 + row // per_tile
            meta = jnp.where(mine & (line8 == line), ((at >> 7) + row * tiles_dev).astype(F32), meta)
            meta = jnp.where(mine & (line8 == line + 4), (at & 127).astype(F32), meta)
    packs[row, :per_dev] = vectors[...]
    packs[row, per_dev:] = meta

    pl.semaphore_wait(barrier, n_row - 1 + NX - 1 + 2)

    def over_x(k):
        return pltpu.make_async_remote_copy(
            src_ref=cut.at[(cx + k) % NX],
            dst_ref=gathered.at[:, cx, cz],
            send_sem=send_a.at[k - 1],
            recv_sem=recv_a.at[k - 1],
            device_id={"cx": (cx + k) % NX},
            device_id_type=mesh,
        )

    def over_x_arrival(k):
        source = (cx + NX - k) % NX
        return pltpu.make_async_remote_copy(
            src_ref=cut.at[source],
            dst_ref=gathered.at[:, source, cz],
            send_sem=send_a.at[k - 1],
            recv_sem=recv_a.at[k - 1],
            device_id={"cx": source},
            device_id_type=mesh,
        )

    def over_row(ref, sends, recvs, k):
        return pltpu.make_async_remote_copy(
            src_ref=ref.at[row],
            dst_ref=ref.at[row],
            send_sem=sends.at[k - 1],
            recv_sem=recvs.at[k - 1],
            device_id={"row": (row + k) % n_row},
            device_id_type=mesh,
        )

    def over_row_arrival(ref, sends, recvs, k):
        source = (row + n_row - k) % n_row
        return pltpu.make_async_remote_copy(
            src_ref=ref.at[source],
            dst_ref=ref.at[source],
            send_sem=sends.at[k - 1],
            recv_sem=recvs.at[k - 1],
            device_id={"row": source},
            device_id_type=mesh,
        )

    pieces = (0, 1, 3, 2)

    def ring(ahead, d, q, arriving):
        step = 1 if ahead else NZ - 1
        held = (cz + (NZ - d * step)) % NZ if ahead else (cz + d) % NZ
        if arriving:
            held = (held + (NZ - step)) % NZ
        source = (cx + NX - pieces[q]) % NX
        place = gathered.at[:, source, held]
        first = d == 0 and q == 0 and not arriving
        return pltpu.make_async_remote_copy(
            src_ref=cut.at[cx] if first else place,
            dst_ref=place,
            send_sem=(send_f if ahead else send_b).at[d * NX + q],
            recv_sem=(recv_f if ahead else recv_b).at[d * NX + q],
            device_id={"cz": (cz + step) % NZ},
            device_id_type=mesh,
        )

    last = NZ // 2 - 1

    def goes(ahead, d, q):
        return d < last or (q < NX // 2) == ahead

    def launch(d, q):
        for ahead in (True, False):
            if goes(ahead, d, q):
                ring(ahead, d, q, False).start()

    def pump(d, q):
        for ahead in (True, False):
            if goes(ahead, d, q):
                ring(ahead, d, q, True).wait_recv()
                if d < last and goes(ahead, d + 1, q):
                    ring(ahead, d + 1, q, False).start()

    launch(0, 0)
    for k in range(1, n_row):
        over_row(packs, send_p, recv_p, k).start()
    for k in (1, 3, 2):
        over_x(k).start()
    own_copy = pltpu.make_async_copy(cut.at[cx], gathered.at[:, cx, cz], own_sem)
    own_copy.start()

    for k in range(1, n_row):
        over_row_arrival(packs, send_p, recv_p, k).wait_recv()
    for q in range(1, NX):
        over_x_arrival(pieces[q]).wait_recv()
        launch(0, q)

    every_meta = packs[0, per_dev:]
    for r in range(1, n_row):
        every_meta = every_meta + packs[r, per_dev:]
    bp = lax.broadcasted_iota(jnp.int32, (BLOCK, BLOCK), 0)
    bq = lax.broadcasted_iota(jnp.int32, (BLOCK, BLOCK), 1)
    diag = bp == bq

    def turned(line):
        return jnp.sum(jnp.where(diag, line, 0.0), axis=1, keepdims=True)

    count = 2 * n_row * half // BLOCK
    across_tile = [every_meta[u : u + 1] for u in range(count)]
    down_tile = []
    for u in range(count):
        s, h = u // 2, u % 2
        low = jnp.concatenate(
            [packs[h * per_tile + k, s * half : (s + 1) * half] for k in range(per_tile)], axis=0
        )
        amount = turned(every_meta[u + 4 : u + 5]).astype(jnp.int32)
        both = jnp.concatenate([low, jnp.zeros_like(low)], axis=1)
        for bit in range(7):
            both = jnp.where(((amount >> bit) & 1) == 1, pltpu.roll(both, 1 << bit, 1), both)
        wide[u * BLOCK : (u + 1) * BLOCK] = both
        down = turned(across_tile[u])
        down_tile.append(down)
        tile_of[u * BLOCK : (u + 1) * BLOCK] = jnp.broadcast_to(down, (BLOCK, LANE))

    def of_row(ref, r):
        return jnp.concatenate(
            [ref[pl.ds(pl.multiple_of(s * n_row * half + r * half, half), half)] for s in range(2)], axis=0
        )

    prev_row = jnp.maximum(row - 1, 0)
    own_wide = of_row(wide, row)
    own_tile = of_row(tile_of, row) - (row * tiles_dev).astype(F32)
    prev_tile = of_row(tile_of, prev_row) - (row * tiles_dev).astype(F32)
    prev_high = jnp.where(prev_tile == -1.0, of_row(wide, prev_row)[:, LANE:], 0.0)

    table = dot3_nt(windows[...], own_wide)
    place = lax.broadcasted_iota(jnp.int32, (rows, per_dev), 1) // refl
    total = jnp.zeros((rows, per_dev), F32)
    for c in range(2 * spans):
        total = total + jnp.where(place == c, table[c * rows : (c + 1) * rows], 0.0)
    behind = dot3_nt(eigen[:, :LANE], prev_high)
    inners[row] = jnp.concatenate([total, behind], axis=1)
    for k in range(1, n_row):
        over_row(inners, send_w, recv_w, k).start()
    pump(0, 0)

    keep = (((bp // refl) == (bq // refl)) & (bp > bq)) | (((bp // refl) != (bq // refl)) & (bp < bq))
    strict, across = {}, []
    for u in range(count):
        mine = wide[u * BLOCK : (u + 1) * BLOCK]
        rest = wide[u * BLOCK :]
        level = dot3_nt(mine, rest)
        after = dot3_nt(mine[:, LANE:], rest[:, :LANE])
        before = dot3_nt(mine[:, :LANE], rest[:, LANE:])
        for t in range(u, count):
            cols_at = slice((t - u) * BLOCK, (t - u + 1) * BLOCK)
            gap = across_tile[t] - down_tile[u]
            tile = jnp.where(
                gap == 0.0,
                level[:, cols_at],
                jnp.where(gap == 1.0, after[:, cols_at], jnp.where(gap == -1.0, before[:, cols_at], 0.0)),
            )
            if t == u:
                picked = jnp.where(diag, tile, 0.0)
                scale = 2.0 / jnp.sum(picked, axis=1, keepdims=True)
                across.append(2.0 / jnp.sum(picked, axis=0, keepdims=True))
                tile = jnp.where(keep, tile, 0.0)
            strict[u, t] = tile * scale
        if u == 1:
            pump(0, 1)
    pump(0, 2)
    inverse = tile_inverses([strict[t, t] for t in range(count)])
    pump(0, 3)

    for k in range(1, n_row):
        over_row_arrival(inners, send_w, recv_w, k).wait_recv()
    lane = lax.broadcasted_iota(jnp.int32, (rows, LANE), 1) // half
    right = [jnp.zeros((rows, LANE), F32) for _ in range(count)]
    for r in range(n_row):
        values = inners[r]
        for s in range(2):
            u = s * 2 + r // per_tile
            moved = pltpu.roll(values, (half * (r % per_tile) - half * s) % LANE, 1)
            right[u] = right[u] + jnp.where(lane == r % per_tile, moved, 0.0)
            if r > 0:
                u = s * 2 + (r - 1) // per_tile
                moved = pltpu.roll(values, (half * ((r - 1) % per_tile) - per_dev - half * s) % LANE, 1)
                right[u] = right[u] + jnp.where(lane == (r - 1) % per_tile, moved, 0.0)
    found = []
    for t in range(count):
        value = right[t]
        for u in range(t):
            value = value - dot3(found[u], strict[u, t])
        found.append(dot3(value, inverse[t]))
    solved = [found[t] * across[t] for t in range(count)]
    pump(1, 0)

    def coeffs_of(r):
        result = jnp.zeros((rows, LANE), F32)
        for s in range(2):
            tile = jnp.where(r // per_tile == 0, solved[s * 2], solved[s * 2 + 1])
            moved = pltpu.roll(tile, (LANE - half * (r % per_tile) + half * s) % LANE, 1)
            result = jnp.where(lane == s, moved, result)
        return result[:, :per_dev]

    own_coeffs = coeffs_of(row)
    coeffs_top, coeffs_low = halves(own_coeffs)
    coeffs_both = jnp.concatenate([coeffs_top, coeffs_low], axis=0)
    first_change = dot3(coeffs_of(prev_row), prev_high)
    low_top, low_low = [v.astype(F32) for v in halves(own_wide[:, :LANE])]
    high_top, high_low = [v.astype(F32) for v in halves(own_wide[:, LANE:])]

    def over(first, second, tile):
        return jnp.where(own_tile == tile, first, jnp.where(own_tile == tile - 1.0, second, 0.0)).astype(BF16)

    def trade(k):
        target = (cx + k) % NX
        return pltpu.make_async_remote_copy(
            src_ref=outgoing.at[target],
            dst_ref=traded.at[cx],
            send_sem=send_x.at[k - 1],
            recv_sem=recv_x.at[k - 1],
            device_id={"cx": target},
            device_id_type=mesh,
        )

    def trade_arrival(k):
        source = (cx + NX - k) % NX
        return pltpu.make_async_remote_copy(
            src_ref=outgoing.at[source],
            dst_ref=traded.at[source],
            send_sem=send_x.at[k - 1],
            recv_sem=recv_x.at[k - 1],
            device_id={"cx": source},
            device_id_type=mesh,
        )

    group = 5
    per_part = part // LANE

    def changed(tile, tiles):
        base = tile.astype(F32) if not isinstance(tile, int) else jnp.float32(tile)
        top = jnp.concatenate([over(low_top, high_top, base + k) for k in range(tiles)], axis=1)
        low = jnp.concatenate([over(low_low, high_low, base + k) for k in range(tiles)], axis=1)
        return spread_dot(coeffs_top, coeffs_both, top, low)

    def apply(x):
        whole_groups = min(per_part, tiles_dev - x * per_part) // group

        def one(step, carry):
            tile = x * per_part + step * group
            at = pl.ds(pl.multiple_of(tile * LANE, LANE), group * LANE)
            value = eigen[:, at] - changed(tile, group)
            kept[:, at] = value
            outgoing[x, :, pl.ds(pl.multiple_of(step * group * LANE, LANE), group * LANE)] = value.astype(BF16)
            return carry

        lax.fori_loop(0, whole_groups, one, 0)
        tile = x * per_part + whole_groups * group
        over_tiles = min((x + 1) * per_part, tiles_dev) - tile
        begin = whole_groups * group * LANE
        if over_tiles > 0:
            value = eigen[:, tile * LANE :] - changed(tile, over_tiles)
            kept[:, tile * LANE :] = value
            outgoing[x, :, begin : begin + over_tiles * LANE] = value.astype(BF16)
            begin += over_tiles * LANE
        if begin < part:
            outgoing[x, :, begin:] = jnp.zeros((rows, part - begin), BF16)
        if x == 0:
            value = kept[:, :LANE] - first_change
            kept[:, :LANE] = value
            outgoing[0, :, :LANE] = value.astype(BF16)

    for x in range(NX):
        apply(x)
        pump(1, x + 1) if x + 1 < NX else None
    for k in (1, 3, 2):
        trade(k).start()
    own_copy.wait()
    keep_own = pltpu.make_async_copy(outgoing.at[cx], traded.at[cx], own_sem)
    keep_own.start()
    for d in range(2, last + 1):
        for q in range(NX):
            pump(d, q)
    keep_own.wait()
    for k in range(1, NX):
        trade(k).wait_send()
        trade_arrival(k).wait_recv()
        over_x(k).wait_send()
    for k in range(1, n_row):
        over_row(packs, send_p, recv_p, k).wait_send()
        over_row(inners, send_w, recv_w, k).wait_send()
    for d in range(last + 1):
        for q in range(NX):
            for ahead in (True, False):
                if goes(ahead, d, q):
                    ring(ahead, d, q, False).wait_send()


def span_step(offs, vectors, windows, eigen, cut, n_row):
    rows, cols = eigen.shape
    n_x, n_panel, refl_dev, part = cut.shape
    per_dev, band = vectors.shape
    dma = pltpu.SemaphoreType.DMA
    vmem = pl.BlockSpec(memory_space=pltpu.VMEM)
    units = (NZ // 2) * NX
    return pl.pallas_call(
        span_kernel,
        out_shape=[
            jax.ShapeDtypeStruct((n_panel, NX, NZ, refl_dev, part), BF16),
            jax.ShapeDtypeStruct((NX, rows, part), BF16),
            jax.ShapeDtypeStruct((rows, cols), F32),
        ],
        in_specs=[pl.BlockSpec(memory_space=pltpu.SMEM), vmem, vmem, vmem, vmem],
        out_specs=[vmem] * 3,
        scratch_shapes=[
            pltpu.VMEM((n_row, per_dev + 8, band), F32),
            pltpu.VMEM((n_row, rows, LANE), F32),
            pltpu.VMEM((n_row * per_dev, 2 * LANE), F32),
            pltpu.VMEM((n_row * per_dev, LANE), F32),
            pltpu.VMEM((NX, rows, part), BF16),
            dma((NX - 1,)),
            dma((NX - 1,)),
            dma((n_row - 1,)),
            dma((n_row - 1,)),
            dma((n_row - 1,)),
            dma((n_row - 1,)),
            dma((units,)),
            dma((units,)),
            dma((units,)),
            dma((units,)),
            dma((NX - 1,)),
            dma((NX - 1,)),
            dma(()),
        ],
        compiler_params=pltpu.CompilerParams(
            collective_id=1, has_side_effects=True, vmem_limit_bytes=50 * 1024 * 1024
        ),
        cost_estimate=pl.CostEstimate(flops=20_000_000_000, bytes_accessed=8_000_000, transcendentals=0),
    )(offs, vectors, windows, eigen, cut)


def prepare_kernel(offs, eigen, panels, windows, cut):
    rows, cols = eigen.shape
    tiles_dev = cols // LANE
    part = cut.shape[3]
    for c in range(windows.shape[0] // rows):
        at = offs[c] >> 7
        inside = jnp.where(at + 1 < tiles_dev, 1.0, 0.0).astype(F32)
        then = jnp.minimum(at + 1, tiles_dev - 1)
        windows[c * rows : (c + 1) * rows, :LANE] = eigen[:, pl.ds(pl.multiple_of(at * LANE, LANE), LANE)]
        windows[c * rows : (c + 1) * rows, LANE:] = (
            eigen[:, pl.ds(pl.multiple_of(then * LANE, LANE), LANE)] * inside
        )
    for x in range(NX):
        size = min(part, cols - x * part)
        for p in range(panels.shape[0]):
            cut[x, p, :, :size] = panels[p, :, x * part : x * part + size]
            if size < part:
                cut[x, p, :, size:] = jnp.zeros((panels.shape[1], part - size), BF16)


def prepare(offs, eigen, panels, part):
    rows = eigen.shape[0]
    n_panel, refl_dev, _ = panels.shape
    vmem = pl.BlockSpec(memory_space=pltpu.VMEM)
    return pl.pallas_call(
        prepare_kernel,
        out_shape=[
            jax.ShapeDtypeStruct((offs.shape[0] * rows, 2 * LANE), F32),
            jax.ShapeDtypeStruct((NX, n_panel, refl_dev, part), BF16),
        ],
        in_specs=[pl.BlockSpec(memory_space=pltpu.SMEM), vmem, vmem],
        out_specs=[vmem] * 2,
    )(offs, eigen, panels)


def local(eigvecs, span_vectors, span_offsets, panels):
    rows, cols = eigvecs.shape
    sweeps, spans_dev, refl, band = span_vectors.shape
    n_row = lax.psum(1, "row")
    part = -(-(cols // LANE) // NX) * LANE
    full = part * NX
    offs = span_offsets.reshape(-1)
    windows, cut = prepare(offs, eigvecs, panels, part)
    gathered, traded, eigen = span_step(offs, span_vectors.reshape(-1, band), windows, eigvecs, cut, n_row)
    home = panel_step(traded.reshape(NX * rows, part), gathered.reshape(-1, part), n_row)
    home = home.transpose(1, 0, 2).reshape(rows, full)[:, :cols]
    return eigen - home.astype(F32)


def solution(mesh):
    finer = Mesh(mesh.devices.reshape(mesh.shape["row"], NX, NZ), ("row", "cx", "cz"))
    col = ("cx", "cz")
    placed = (P(col, "row"), P(None, "row", None, None), P(None, "row"), P(None, col, "row"))
    return jax.shard_map(local, mesh=finer, in_specs=placed, out_specs=P(col, "row"), check_vma=False)
```

```python
import functools

import jax
import jax.numpy as jnp
from jax import lax
from jax.experimental import pallas as pl
from jax.experimental.pallas import tpu as pltpu
from jax.sharding import Mesh
from jax.sharding import PartitionSpec as P

LANE = 128
BLOCK = 128
NX = 4
NZ = 8
CHUNKS = 5
F32 = jnp.float32
BF16 = jnp.bfloat16
NT = (((1,), (1,)), ((), ()))
NN = (((1,), (0,)), ((), ()))


def halves(a):
    top = a.astype(BF16)
    return top, (a - top.astype(F32)).astype(BF16)


def dot3(a, b):
    a_top, a_low = halves(a)
    b_top, b_low = halves(b)
    d = functools.partial(lax.dot_general, dimension_numbers=NN, preferred_element_type=F32)
    return d(a_top, b_top) + (d(a_top, b_low) + d(a_low, b_top))


GRAM_TILES = ((0, 0), (0, 2), (0, 3), (1, 0), (1, 1), (1, 2), (1, 3), (2, 2), (3, 2), (3, 3))


def dot3_nt(a, b):
    a_top, a_low = halves(a)
    b_top, b_low = halves(b)
    d = functools.partial(lax.dot_general, dimension_numbers=NT, preferred_element_type=F32)
    return d(a_top, b_top) + (d(a_top, b_low) + d(a_low, b_top))


def tile_inverses(tiles):
    bp = lax.broadcasted_iota(jnp.int32, (BLOCK, BLOCK), 0)
    bq = lax.broadcasted_iota(jnp.int32, (BLOCK, BLOCK), 1)
    eye = (bp == bq).astype(F32)
    inverse = [eye - jnp.where(bp // 2 == bq // 2, tile, 0.0) for tile in tiles]
    size = 2
    while size < BLOCK:
        joined = (bp // (2 * size) == bq // (2 * size)) & (bp // size != bq // size)
        left = [dot3(inv, jnp.where(joined, tile, 0.0)) for inv, tile in zip(inverse, tiles)]
        inverse = [inv - dot3(lhs, inv) for inv, lhs in zip(inverse, left)]
        size *= 2
    return inverse


def fused_kernel(offs, vectors, eigen, panels, kept, home, cut, gathered, packs, inners, wide, tile_of, placed_top,
                 placed_low, outgoing, traded, acc_top, acc_low, work, slots, whole, change, send_a, recv_a, send_p,
                 recv_p, send_w, recv_w, send_f, recv_f, send_b, recv_b, send_x, recv_x, send_rs, recv_rs, send_ag,
                 recv_ag, send_h, recv_h, own_sem):
    row, cx, cz = lax.axis_index("row"), lax.axis_index("cx"), lax.axis_index("cz")
    n_row = lax.axis_size("row")
    rows, cols = eigen.shape
    tiles_dev = cols // LANE
    part = cut.shape[3]
    per_part = part // LANE
    chunk = part // CHUNKS
    per_dev = vectors.shape[0]
    half = per_dev // 2
    refl = 4
    spans = half // refl
    per_tile = BLOCK // half
    peers = n_row * NX
    me = row * NX + cx
    owners = work.shape[0]
    mesh = pl.DeviceIdType.MESH

    def device(place):
        return {"row": place // NX, "cx": place % NX}

    barrier = pltpu.get_barrier_semaphore()
    for k in (1, NZ - 1):
        pl.semaphore_signal(barrier, inc=1, device_id={"cz": (cz + k) % NZ}, device_id_type=mesh)
    for k in range(1, peers):
        pl.semaphore_signal(barrier, inc=1, device_id=device((me + k) % peers), device_id_type=mesh)

    for x in range(NX):
        size = min(part, cols - x * part)
        for p in range(panels.shape[0]):
            cut[x, p, :, :size] = panels[p, :, x * part : x * part + size]
            if size < part:
                cut[x, p, :, size:] = jnp.zeros((panels.shape[1], part - size), BF16)

    lane8 = lax.broadcasted_iota(jnp.int32, (8, LANE), 1)
    line8 = lax.broadcasted_iota(jnp.int32, (8, LANE), 0)
    line64 = lax.broadcasted_iota(jnp.int32, (per_dev, LANE), 0) // refl
    meta = jnp.zeros((8, LANE), F32)
    own_tile = jnp.zeros((per_dev, LANE), F32)
    own_shift = jnp.zeros((per_dev, LANE), jnp.int32)
    for s in range(2):
        for b in range(spans):
            at = offs[s, b]
            tile_at = at >> 7
            shift_at = at & 127
            place = (row % per_tile) * half + b * refl
            mine = (lane8 >= place) & (lane8 < place + refl)
            line = s * 2 + row // per_tile
            meta = jnp.where(mine & (line8 == line), (tile_at + row * tiles_dev).astype(F32), meta)
            meta = jnp.where(mine & (line8 == line + 4), shift_at.astype(F32), meta)
            own_tile = jnp.where(line64 == s * spans + b, tile_at.astype(F32), own_tile)
            own_shift = jnp.where(line64 == s * spans + b, shift_at, own_shift)
    packs[row, :per_dev] = vectors[...]
    packs[row, per_dev:] = meta

    def over_x(j, k):
        at = pl.ds(j * chunk, chunk)
        return pltpu.make_async_remote_copy(
            src_ref=cut.at[(cx + k) % NX, :, :, at],
            dst_ref=gathered.at[:, cx, cz, :, at],
            send_sem=send_a.at[j, k - 1],
            recv_sem=recv_a.at[j, k - 1],
            device_id={"cx": (cx + k) % NX},
            device_id_type=mesh,
        )

    def over_x_arrival(j, k):
        at = pl.ds(j * chunk, chunk)
        source = (cx + NX - k) % NX
        return pltpu.make_async_remote_copy(
            src_ref=cut.at[source, :, :, at],
            dst_ref=gathered.at[:, source, cz, :, at],
            send_sem=send_a.at[j, k - 1],
            recv_sem=recv_a.at[j, k - 1],
            device_id={"cx": source},
            device_id_type=mesh,
        )

    def over_row(ref, sends, recvs, k):
        return pltpu.make_async_remote_copy(
            src_ref=ref.at[row],
            dst_ref=ref.at[row],
            send_sem=sends.at[k - 1],
            recv_sem=recvs.at[k - 1],
            device_id={"row": (row + k) % n_row},
            device_id_type=mesh,
        )

    def over_row_arrival(ref, sends, recvs, k):
        source = (row + n_row - k) % n_row
        return pltpu.make_async_remote_copy(
            src_ref=ref.at[source],
            dst_ref=ref.at[source],
            send_sem=sends.at[k - 1],
            recv_sem=recvs.at[k - 1],
            device_id={"row": source},
            device_id_type=mesh,
        )

    last = NZ // 2 - 1

    def ring(ahead, d, j, arriving):
        step = 1 if ahead else NZ - 1
        held = (cz + (NZ - d)) % NZ if ahead else (cz + d) % NZ
        if arriving:
            held = (held + (NZ - step)) % NZ
        at = pl.ds(j * chunk, chunk)
        panel = slice(None) if d < last else (pl.ds(0, 1) if ahead else pl.ds(1, 1))
        place = gathered.at[panel, :, held, :, at]
        return pltpu.make_async_remote_copy(
            src_ref=place,
            dst_ref=place,
            send_sem=(send_f if ahead else send_b).at[d * CHUNKS + j],
            recv_sem=(recv_f if ahead else recv_b).at[d * CHUNKS + j],
            device_id={"cz": (cz + step) % NZ},
            device_id_type=mesh,
        )

    def launch(d, j):
        for ahead in (True, False):
            ring(ahead, d, j, False).start()

    def pump(d, j):
        for ahead in (True, False):
            ring(ahead, d, j, True).wait_recv()
            if d < last:
                ring(ahead, d + 1, j, False).start()

    own_copy = pltpu.make_async_copy(cut.at[cx], gathered.at[:, cx, cz], own_sem)
    own_copy.start()
    pl.semaphore_wait(barrier, peers - 1 + 2)
    for j in range(CHUNKS):
        for k in (1, 3, 2):
            over_x(j, k).start()
        if j == 0:
            for k in range(1, n_row):
                over_row(packs, send_p, recv_p, k).start()

    def shifted(values, amount):
        both = jnp.concatenate([values, jnp.zeros_like(values)], axis=1)
        for bit in range(7):
            both = jnp.where(((amount >> bit) & 1) == 1, pltpu.roll(both, 1 << bit, 1), both)
        return both

    own_wide = shifted(vectors[...], jnp.concatenate([own_shift, own_shift], axis=1))
    low_top, low_low = [v.astype(F32) for v in halves(own_wide[:, :LANE])]
    high_top, high_low = [v.astype(F32) for v in halves(own_wide[:, LANE:])]
    group = 7

    def build(step, carry):
        for k in range(group):
            tile = (step * group + k).astype(F32)
            first, second = own_tile == tile, own_tile == tile - 1.0
            at = pl.ds(pl.multiple_of((step * group + k) * LANE, LANE), LANE)
            placed_top[:, at] = jnp.where(first, low_top, jnp.where(second, high_top, 0.0)).astype(BF16)
            placed_low[:, at] = jnp.where(first, low_low, jnp.where(second, high_low, 0.0)).astype(BF16)
        return carry

    lax.fori_loop(0, tiles_dev // group, build, 0)
    own_copy.wait()
    for j in range(CHUNKS):
        for k in (1, 3, 2):
            over_x_arrival(j, k).wait_recv()
        launch(0, j)

    mxu_nt = functools.partial(lax.dot_general, dimension_numbers=NT, preferred_element_type=F32)
    mxu = functools.partial(lax.dot_general, dimension_numbers=NN, preferred_element_type=F32)

    def inner_step(step, total):
        at = pl.ds(pl.multiple_of(step * group * LANE, LANE), group * LANE)
        top, low = halves(eigen[:, at])
        first = mxu_nt(jnp.concatenate([top, low], axis=0), placed_top[:, at])
        return total + first[:rows] + first[rows:] + mxu_nt(top, placed_low[:, at])

    total = lax.fori_loop(0, tiles_dev // group, inner_step, jnp.zeros((rows, per_dev), F32))

    for k in range(1, n_row):
        over_row_arrival(packs, send_p, recv_p, k).wait_recv()
    every_meta = packs[0, per_dev:]
    for r in range(1, n_row):
        every_meta = every_meta + packs[r, per_dev:]
    bp = lax.broadcasted_iota(jnp.int32, (BLOCK, BLOCK), 0)
    bq = lax.broadcasted_iota(jnp.int32, (BLOCK, BLOCK), 1)
    diag = bp == bq

    def turned(line):
        return jnp.sum(jnp.where(diag, line, 0.0), axis=1, keepdims=True)

    count = 2 * n_row * half // BLOCK
    across_tile = [every_meta[u : u + 1] for u in range(count)]
    down_tile = []
    for u in range(count):
        s, h = u // 2, u % 2
        low = jnp.concatenate(
            [packs[h * per_tile + k, s * half : (s + 1) * half] for k in range(per_tile)], axis=0
        )
        wide[u * BLOCK : (u + 1) * BLOCK] = shifted(low, turned(every_meta[u + 4 : u + 5]).astype(jnp.int32))
        down = turned(across_tile[u])
        down_tile.append(down)
        tile_of[u * BLOCK : (u + 1) * BLOCK] = jnp.broadcast_to(down, (BLOCK, LANE))

    def of_row(ref, r):
        return jnp.concatenate(
            [ref[pl.ds(pl.multiple_of(s * n_row * half + r * half, half), half)] for s in range(2)], axis=0
        )

    prev_row = jnp.maximum(row - 1, 0)
    prev_tile = of_row(tile_of, prev_row) - (row * tiles_dev).astype(F32)
    prev_high = jnp.where(prev_tile == -1.0, of_row(wide, prev_row)[:, LANE:], 0.0)
    behind = dot3_nt(eigen[:, :LANE], prev_high)
    inners[row] = jnp.concatenate([total, behind], axis=1)
    for k in range(1, n_row):
        over_row(inners, send_w, recv_w, k).start()
    pump(0, 0)
    pump(0, 1)

    keep = (((bp // refl) == (bq // refl)) & (bp > bq)) | (((bp // refl) != (bq // refl)) & (bp < bq))
    strict, across = {}, []
    for u in range(count):
        mine = wide[u * BLOCK : (u + 1) * BLOCK]
        rest = wide[u * BLOCK :]
        level = dot3_nt(mine, rest)
        after = dot3_nt(mine[:, LANE:], rest[:, :LANE])
        before = dot3_nt(mine[:, :LANE], rest[:, LANE:])
        for t in range(u, count):
            cols_at = slice((t - u) * BLOCK, (t - u + 1) * BLOCK)
            gap = across_tile[t] - down_tile[u]
            tile = jnp.where(
                gap == 0.0,
                level[:, cols_at],
                jnp.where(gap == 1.0, after[:, cols_at], jnp.where(gap == -1.0, before[:, cols_at], 0.0)),
            )
            if t == u:
                picked = jnp.where(diag, tile, 0.0)
                scale = 2.0 / jnp.sum(picked, axis=1, keepdims=True)
                across.append(2.0 / jnp.sum(picked, axis=0, keepdims=True))
                tile = jnp.where(keep, tile, 0.0)
            strict[u, t] = tile * scale
        if u == 1:
            pump(0, 2)
    pump(0, 3)
    inverse = tile_inverses([strict[t, t] for t in range(count)])
    pump(0, 4)

    for k in range(1, n_row):
        over_row_arrival(inners, send_w, recv_w, k).wait_recv()
    lane = lax.broadcasted_iota(jnp.int32, (rows, LANE), 1) // half
    right = [jnp.zeros((rows, LANE), F32) for _ in range(count)]
    for r in range(n_row):
        values = inners[r]
        for s in range(2):
            u = s * 2 + r // per_tile
            moved = pltpu.roll(values, (half * (r % per_tile) - half * s) % LANE, 1)
            right[u] = right[u] + jnp.where(lane == r % per_tile, moved, 0.0)
            if r > 0:
                u = s * 2 + (r - 1) // per_tile
                moved = pltpu.roll(values, (half * ((r - 1) % per_tile) - per_dev - half * s) % LANE, 1)
                right[u] = right[u] + jnp.where(lane == (r - 1) % per_tile, moved, 0.0)
    found = []
    for t in range(count):
        value = right[t]
        for u in range(t):
            value = value - dot3(found[u], strict[u, t])
        found.append(dot3(value, inverse[t]))
    solved = [found[t] * across[t] for t in range(count)]
    pump(1, 0)

    def coeffs_of(r):
        result = jnp.zeros((rows, LANE), F32)
        for s in range(2):
            tile = jnp.where(r // per_tile == 0, solved[s * 2], solved[s * 2 + 1])
            moved = pltpu.roll(tile, (LANE - half * (r % per_tile) + half * s) % LANE, 1)
            result = jnp.where(lane == s, moved, result)
        return result[:, :per_dev]

    coeffs_top, coeffs_low = halves(coeffs_of(row))
    coeffs_both = jnp.concatenate([coeffs_top, coeffs_low], axis=0)
    first_change = dot3(coeffs_of(prev_row), prev_high)

    def changed(at):
        first = mxu(coeffs_both, placed_top[:, at])
        return first[:rows] + first[rows:] + mxu(coeffs_top, placed_low[:, at])

    def trade(x):
        return pltpu.make_async_remote_copy(
            src_ref=outgoing.at[x],
            dst_ref=traded.at[cx],
            send_sem=send_x.at[x],
            recv_sem=recv_x.at[cx],
            device_id={"cx": x},
            device_id_type=mesh,
        )

    def trade_arrival(x):
        return pltpu.make_async_remote_copy(
            src_ref=outgoing.at[x],
            dst_ref=traded.at[x],
            send_sem=send_x.at[x],
            recv_sem=recv_x.at[x],
            device_id={"cx": x},
            device_id_type=mesh,
        )

    five = 5

    def apply(x):
        whole_groups = min(per_part, tiles_dev - x * per_part) // five

        def one(step, carry):
            tile = x * per_part + step * five
            at = pl.ds(pl.multiple_of(tile * LANE, LANE), five * LANE)
            value = eigen[:, at] - changed(at)
            kept[:, at] = value
            outgoing[x, :, pl.ds(pl.multiple_of(step * five * LANE, LANE), five * LANE)] = value.astype(BF16)
            return carry

        lax.fori_loop(0, whole_groups, one, 0)
        tile = x * per_part + whole_groups * five
        over_tiles = min((x + 1) * per_part, tiles_dev) - tile
        begin = whole_groups * five * LANE
        if over_tiles > 0:
            at = slice(tile * LANE, (tile + over_tiles) * LANE)
            value = eigen[:, at] - changed(at)
            kept[:, at] = value
            outgoing[x, :, begin : begin + over_tiles * LANE] = value.astype(BF16)
            begin += over_tiles * LANE
        if begin < part:
            outgoing[x, :, begin:] = jnp.zeros((rows, part - begin), BF16)
        if x == 0:
            value = kept[:, :LANE] - first_change
            kept[:, :LANE] = value
            outgoing[0, :, :LANE] = value.astype(BF16)

    for x in range(NX):
        apply(x)
        pl.when(cx != x)(trade(x).start)
        pump(1, x + 1)
    keep_own = pltpu.make_async_copy(outgoing.at[cx], traded.at[cx], own_sem)
    keep_own.start()
    acc_top[...] = jnp.zeros_like(acc_top)
    acc_low[...] = jnp.zeros_like(acc_low)
    for j in range(CHUNKS):
        pump(2, j)
    keep_own.wait()
    for x in range(NX):
        pl.when(cx != x)(trade_arrival(x).wait_recv)

    def reflect(at, panel):
        return gathered[panel, :, :, :, at].reshape(-1, chunk)

    for j in range(CHUNKS):
        pump(last, j)
        at = slice(j * chunk, (j + 1) * chunk)
        upper, lower = reflect(at, 0), reflect(at, 1)
        both = jnp.concatenate([upper, lower], axis=0)
        top = jnp.concatenate([traded[:, :, at].reshape(-1, chunk), upper], axis=0)
        acc_top[...] += mxu_nt(top, both)
        acc_low[...] += mxu_nt(lower, lower)

    piece = BLOCK // 2

    def put(place, value):
        rounded = value.astype(BF16)
        work[2 * place] = rounded[:piece]
        work[2 * place + 1] = rounded[piece:]

    for place, (u, t) in enumerate(GRAM_TILES):
        if u < 2:
            put(place, acc_top[(1 + u) * BLOCK : (2 + u) * BLOCK, t * BLOCK : (t + 1) * BLOCK])
        else:
            put(place, acc_low[(u - 2) * BLOCK : (u - 1) * BLOCK, (t - 2) * BLOCK : (t - 1) * BLOCK])
    for t in range(4):
        put(len(GRAM_TILES) + t, acc_top[:BLOCK, t * BLOCK : (t + 1) * BLOCK])

    def scatter(k):
        target = (me + k) % peers
        return target, pltpu.make_async_remote_copy(
            src_ref=work.at[lax.rem(target, owners)],
            dst_ref=slots.at[k - 1],
            send_sem=send_rs.at[k - 1],
            recv_sem=recv_rs.at[k - 1],
            device_id=device(target),
            device_id_type=mesh,
        )

    def gather(k):
        return pltpu.make_async_remote_copy(
            src_ref=whole.at[lax.rem(me, owners)],
            dst_ref=whole.at[lax.rem(me, owners)],
            send_sem=send_ag.at[k - 1],
            recv_sem=recv_ag.at[k - 1],
            device_id=device((me + k) % peers),
            device_id_type=mesh,
        )

    def arrival(k):
        source = lax.rem((me + peers - k) % peers, owners)
        return pltpu.make_async_remote_copy(
            src_ref=whole.at[source],
            dst_ref=whole.at[source],
            send_sem=send_ag.at[k - 1],
            recv_sem=recv_ag.at[k - 1],
            device_id=device((me + k) % peers),
            device_id_type=mesh,
        )

    for k in range(1, peers):
        target, copy = scatter(k)
        pl.when(target < owners)(copy.start)

    @pl.when(me < owners)
    def _():
        value = work[lax.rem(me, owners)].astype(F32)
        for k in range(1, peers):
            scatter(k)[1].wait_recv()
            value = value + slots[k - 1].astype(F32)
        whole[lax.rem(me, owners)] = value.astype(BF16)
        for k in range(1, peers):
            gather(k).start()

    for k in range(1, peers):
        source = (me + peers - k) % peers
        pl.when(source < owners)(arrival(k).wait_recv)

    def got(place):
        return jnp.concatenate([whole[2 * place].astype(F32), whole[2 * place + 1].astype(F32)], axis=0)

    gram = {key: got(place) for place, key in enumerate(GRAM_TILES)}
    picked = [jnp.where(diag, gram[t, t], 0.0) for t in range(4)]
    down = [2.0 / jnp.sum(p, axis=1, keepdims=True) for p in picked]
    beside = [2.0 / jnp.sum(p, axis=0, keepdims=True) for p in picked]
    panel_strict = {(u, t): gram[u, t] * down[u] for u, t in GRAM_TILES}
    for t in range(4):
        panel_strict[t, t] = jnp.where(bp > bq, panel_strict[t, t], 0.0)
    panel_inverse = tile_inverses([panel_strict[t, t] for t in range(4)])
    answer = {}
    for t in (1, 0, 3, 2):
        value = got(len(GRAM_TILES) + t)
        for u in tuple(answer):
            value = value - dot3(answer[u], panel_strict[u, t])
        answer[t] = dot3(value, panel_inverse[t])
    coeffs = jnp.concatenate([(answer[t] * beside[t]).astype(BF16) for t in range(4)], axis=1)

    def back(j, k):
        target = (cx + k) % NX
        at = pl.ds(j * chunk, chunk)
        return pltpu.make_async_remote_copy(
            src_ref=change.at[target, :, at],
            dst_ref=home.at[cx, :, at],
            send_sem=send_h.at[j, k - 1],
            recv_sem=recv_h.at[j, k - 1],
            device_id={"cx": target},
            device_id_type=mesh,
        )

    def back_arrival(j, k):
        source = (cx + NX - k) % NX
        at = pl.ds(j * chunk, chunk)
        return pltpu.make_async_remote_copy(
            src_ref=change.at[source, :, at],
            dst_ref=home.at[source, :, at],
            send_sem=send_h.at[j, k - 1],
            recv_sem=recv_h.at[j, k - 1],
            device_id={"cx": source},
            device_id_type=mesh,
        )

    for j in range(CHUNKS):
        at = slice(j * chunk, (j + 1) * chunk)
        value = mxu(coeffs, jnp.concatenate([reflect(at, 0), reflect(at, 1)], axis=0)).astype(BF16)
        for x in range(NX):
            change[x, :, at] = value[x * rows : (x + 1) * rows]
        for k in (2, 1, 3):
            back(j, k).start()
    keep_home = pltpu.make_async_copy(change.at[cx], home.at[cx], own_sem)
    keep_home.start()

    for x in range(NX):
        pl.when(cx != x)(trade(x).wait_send)
    for k in range(1, n_row):
        over_row(packs, send_p, recv_p, k).wait_send()
        over_row(inners, send_w, recv_w, k).wait_send()
    for d in range(last + 1):
        for j in range(CHUNKS):
            for ahead in (True, False):
                ring(ahead, d, j, False).wait_send()
    for k in range(1, peers):
        target, copy = scatter(k)
        pl.when(target < owners)(copy.wait_send)

    @pl.when(me < owners)
    def _():
        for k in range(1, peers):
            gather(k).wait_send()

    keep_home.wait()
    for j in range(CHUNKS):
        for k in range(1, NX):
            over_x(j, k).wait_send()
            back(j, k).wait_send()
            back_arrival(j, k).wait_recv()


def fused_step(offs, vectors, eigen, panels, n_row):
    rows, cols = eigen.shape
    n_panel, refl_dev, _ = panels.shape
    part = -(-(cols // LANE) // NX) * LANE
    per_dev, band = vectors.shape
    peers = n_row * NX
    owners = 2 * (len(GRAM_TILES) + 4)
    piece = BLOCK // 2
    dma = pltpu.SemaphoreType.DMA
    vmem = pl.BlockSpec(memory_space=pltpu.VMEM)
    units = (NZ // 2) * CHUNKS
    return pl.pallas_call(
        fused_kernel,
        out_shape=[jax.ShapeDtypeStruct((rows, cols), F32), jax.ShapeDtypeStruct((NX, rows, part), BF16)],
        in_specs=[pl.BlockSpec(memory_space=pltpu.SMEM), vmem, vmem, vmem],
        out_specs=[vmem] * 2,
        scratch_shapes=[
            pltpu.VMEM((NX, n_panel, refl_dev, part), BF16),
            pltpu.VMEM((n_panel, NX, NZ, refl_dev, part), BF16),
            pltpu.VMEM((n_row, per_dev + 8, band), F32),
            pltpu.VMEM((n_row, rows, LANE), F32),
            pltpu.VMEM((n_row * per_dev, 2 * LANE), F32),
            pltpu.VMEM((n_row * per_dev, LANE), F32),
            pltpu.VMEM((per_dev, cols), BF16),
            pltpu.VMEM((per_dev, cols), BF16),
            pltpu.VMEM((NX, rows, part), BF16),
            pltpu.VMEM((NX, rows, part), BF16),
            pltpu.VMEM((NX * rows + 2 * BLOCK, 4 * BLOCK), F32),
            pltpu.VMEM((2 * BLOCK, 2 * BLOCK), F32),
            pltpu.VMEM((owners, piece, BLOCK), BF16),
            pltpu.VMEM((peers - 1, piece, BLOCK), BF16),
            pltpu.VMEM((owners, piece, BLOCK), BF16),
            pltpu.VMEM((NX, rows, part), BF16),
            dma((CHUNKS, NX - 1)),
            dma((CHUNKS, NX - 1)),
            dma((n_row - 1,)),
            dma((n_row - 1,)),
            dma((n_row - 1,)),
            dma((n_row - 1,)),
            dma((units,)),
            dma((units,)),
            dma((units,)),
            dma((units,)),
            dma((NX,)),
            dma((NX,)),
            dma((peers - 1,)),
            dma((peers - 1,)),
            dma((peers - 1,)),
            dma((peers - 1,)),
            dma((CHUNKS, NX - 1)),
            dma((CHUNKS, NX - 1)),
            dma(()),
        ],
        compiler_params=pltpu.CompilerParams(
            collective_id=0, has_side_effects=True, vmem_limit_bytes=40 * 1024 * 1024
        ),
        cost_estimate=pl.CostEstimate(flops=20_000_000_000, bytes_accessed=8_000_000, transcendentals=0),
    )(offs, vectors, eigen, panels)


def local(eigvecs, span_vectors, span_offsets, panels):
    rows, cols = eigvecs.shape
    band = span_vectors.shape[3]
    n_row = lax.psum(1, "row")
    eigen, home = fused_step(span_offsets, span_vectors.reshape(-1, band), eigvecs, panels, n_row)
    home = home.transpose(1, 0, 2).reshape(rows, -1)[:, :cols]
    return eigen - home.astype(F32)


def solution(mesh):
    finer = Mesh(mesh.devices.reshape(mesh.shape["row"], NX, NZ), ("row", "cx", "cz"))
    col = ("cx", "cz")
    placed = (P(col, "row"), P(None, "row", None, None), P(None, "row"), P(None, col, "row"))
    return jax.shard_map(local, mesh=finer, in_specs=placed, out_specs=P(col, "row"), check_vma=False)
```

```python
import functools

import jax
import jax.numpy as jnp
from jax import lax
from jax.experimental import pallas as pl
from jax.experimental.pallas import tpu as pltpu
from jax.sharding import Mesh
from jax.sharding import PartitionSpec as P

LANE = 128
BLOCK = 128
NX = 4
NZ = 8
CHUNKS = 5
F32 = jnp.float32
BF16 = jnp.bfloat16
NT = (((1,), (1,)), ((), ()))
NN = (((1,), (0,)), ((), ()))


def halves(a):
    top = a.astype(BF16)
    return top, (a - top.astype(F32)).astype(BF16)


def dot3(a, b):
    a_top, a_low = halves(a)
    b_top, b_low = halves(b)
    d = functools.partial(lax.dot_general, dimension_numbers=NN, preferred_element_type=F32)
    return d(a_top, b_top) + (d(a_top, b_low) + d(a_low, b_top))


def dot3_nt(a, b):
    a_top, a_low = halves(a)
    b_top, b_low = halves(b)
    d = functools.partial(lax.dot_general, dimension_numbers=NT, preferred_element_type=F32)
    return d(a_top, b_top) + (d(a_top, b_low) + d(a_low, b_top))


def tile_inverses(tiles, between=None):
    bp = lax.broadcasted_iota(jnp.int32, (BLOCK, BLOCK), 0)
    bq = lax.broadcasted_iota(jnp.int32, (BLOCK, BLOCK), 1)
    eye = (bp == bq).astype(F32)
    inverse = [eye - jnp.where(bp // 2 == bq // 2, tile, 0.0) for tile in tiles]
    size = 2
    while size < BLOCK:
        joined = (bp // (2 * size) == bq // (2 * size)) & (bp // size != bq // size)
        left = [dot3(inv, jnp.where(joined, tile, 0.0)) for inv, tile in zip(inverse, tiles)]
        inverse = [inv - dot3(lhs, inv) for inv, lhs in zip(inverse, left)]
        if between is not None:
            between(size)
        size *= 2
    return inverse


def fused_kernel(offs_hbm, vectors_hbm, eigen_hbm, panels_hbm, kept, home, offs, vectors, eigen, cut, gathered, packs,
                 inners, wide, tile_of, placed_top, placed_low, outgoing, traded, shared, held, rounded, delta, acc,
                 work, slots, whole, change, load, send_a, recv_a, send_p, recv_p, send_w, recv_w, send_f, recv_f,
                 send_b, recv_b, send_x, recv_x, send_c, recv_c, send_rs, recv_rs, send_ag, recv_ag, send_h, recv_h,
                 own_sem):
    row, cx, cz = lax.axis_index("row"), lax.axis_index("cx"), lax.axis_index("cz")
    n_row = lax.axis_size("row")
    rows, cols = eigen.shape
    every = NX * rows
    tiles_dev = cols // LANE
    part = cut.shape[3]
    chunk = part // CHUNKS
    n_panel = cut.shape[1]
    per_dev = vectors.shape[0]
    half = per_dev // 2
    refl = 4
    spans = half // refl
    per_tile = BLOCK // half
    peers = n_row * NX
    me = row * NX + cx
    owners = work.shape[1]
    mesh = pl.DeviceIdType.MESH
    mxu_nt = functools.partial(lax.dot_general, dimension_numbers=NT, preferred_element_type=F32)
    mxu = functools.partial(lax.dot_general, dimension_numbers=NN, preferred_element_type=F32)

    def device(place):
        return {"row": place // NX, "cx": place % NX}

    loads = [
        pltpu.make_async_copy(offs_hbm, offs, load.at[0]),
        pltpu.make_async_copy(vectors_hbm, vectors, load.at[1]),
        pltpu.make_async_copy(eigen_hbm, eigen, load.at[2]),
    ]
    for x in range(NX):
        size = min(part, cols - x * part)
        loads.append(
            pltpu.make_async_copy(
                panels_hbm.at[:, :, pl.ds(x * part, size)], cut.at[x, :, :, pl.ds(0, size)], load.at[3 + x]
            )
        )
        if size < part:
            cut[x, :, :, size:] = jnp.zeros((n_panel, cut.shape[2], part - size), BF16)
    for copy in loads:
        copy.start()
    barrier = pltpu.get_barrier_semaphore()
    for k in (1, NZ - 1):
        pl.semaphore_signal(barrier, inc=1, device_id={"cz": (cz + k) % NZ}, device_id_type=mesh)
    for k in range(1, peers):
        pl.semaphore_signal(barrier, inc=1, device_id=device((me + k) % peers), device_id_type=mesh)
    for copy in loads:
        copy.wait()

    lane8 = lax.broadcasted_iota(jnp.int32, (8, LANE), 1)
    line8 = lax.broadcasted_iota(jnp.int32, (8, LANE), 0)
    line64 = lax.broadcasted_iota(jnp.int32, (per_dev, LANE), 0) // refl
    meta = jnp.zeros((8, LANE), F32)
    own_tile = jnp.zeros((per_dev, LANE), F32)
    own_shift = jnp.zeros((per_dev, LANE), jnp.int32)
    for s in range(2):
        for b in range(spans):
            at = offs[s, b]
            tile_at = at >> 7
            shift_at = at & 127
            place = (row % per_tile) * half + b * refl
            mine = (lane8 >= place) & (lane8 < place + refl)
            line = s * 2 + row // per_tile
            meta = jnp.where(mine & (line8 == line), (tile_at + row * tiles_dev).astype(F32), meta)
            meta = jnp.where(mine & (line8 == line + 4), shift_at.astype(F32), meta)
            own_tile = jnp.where(line64 == s * spans + b, tile_at.astype(F32), own_tile)
            own_shift = jnp.where(line64 == s * spans + b, shift_at, own_shift)
    packs[row, :per_dev] = vectors[...]
    packs[row, per_dev:] = meta
    for x in range(NX):
        size = min(part, cols - x * part)
        outgoing[x, :, :size] = eigen[:, x * part : x * part + size].astype(BF16)
        if size < part:
            outgoing[x, :, size:] = jnp.zeros((rows, part - size), BF16)

    def over_x(p, j, k):
        at = pl.ds(j * chunk, chunk)
        return pltpu.make_async_remote_copy(
            src_ref=cut.at[(cx + k) % NX, p, :, at],
            dst_ref=gathered.at[p, cx, cz, :, at],
            send_sem=send_a.at[p * CHUNKS + j, k - 1],
            recv_sem=recv_a.at[p * CHUNKS + j, k - 1],
            device_id={"cx": (cx + k) % NX},
            device_id_type=mesh,
        )

    def over_x_arrival(p, j, k):
        at = pl.ds(j * chunk, chunk)
        source = (cx + NX - k) % NX
        return pltpu.make_async_remote_copy(
            src_ref=cut.at[source, p, :, at],
            dst_ref=gathered.at[p, source, cz, :, at],
            send_sem=send_a.at[p * CHUNKS + j, k - 1],
            recv_sem=recv_a.at[p * CHUNKS + j, k - 1],
            device_id={"cx": source},
            device_id_type=mesh,
        )

    def over_row(ref, sends, recvs, k):
        return pltpu.make_async_remote_copy(
            src_ref=ref.at[row],
            dst_ref=ref.at[row],
            send_sem=sends.at[k - 1],
            recv_sem=recvs.at[k - 1],
            device_id={"row": (row + k) % n_row},
            device_id_type=mesh,
        )

    def over_row_arrival(ref, sends, recvs, k):
        source = (row + n_row - k) % n_row
        return pltpu.make_async_remote_copy(
            src_ref=ref.at[source],
            dst_ref=ref.at[source],
            send_sem=sends.at[k - 1],
            recv_sem=recvs.at[k - 1],
            device_id={"row": source},
            device_id_type=mesh,
        )

    def along_x(source_ref, target_ref, sends, recvs, k):
        target = (cx + k) % NX
        return pltpu.make_async_remote_copy(
            src_ref=source_ref.at[target] if source_ref is not target_ref else source_ref.at[cx],
            dst_ref=target_ref.at[cx],
            send_sem=sends.at[k - 1],
            recv_sem=recvs.at[k - 1],
            device_id={"cx": target},
            device_id_type=mesh,
        )

    def along_x_arrival(source_ref, target_ref, sends, recvs, k):
        source = (cx + NX - k) % NX
        return pltpu.make_async_remote_copy(
            src_ref=source_ref.at[source],
            dst_ref=target_ref.at[source],
            send_sem=sends.at[k - 1],
            recv_sem=recvs.at[k - 1],
            device_id={"cx": source},
            device_id_type=mesh,
        )

    last = NZ // 2 - 1

    def ring(p, ahead, d, j, arriving):
        step = 1 if ahead else NZ - 1
        held_at = (cz + (NZ - d)) % NZ if ahead else (cz + d) % NZ
        if arriving:
            held_at = (held_at + (NZ - step)) % NZ
        at = pl.ds(j * chunk, chunk)
        share = slice(None) if d < last else (pl.ds(0, NX // 2) if ahead else pl.ds(NX // 2, NX // 2))
        place = gathered.at[p, share, held_at, :, at]
        unit = ((last + 1) * p + d) * CHUNKS + j
        return pltpu.make_async_remote_copy(
            src_ref=place,
            dst_ref=place,
            send_sem=(send_f if ahead else send_b).at[unit],
            recv_sem=(recv_f if ahead else recv_b).at[unit],
            device_id={"cz": (cz + step) % NZ},
            device_id_type=mesh,
        )

    def launch(p, j):
        for k in (1, 3, 2):
            over_x_arrival(p, j, k).wait_recv()
        for ahead in (True, False):
            ring(p, ahead, 0, j, False).start()

    def reflect(p, at):
        return gathered[p, :, :, :, at].reshape(-1, chunk)

    def product(p, j):
        at = slice(j * chunk, (j + 1) * chunk)
        mine = reflect(p, at)
        value = mxu_nt(jnp.concatenate([rounded[:, at], mine], axis=0), mine)
        acc[...] = value if j == 0 else acc[...] + value

    queue = [(p, d, j) for p in range(n_panel) for d in range(last + 1) for j in range(CHUNKS)]

    def pump(count):
        for _ in range(count):
            p, d, j = queue.pop(0)
            for ahead in (True, False):
                ring(p, ahead, d, j, True).wait_recv()
                if d < last:
                    ring(p, ahead, d + 1, j, False).start()
            if p == 0 and d == last - 1:
                launch(1, j)
            if d == last:
                product(p, j)

    def shifted(values, amount):
        both = jnp.concatenate([values, jnp.zeros_like(values)], axis=1)
        for bit in range(7):
            both = jnp.where(((amount >> bit) & 1) == 1, pltpu.roll(both, 1 << bit, 1), both)
        return both

    own_wide = shifted(vectors[...], jnp.concatenate([own_shift, own_shift], axis=1))
    low_top, low_low = [v.astype(F32) for v in halves(own_wide[:, :LANE])]
    high_top, high_low = [v.astype(F32) for v in halves(own_wide[:, LANE:])]
    group = 7

    def build(step, carry):
        for k in range(group):
            tile = (step * group + k).astype(F32)
            first, second = own_tile == tile, own_tile == tile - 1.0
            at = pl.ds(pl.multiple_of((step * group + k) * LANE, LANE), LANE)
            placed_top[:, at] = jnp.where(first, low_top, jnp.where(second, high_top, 0.0)).astype(BF16)
            placed_low[:, at] = jnp.where(first, low_low, jnp.where(second, high_low, 0.0)).astype(BF16)
        return carry

    lax.fori_loop(0, tiles_dev // group, build, 0)
    placed_top[:, cols:] = jnp.zeros((per_dev, NX * part - cols), BF16)
    placed_low[:, cols:] = jnp.zeros((per_dev, NX * part - cols), BF16)
    own_copy = pltpu.make_async_copy(cut.at[cx], gathered.at[:, cx, cz], own_sem.at[0])
    own_copy.start()
    own_trade = pltpu.make_async_copy(outgoing.at[cx], traded.at[cx], own_sem.at[1])
    own_trade.start()
    own_copy.wait()

    pl.semaphore_wait(barrier, peers - 1 + 2)
    for j in range(CHUNKS):
        for k in (1, 3, 2):
            over_x(0, j, k).start()
    for k in range(1, n_row):
        over_row(packs, send_p, recv_p, k).start()
    for j in range(CHUNKS):
        for k in (1, 3, 2):
            over_x(1, j, k).start()
    for k in (1, 3, 2):
        along_x(outgoing, traded, send_x, recv_x, k).start()
    for j in range(CHUNKS):
        launch(0, j)

    def inner_step(step, total):
        at = pl.ds(pl.multiple_of(step * group * LANE, LANE), group * LANE)
        top, low = halves(eigen[:, at])
        first = mxu_nt(jnp.concatenate([top, low], axis=0), placed_top[:, at])
        return total + first[:rows] + first[rows:] + mxu_nt(top, placed_low[:, at])

    steps = tiles_dev // group
    total = lax.fori_loop(0, steps // 2, inner_step, jnp.zeros((rows, per_dev), F32))
    pump(1)
    total = lax.fori_loop(steps // 2, steps, inner_step, total)
    pump(2)

    for k in range(1, n_row):
        over_row_arrival(packs, send_p, recv_p, k).wait_recv()
    every_meta = packs[0, per_dev:]
    for r in range(1, n_row):
        every_meta = every_meta + packs[r, per_dev:]
    bp = lax.broadcasted_iota(jnp.int32, (BLOCK, BLOCK), 0)
    bq = lax.broadcasted_iota(jnp.int32, (BLOCK, BLOCK), 1)
    diag = bp == bq

    def turned(line):
        return jnp.sum(jnp.where(diag, line, 0.0), axis=1, keepdims=True)

    count = 2 * n_row * half // BLOCK
    across_tile = [every_meta[u : u + 1] for u in range(count)]
    down_tile = []
    for u in range(count):
        s, h = u // 2, u % 2
        low = jnp.concatenate(
            [packs[h * per_tile + k, s * half : (s + 1) * half] for k in range(per_tile)], axis=0
        )
        wide[u * BLOCK : (u + 1) * BLOCK] = shifted(low, turned(every_meta[u + 4 : u + 5]).astype(jnp.int32))
        down = turned(across_tile[u])
        down_tile.append(down)
        tile_of[u * BLOCK : (u + 1) * BLOCK] = jnp.broadcast_to(down, (BLOCK, LANE))
        if u == 1:
            pump(1)

    def of_row(ref, r):
        return jnp.concatenate(
            [ref[pl.ds(pl.multiple_of(s * n_row * half + r * half, half), half)] for s in range(2)], axis=0
        )

    prev_row = jnp.maximum(row - 1, 0)
    prev_tile = of_row(tile_of, prev_row) - (row * tiles_dev).astype(F32)
    prev_high = jnp.where(prev_tile == -1.0, of_row(wide, prev_row)[:, LANE:], 0.0)
    behind = dot3_nt(eigen[:, :LANE], prev_high)
    inners[row] = jnp.concatenate([total, behind], axis=1)
    for k in range(1, n_row):
        over_row(inners, send_w, recv_w, k).start()
    pump(2)

    keep = (((bp // refl) == (bq // refl)) & (bp > bq)) | (((bp // refl) != (bq // refl)) & (bp < bq))
    strict, across = {}, []
    for u in range(count):
        mine = wide[u * BLOCK : (u + 1) * BLOCK]
        rest = wide[u * BLOCK :]
        level = dot3_nt(mine, rest)
        after = dot3_nt(mine[:, LANE:], rest[:, :LANE])
        before = dot3_nt(mine[:, :LANE], rest[:, LANE:])
        for t in range(u, count):
            cols_at = slice((t - u) * BLOCK, (t - u + 1) * BLOCK)
            gap = across_tile[t] - down_tile[u]
            tile = jnp.where(
                gap == 0.0,
                level[:, cols_at],
                jnp.where(gap == 1.0, after[:, cols_at], jnp.where(gap == -1.0, before[:, cols_at], 0.0)),
            )
            if t == u:
                picked = jnp.where(diag, tile, 0.0)
                scale = 2.0 / jnp.sum(picked, axis=1, keepdims=True)
                across.append(2.0 / jnp.sum(picked, axis=0, keepdims=True))
                tile = jnp.where(keep, tile, 0.0)
            strict[u, t] = tile * scale
        if u in (0, 2):
            pump(1)
    inverse = tile_inverses([strict[t, t] for t in range(count)], lambda size: pump(1) if size == 8 else None)
    pump(2)

    for k in range(1, n_row):
        over_row_arrival(inners, send_w, recv_w, k).wait_recv()
    lane = lax.broadcasted_iota(jnp.int32, (rows, LANE), 1) // half
    right = [jnp.zeros((rows, LANE), F32) for _ in range(count)]
    for r in range(n_row):
        values = inners[r]
        for s in range(2):
            u = s * 2 + r // per_tile
            moved = pltpu.roll(values, (half * (r % per_tile) - half * s) % LANE, 1)
            right[u] = right[u] + jnp.where(lane == r % per_tile, moved, 0.0)
            if r > 0:
                u = s * 2 + (r - 1) // per_tile
                moved = pltpu.roll(values, (half * ((r - 1) % per_tile) - per_dev - half * s) % LANE, 1)
                right[u] = right[u] + jnp.where(lane == (r - 1) % per_tile, moved, 0.0)
    found = []
    for t in range(count):
        value = right[t]
        for u in range(t):
            value = value - dot3(found[u], strict[u, t])
        found.append(dot3(value, inverse[t]))
    solved = [found[t] * across[t] for t in range(count)]

    def coeffs_of(r):
        result = jnp.zeros((rows, LANE), F32)
        for s in range(2):
            tile = jnp.where(r // per_tile == 0, solved[s * 2], solved[s * 2 + 1])
            moved = pltpu.roll(tile, (LANE - half * (r % per_tile) + half * s) % LANE, 1)
            result = jnp.where(lane == s, moved, result)
        return result[:, :per_dev]

    own_coeffs, prev_coeffs = coeffs_of(row), coeffs_of(prev_row)
    shared[cx] = jnp.concatenate([own_coeffs, prev_coeffs], axis=1)
    for k in (1, 3, 2):
        along_x(shared, shared, send_c, recv_c, k).start()
    pump(2)

    def both_halves(values):
        top, low = halves(values)
        return top, jnp.concatenate([top, low], axis=0)

    def changed(top, both, at):
        size = top.shape[0]
        first = mxu(both, placed_top[:, at])
        return first[:size] + first[size:] + mxu(top, placed_low[:, at])

    coeffs_top, coeffs_both = both_halves(own_coeffs)
    first_change = dot3(prev_coeffs, prev_high)

    def keep_step(step, carry):
        at = pl.ds(pl.multiple_of(step * group * LANE, LANE), group * LANE)
        kept[:, at] = eigen[:, at] - changed(coeffs_top, coeffs_both, at)
        return carry

    lax.fori_loop(0, steps // 4, keep_step, 0)
    pump(1)
    kept[:, :LANE] = kept[:, :LANE] - first_change

    own_trade.wait()
    for k in (1, 3, 2):
        along_x_arrival(outgoing, traded, send_x, recv_x, k).wait_recv()
    for k in (1, 3, 2):
        along_x_arrival(shared, shared, send_c, recv_c, k).wait_recv()
    all_shared = shared[...].reshape(every, LANE)
    slice_top, slice_both = both_halves(all_shared[:, :per_dev])
    begin_change = jnp.where(cx == 0, 1.0, 0.0).astype(F32) * dot3(all_shared[:, per_dev:], prev_high)
    for j in range(CHUNKS):
        at = slice(j * chunk, (j + 1) * chunk)
        source = pl.ds(pl.multiple_of(cx * part + j * chunk, LANE), chunk)
        value = traded[:, :, at].reshape(every, chunk).astype(F32) - changed(slice_top, slice_both, source)
        if j == 0:
            value = jnp.concatenate([value[:, :LANE] - begin_change, value[:, LANE:]], axis=1)
        held[:, at] = value
        rounded[:, at] = value.astype(BF16)
        if j == 1:
            pump(1)
    pump(CHUNKS)

    piece = work.shape[2]
    per_block = BLOCK // piece

    def piece_of(place):
        return jnp.minimum((place * 5 + 7) // 8, owners - 1)

    def owns(place):
        return (((place * 5 + 7) // 8) * 8) // 5 == place

    def put(p):
        blocks = (
            acc[every : every + BLOCK, :BLOCK],
            acc[every + BLOCK :, :BLOCK],
            acc[every + BLOCK :, BLOCK:],
            acc[:every, :BLOCK],
            acc[:every, BLOCK:],
        )
        for place, block in enumerate(blocks):
            value = block.astype(BF16)
            for k in range(per_block):
                work[p, place * per_block + k] = value[k * piece : (k + 1) * piece]

    def scatter(p, k):
        target = (me + k) % peers
        return pltpu.make_async_remote_copy(
            src_ref=work.at[p, piece_of(target)],
            dst_ref=slots.at[p, k - 1],
            send_sem=send_rs.at[p, k - 1],
            recv_sem=recv_rs.at[p, k - 1],
            device_id=device(target),
            device_id_type=mesh,
        )

    def gather(p, k, arriving):
        place = piece_of((me + peers - k) % peers if arriving else me)
        return pltpu.make_async_remote_copy(
            src_ref=whole.at[p, place],
            dst_ref=whole.at[p, place],
            send_sem=send_ag.at[p, k - 1],
            recv_sem=recv_ag.at[p, k - 1],
            device_id=device((me + k) % peers),
            device_id_type=mesh,
        )

    def start_reduce(p):
        put(p)
        for k in range(1, peers):
            pl.when(owns((me + k) % peers))(scatter(p, k).start)

    def finish_reduce(p):
        @pl.when(owns(me))
        def _():
            value = work[p, piece_of(me)].astype(F32)
            for k in range(1, peers):
                scatter(p, k).wait_recv()
                value = value + slots[p, k - 1].astype(F32)
            whole[p, piece_of(me)] = value.astype(BF16)
            for k in range(1, peers):
                gather(p, k, False).start()

    def finish_gather(p):
        for k in range(1, peers):
            pl.when(owns((me + peers - k) % peers))(gather(p, k, True).wait_recv)

    def panel_solve(p, between):
        def got(place):
            return jnp.concatenate(
                [whole[p, place * per_block + k].astype(F32) for k in range(per_block)], axis=0
            )

        gram = {(0, 0): got(0), (1, 0): got(1), (1, 1): got(2)}
        picked = [jnp.where(diag, gram[t, t], 0.0) for t in range(2)]
        down = [2.0 / jnp.sum(v, axis=1, keepdims=True) for v in picked]
        beside = [2.0 / jnp.sum(v, axis=0, keepdims=True) for v in picked]
        below = [jnp.where(bp > bq, gram[t, t] * down[t], 0.0) for t in range(2)]
        inverses = tile_inverses(below, between)
        second = dot3(got(4), inverses[1])
        first = dot3(got(3) - dot3(second, gram[1, 0] * down[1]), inverses[0])
        return jnp.concatenate([(first * beside[0]).astype(BF16), (second * beside[1]).astype(BF16)], axis=1)

    start_reduce(0)
    pump(1)
    lax.fori_loop(steps // 4, steps // 2, keep_step, 0)
    pump(1)
    lax.fori_loop(steps // 2, 3 * steps // 4, keep_step, 0)
    pump(1)
    finish_reduce(0)
    pump(1)
    lax.fori_loop(3 * steps // 4, steps, keep_step, 0)
    pump(3)
    finish_gather(0)
    coeffs = panel_solve(0, lambda size: pump(1) if size in (4, 32) else None)
    pump(1)
    for j in range(CHUNKS):
        at = slice(j * chunk, (j + 1) * chunk)
        value = mxu(coeffs, reflect(0, at))
        delta[:, at] = value
        rounded[:, at] = (held[:, at] - value).astype(BF16)
        if j in (1, 3):
            pump(1)
    pump(len(queue))
    start_reduce(1)
    finish_reduce(1)
    finish_gather(1)
    coeffs = panel_solve(1, None)

    def back(j, k, arriving):
        source = (cx + NX - k) % NX if arriving else (cx + k) % NX
        at = pl.ds(j * chunk, chunk)
        return pltpu.make_async_remote_copy(
            src_ref=change.at[source, :, at],
            dst_ref=home.at[source if arriving else cx, :, at],
            send_sem=send_h.at[j, k - 1],
            recv_sem=recv_h.at[j, k - 1],
            device_id={"cx": source},
            device_id_type=mesh,
        )

    for j in range(CHUNKS):
        at = slice(j * chunk, (j + 1) * chunk)
        value = (delta[:, at] + mxu(coeffs, reflect(1, at))).astype(BF16)
        for x in range(NX):
            change[x, :, at] = value[x * rows : (x + 1) * rows]
        for k in (2, 1, 3):
            back(j, k, False).start()
    keep_home = pltpu.make_async_copy(change.at[cx], home.at[cx], own_sem.at[0])
    keep_home.start()

    for k in range(1, n_row):
        over_row(packs, send_p, recv_p, k).wait_send()
        over_row(inners, send_w, recv_w, k).wait_send()
    for k in range(1, NX):
        along_x(outgoing, traded, send_x, recv_x, k).wait_send()
        along_x(shared, shared, send_c, recv_c, k).wait_send()
        for p in range(n_panel):
            for j in range(CHUNKS):
                over_x(p, j, k).wait_send()
    for p in range(n_panel):
        for d in range(last + 1):
            for j in range(CHUNKS):
                for ahead in (True, False):
                    ring(p, ahead, d, j, False).wait_send()
        for k in range(1, peers):
            pl.when(owns((me + k) % peers))(scatter(p, k).wait_send)

        @pl.when(owns(me))
        def _():
            for k in range(1, peers):
                gather(p, k, False).wait_send()

    keep_home.wait()
    for j in range(CHUNKS):
        for k in range(1, NX):
            back(j, k, False).wait_send()
            back(j, k, True).wait_recv()


def fused_step(offs, vectors, eigen, panels, n_row):
    rows, cols = eigen.shape
    n_panel, refl_dev, _ = panels.shape
    part = -(-(cols // LANE) // NX) * LANE
    per_dev, band = vectors.shape
    peers = n_row * NX
    owners, piece = 20, 32
    every = NX * rows
    dma = pltpu.SemaphoreType.DMA
    vmem = pl.BlockSpec(memory_space=pltpu.VMEM)
    hbm = pl.BlockSpec(memory_space=pltpu.HBM)
    units = n_panel * (NZ // 2) * CHUNKS
    trade = (NX, rows, part)
    return pl.pallas_call(
        fused_kernel,
        out_shape=[jax.ShapeDtypeStruct((rows, cols), F32), jax.ShapeDtypeStruct(trade, BF16)],
        in_specs=[hbm] * 4,
        out_specs=[vmem] * 2,
        scratch_shapes=[
            pltpu.SMEM(offs.shape, jnp.int32),
            pltpu.VMEM((per_dev, band), F32),
            pltpu.VMEM((rows, cols), F32),
            pltpu.VMEM((NX, n_panel, refl_dev, part), BF16),
            pltpu.VMEM((n_panel, NX, NZ, refl_dev, part), BF16),
            pltpu.VMEM((n_row, per_dev + 8, band), F32),
            pltpu.VMEM((n_row, rows, LANE), F32),
            pltpu.VMEM((n_row * per_dev, 2 * LANE), F32),
            pltpu.VMEM((n_row * per_dev, LANE), F32),
            pltpu.VMEM((per_dev, NX * part), BF16),
            pltpu.VMEM((per_dev, NX * part), BF16),
            pltpu.VMEM(trade, BF16),
            pltpu.VMEM(trade, BF16),
            pltpu.VMEM((NX, rows, LANE), F32),
            pltpu.VMEM((every, part), F32),
            pltpu.VMEM((every, part), BF16),
            pltpu.VMEM((every, part), F32),
            pltpu.VMEM((every + 2 * BLOCK, 2 * BLOCK), F32),
            pltpu.VMEM((n_panel, owners, piece, BLOCK), BF16),
            pltpu.VMEM((n_panel, peers - 1, piece, BLOCK), BF16),
            pltpu.VMEM((n_panel, owners, piece, BLOCK), BF16),
            pltpu.VMEM(trade, BF16),
            dma((3 + NX,)),
            dma((n_panel * CHUNKS, NX - 1)),
            dma((n_panel * CHUNKS, NX - 1)),
            dma((n_row - 1,)),
            dma((n_row - 1,)),
            dma((n_row - 1,)),
            dma((n_row - 1,)),
            dma((units,)),
            dma((units,)),
            dma((units,)),
            dma((units,)),
            dma((NX - 1,)),
            dma((NX - 1,)),
            dma((NX - 1,)),
            dma((NX - 1,)),
            dma((n_panel, peers - 1)),
            dma((n_panel, peers - 1)),
            dma((n_panel, peers - 1)),
            dma((n_panel, peers - 1)),
            dma((CHUNKS, NX - 1)),
            dma((CHUNKS, NX - 1)),
            dma((2,)),
        ],
        compiler_params=pltpu.CompilerParams(
            collective_id=0, has_side_effects=True, vmem_limit_bytes=40 * 1024 * 1024
        ),
        cost_estimate=pl.CostEstimate(flops=20_000_000_000, bytes_accessed=8_000_000, transcendentals=0),
    )(offs, vectors, eigen, panels)


def local(eigvecs, span_vectors, span_offsets, panels):
    rows, cols = eigvecs.shape
    band = span_vectors.shape[3]
    n_row = lax.psum(1, "row")
    eigen, home = fused_step(span_offsets, span_vectors.reshape(-1, band), eigvecs, panels, n_row)
    home = home.transpose(1, 0, 2).reshape(rows, -1)[:, :cols]
    return eigen - home.astype(F32)


def solution(mesh):
    finer = Mesh(mesh.devices.reshape(mesh.shape["row"], NX, NZ), ("row", "cx", "cz"))
    col = ("cx", "cz")
    placed = (P(col, "row"), P(None, "row", None, None), P(None, "row"), P(None, col, "row"))
    return jax.shard_map(local, mesh=finer, in_specs=placed, out_specs=P(col, "row"), check_vma=False)
```

```python
import functools

import jax
import jax.numpy as jnp
from jax import lax
from jax.experimental import pallas as pl
from jax.experimental.pallas import tpu as pltpu
from jax.sharding import Mesh
from jax.sharding import PartitionSpec as P

LANE = 128
BLOCK = 128
NX = 4
NZ = 8
CHUNKS = 5
F32 = jnp.float32
BF16 = jnp.bfloat16
NT = (((1,), (1,)), ((), ()))
NN = (((1,), (0,)), ((), ()))


def halves(a):
    top = a.astype(BF16)
    return top, (a - top.astype(F32)).astype(BF16)


def dot3(a, b):
    a_top, a_low = halves(a)
    b_top, b_low = halves(b)
    d = functools.partial(lax.dot_general, dimension_numbers=NN, preferred_element_type=F32)
    return d(a_top, b_top) + (d(a_top, b_low) + d(a_low, b_top))


def dot3_nt(a, b):
    a_top, a_low = halves(a)
    b_top, b_low = halves(b)
    d = functools.partial(lax.dot_general, dimension_numbers=NT, preferred_element_type=F32)
    return d(a_top, b_top) + (d(a_top, b_low) + d(a_low, b_top))


def tile_inverses(tiles, between=None):
    bp = lax.broadcasted_iota(jnp.int32, (BLOCK, BLOCK), 0)
    bq = lax.broadcasted_iota(jnp.int32, (BLOCK, BLOCK), 1)
    eye = (bp == bq).astype(F32)
    inverse = [eye - jnp.where(bp // 2 == bq // 2, tile, 0.0) for tile in tiles]
    size = 2
    while size < BLOCK:
        joined = (bp // (2 * size) == bq // (2 * size)) & (bp // size != bq // size)
        left = [dot3(inv, jnp.where(joined, tile, 0.0)) for inv, tile in zip(inverse, tiles)]
        inverse = [inv - dot3(lhs, inv) for inv, lhs in zip(inverse, left)]
        if between is not None:
            between(size)
        size *= 2
    return inverse


def fused_kernel(offs_hbm, vectors_hbm, eigen_hbm, panels_hbm, kept_hbm, home, kept, offs, vectors, eigen, cut, gathered, packs,
                 inners, wide, tile_of, placed_top, placed_low, outgoing, traded, shared, held, rounded, delta, acc,
                 work, slots, whole, change, load, send_a, recv_a, send_p, recv_p, send_w, recv_w, send_f, recv_f,
                 send_x, recv_x, send_c, recv_c, send_rs, recv_rs, send_ag, recv_ag, send_h, recv_h,
                 own_sem):
    row, cx, cz = lax.axis_index("row"), lax.axis_index("cx"), lax.axis_index("cz")
    n_row = lax.axis_size("row")
    rows, cols = eigen.shape
    every = NX * rows
    tiles_dev = cols // LANE
    part = cut.shape[3]
    chunk = part // CHUNKS
    n_panel = cut.shape[1]
    per_dev = vectors.shape[0]
    half = per_dev // 2
    refl = 4
    spans = half // refl
    per_tile = BLOCK // half
    peers = n_row * NX
    me = row * NX + cx
    owners = work.shape[1]
    mesh = pl.DeviceIdType.MESH
    mxu_nt = functools.partial(lax.dot_general, dimension_numbers=NT, preferred_element_type=F32)
    mxu = functools.partial(lax.dot_general, dimension_numbers=NN, preferred_element_type=F32)

    def device(place):
        return {"row": place // NX, "cx": place % NX}

    loads = [
        pltpu.make_async_copy(offs_hbm, offs, load.at[0]),
        pltpu.make_async_copy(vectors_hbm, vectors, load.at[1]),
    ]
    eigen_load = pltpu.make_async_copy(eigen_hbm, eigen, load.at[2])
    for x in range(NX):
        size = min(part, cols - x * part)
        loads.append(
            pltpu.make_async_copy(
                panels_hbm.at[:, :, pl.ds(x * part, size)], cut.at[x, :, :, pl.ds(0, size)], load.at[3 + x]
            )
        )
        if size < part:
            cut[x, :, :, size:] = jnp.zeros((n_panel, cut.shape[2], part - size), BF16)
    for copy in loads:
        copy.start()
    eigen_load.start()
    barrier = pltpu.get_barrier_semaphore()
    for k in (1, NZ - 1):
        pl.semaphore_signal(barrier, inc=1, device_id={"cz": (cz + k) % NZ}, device_id_type=mesh)
    for k in range(1, peers):
        pl.semaphore_signal(barrier, inc=1, device_id=device((me + k) % peers), device_id_type=mesh)
    for copy in loads:
        copy.wait()

    lane8 = lax.broadcasted_iota(jnp.int32, (8, LANE), 1)
    line8 = lax.broadcasted_iota(jnp.int32, (8, LANE), 0)
    line64 = lax.broadcasted_iota(jnp.int32, (per_dev, LANE), 0) // refl
    meta = jnp.zeros((8, LANE), F32)
    own_tile = jnp.zeros((per_dev, LANE), F32)
    own_shift = jnp.zeros((per_dev, LANE), jnp.int32)
    for s in range(2):
        for b in range(spans):
            at = offs[s, b]
            tile_at = at >> 7
            shift_at = at & 127
            place = (row % per_tile) * half + b * refl
            mine = (lane8 >= place) & (lane8 < place + refl)
            line = s * 2 + row // per_tile
            meta = jnp.where(mine & (line8 == line), (tile_at + row * tiles_dev).astype(F32), meta)
            meta = jnp.where(mine & (line8 == line + 4), shift_at.astype(F32), meta)
            own_tile = jnp.where(line64 == s * spans + b, tile_at.astype(F32), own_tile)
            own_shift = jnp.where(line64 == s * spans + b, shift_at, own_shift)
    packs[row, :per_dev] = vectors[...]
    packs[row, per_dev:] = meta
    def sized(ref, send, recv):
        return pltpu.make_async_remote_copy(
            src_ref=ref, dst_ref=ref, send_sem=send, recv_sem=recv, device_id={"cx": (cx + 1) % NX}, device_id_type=mesh
        )

    def over_x(p, j, k):
        at = pl.ds(j * chunk, chunk)
        return pltpu.make_async_remote_copy(
            src_ref=cut.at[(cx + k) % NX, p, :, at],
            dst_ref=gathered.at[p, cx, cz, :, at],
            send_sem=send_a.at[0],
            recv_sem=recv_a.at[p * CHUNKS + j],
            device_id={"cx": (cx + k) % NX},
            device_id_type=mesh,
        )

    def over_row(ref, sends, recvs, k):
        return pltpu.make_async_remote_copy(
            src_ref=ref.at[row],
            dst_ref=ref.at[row],
            send_sem=sends.at[0],
            recv_sem=recvs.at[0],
            device_id={"row": (row + k) % n_row},
            device_id_type=mesh,
        )

    def along_x(source_ref, target_ref, sends, recvs, k):
        target = (cx + k) % NX
        return pltpu.make_async_remote_copy(
            src_ref=source_ref.at[target] if source_ref is not target_ref else source_ref.at[cx],
            dst_ref=target_ref.at[cx],
            send_sem=sends.at[0],
            recv_sem=recvs.at[0],
            device_id={"cx": target},
            device_id_type=mesh,
        )

    last = NZ // 2 - 1

    def ring(p, ahead, d, j):
        step = 1 if ahead else NZ - 1
        at = pl.ds(j * chunk, chunk)
        share = slice(None) if d < last else (pl.ds(0, NX // 2) if ahead else pl.ds(NX // 2, NX // 2))
        place = gathered.at[p, share, (cz + NZ - d * step) % NZ if ahead else (cz + d) % NZ, :, at]
        return pltpu.make_async_remote_copy(
            src_ref=place,
            dst_ref=place,
            send_sem=send_f.at[0],
            recv_sem=recv_f.at[((last + 1) * p + d) * CHUNKS + j],
            device_id={"cz": (cz + step) % NZ},
            device_id_type=mesh,
        )

    def launch(p, j):
        at = pl.ds(j * chunk, chunk)
        sized(gathered.at[p, pl.ds(0, NX - 1), cz, :, at], send_a.at[0], recv_a.at[p * CHUNKS + j]).wait_recv()
        for ahead in (True, False):
            ring(p, ahead, 0, j).start()

    def reflect(p, at):
        return gathered[p, :, :, :, at].reshape(-1, chunk)

    def product(p, j):
        at = slice(j * chunk, (j + 1) * chunk)
        mine = reflect(p, at)
        value = mxu_nt(jnp.concatenate([rounded[:, at], mine], axis=0), mine)
        acc[...] = value if j == 0 else acc[...] + value

    queue = [(p, d, j) for p in range(n_panel) for d in range(last + 1) for j in range(CHUNKS)]

    def pump(count):
        for _ in range(count):
            p, d, j = queue.pop(0)
            at = pl.ds(j * chunk, chunk)
            both = gathered.at[p, :, pl.ds(0, 2 if d < last else 1), :, at]
            sized(both, send_f.at[0], recv_f.at[((last + 1) * p + d) * CHUNKS + j]).wait_recv()
            if d < last:
                for ahead in (True, False):
                    ring(p, ahead, d + 1, j).start()
            if p == 0 and d == last - 1:
                launch(1, j)
            if d == last:
                product(p, j)

    def shifted(values, amount):
        both = jnp.concatenate([values, jnp.zeros_like(values)], axis=1)
        for bit in range(7):
            both = jnp.where(((amount >> bit) & 1) == 1, pltpu.roll(both, 1 << bit, 1), both)
        return both

    own_wide = shifted(vectors[...], jnp.concatenate([own_shift, own_shift], axis=1))
    low_top, low_low = [v.astype(F32) for v in halves(own_wide[:, :LANE])]
    high_top, high_low = [v.astype(F32) for v in halves(own_wide[:, LANE:])]
    group = 7

    def build(step, carry):
        for k in range(group):
            tile = (step * group + k).astype(F32)
            first, second = own_tile == tile, own_tile == tile - 1.0
            at = pl.ds(pl.multiple_of((step * group + k) * LANE, LANE), LANE)
            placed_top[:, at] = jnp.where(first, low_top, jnp.where(second, high_top, 0.0)).astype(BF16)
            placed_low[:, at] = jnp.where(first, low_low, jnp.where(second, high_low, 0.0)).astype(BF16)
        return carry

    lax.fori_loop(0, tiles_dev // group, build, 0)
    placed_top[:, cols:] = jnp.zeros((per_dev, NX * part - cols), BF16)
    placed_low[:, cols:] = jnp.zeros((per_dev, NX * part - cols), BF16)
    own_copy = pltpu.make_async_copy(cut.at[cx], gathered.at[:, cx, cz], own_sem.at[0])
    own_copy.start()
    own_copy.wait()

    pl.semaphore_wait(barrier, peers - 1 + 2)
    for j in range(CHUNKS):
        for k in (1, 3, 2):
            over_x(0, j, k).start()
    for k in range(1, n_row):
        over_row(packs, send_p, recv_p, k).start()
    eigen_load.wait()
    for x in range(NX):
        size = min(part, cols - x * part)
        outgoing[x, :, :size] = eigen[:, x * part : x * part + size].astype(BF16)
        if size < part:
            outgoing[x, :, size:] = jnp.zeros((rows, part - size), BF16)

    own_trade = pltpu.make_async_copy(outgoing.at[cx], traded.at[cx], own_sem.at[1])
    own_trade.start()
    for k in (1, 3, 2):
        along_x(outgoing, traded, send_x, recv_x, k).start()
    for j in range(CHUNKS):
        launch(0, j)
    for j in range(CHUNKS):
        for k in (1, 3, 2):
            over_x(1, j, k).start()

    def inner_step(step, total):
        at = pl.ds(pl.multiple_of(step * group * LANE, LANE), group * LANE)
        top, low = halves(eigen[:, at])
        first = mxu_nt(jnp.concatenate([top, low], axis=0), placed_top[:, at])
        return total + first[:rows] + first[rows:] + mxu_nt(top, placed_low[:, at])

    steps = tiles_dev // group
    total = lax.fori_loop(0, steps // 2, inner_step, jnp.zeros((rows, per_dev), F32))
    pump(1)
    total = lax.fori_loop(steps // 2, steps, inner_step, total)
    pump(3)

    sized(packs.at[pl.ds(0, n_row - 1)], send_p.at[0], recv_p.at[0]).wait_recv()
    every_meta = packs[0, per_dev:]
    for r in range(1, n_row):
        every_meta = every_meta + packs[r, per_dev:]
    bp = lax.broadcasted_iota(jnp.int32, (BLOCK, BLOCK), 0)
    bq = lax.broadcasted_iota(jnp.int32, (BLOCK, BLOCK), 1)
    diag = bp == bq

    def turned(line):
        return jnp.sum(jnp.where(diag, line, 0.0), axis=1, keepdims=True)

    count = 2 * n_row * half // BLOCK
    across_tile = [every_meta[u : u + 1] for u in range(count)]
    down_tile = []
    for u in range(count):
        s, h = u // 2, u % 2
        low = jnp.concatenate(
            [packs[h * per_tile + k, s * half : (s + 1) * half] for k in range(per_tile)], axis=0
        )
        wide[u * BLOCK : (u + 1) * BLOCK] = shifted(low, turned(every_meta[u + 4 : u + 5]).astype(jnp.int32))
        down = turned(across_tile[u])
        down_tile.append(down)
        tile_of[u * BLOCK : (u + 1) * BLOCK] = jnp.broadcast_to(down, (BLOCK, LANE))
        if u == 1:
            pump(1)

    def of_row(ref, r):
        return jnp.concatenate(
            [ref[pl.ds(pl.multiple_of(s * n_row * half + r * half, half), half)] for s in range(2)], axis=0
        )

    prev_row = jnp.maximum(row - 1, 0)
    prev_tile = of_row(tile_of, prev_row) - (row * tiles_dev).astype(F32)
    prev_high = jnp.where(prev_tile == -1.0, of_row(wide, prev_row)[:, LANE:], 0.0)
    behind = dot3_nt(eigen[:, :LANE], prev_high)
    inners[row] = jnp.concatenate([total, behind], axis=1)
    for k in range(1, n_row):
        over_row(inners, send_w, recv_w, k).start()
    pump(2)

    keep = (((bp // refl) == (bq // refl)) & (bp > bq)) | (((bp // refl) != (bq // refl)) & (bp < bq))
    strict, across = {}, []
    for u in range(count):
        mine = wide[u * BLOCK : (u + 1) * BLOCK]
        rest = wide[u * BLOCK :]
        level = dot3_nt(mine, rest)
        after = dot3_nt(mine[:, LANE:], rest[:, :LANE])
        before = dot3_nt(mine[:, :LANE], rest[:, LANE:])
        for t in range(u, count):
            cols_at = slice((t - u) * BLOCK, (t - u + 1) * BLOCK)
            gap = across_tile[t] - down_tile[u]
            tile = jnp.where(
                gap == 0.0,
                level[:, cols_at],
                jnp.where(gap == 1.0, after[:, cols_at], jnp.where(gap == -1.0, before[:, cols_at], 0.0)),
            )
            if t == u:
                picked = jnp.where(diag, tile, 0.0)
                scale = 2.0 / jnp.sum(picked, axis=1, keepdims=True)
                across.append(2.0 / jnp.sum(picked, axis=0, keepdims=True))
                tile = jnp.where(keep, tile, 0.0)
            strict[u, t] = tile * scale
        if u in (0, 2):
            pump(1)
    inverse = tile_inverses([strict[t, t] for t in range(count)], lambda size: pump(1) if size == 8 else None)
    pump(2)

    sized(inners.at[pl.ds(0, n_row - 1)], send_w.at[0], recv_w.at[0]).wait_recv()
    lane = lax.broadcasted_iota(jnp.int32, (rows, LANE), 1) // half
    right = [jnp.zeros((rows, LANE), F32) for _ in range(count)]
    for r in range(n_row):
        values = inners[r]
        for s in range(2):
            u = s * 2 + r // per_tile
            moved = pltpu.roll(values, (half * (r % per_tile) - half * s) % LANE, 1)
            right[u] = right[u] + jnp.where(lane == r % per_tile, moved, 0.0)
            if r > 0:
                u = s * 2 + (r - 1) // per_tile
                moved = pltpu.roll(values, (half * ((r - 1) % per_tile) - per_dev - half * s) % LANE, 1)
                right[u] = right[u] + jnp.where(lane == (r - 1) % per_tile, moved, 0.0)
    found = []
    for t in range(count):
        value = right[t]
        for u in range(t):
            value = value - dot3(found[u], strict[u, t])
        found.append(dot3(value, inverse[t]))
    solved = [found[t] * across[t] for t in range(count)]

    def coeffs_of(r):
        result = jnp.zeros((rows, LANE), F32)
        for s in range(2):
            tile = jnp.where(r // per_tile == 0, solved[s * 2], solved[s * 2 + 1])
            moved = pltpu.roll(tile, (LANE - half * (r % per_tile) + half * s) % LANE, 1)
            result = jnp.where(lane == s, moved, result)
        return result[:, :per_dev]

    own_coeffs, prev_coeffs = coeffs_of(row), coeffs_of(prev_row)
    shared[cx] = jnp.concatenate([own_coeffs, prev_coeffs], axis=1)
    for k in (1, 3, 2):
        along_x(shared, shared, send_c, recv_c, k).start()
    pump(1)

    def both_halves(values):
        top, low = halves(values)
        return top, jnp.concatenate([top, low], axis=0)

    def changed(top, both, at):
        size = top.shape[0]
        first = mxu(both, placed_top[:, at])
        return first[:size] + first[size:] + mxu(top, placed_low[:, at])

    coeffs_top, coeffs_both = both_halves(own_coeffs)
    first_change = dot3(prev_coeffs, prev_high)

    def keep_step(step, carry):
        at = pl.ds(pl.multiple_of(step * group * LANE, LANE), group * LANE)
        kept[:, at] = eigen[:, at] - changed(coeffs_top, coeffs_both, at)
        return carry

    lax.fori_loop(0, steps // 4, keep_step, 0)
    pump(1)
    kept[:, :LANE] = kept[:, :LANE] - first_change

    own_trade.wait()
    sized(traded.at[pl.ds(0, NX - 1)], send_x.at[0], recv_x.at[0]).wait_recv()
    sized(shared.at[pl.ds(0, NX - 1)], send_c.at[0], recv_c.at[0]).wait_recv()
    all_shared = shared[...].reshape(every, LANE)
    slice_top, slice_both = both_halves(all_shared[:, :per_dev])
    begin_change = jnp.where(cx == 0, 1.0, 0.0).astype(F32) * dot3(all_shared[:, per_dev:], prev_high)
    for j in range(CHUNKS):
        at = slice(j * chunk, (j + 1) * chunk)
        source = pl.ds(pl.multiple_of(cx * part + j * chunk, LANE), chunk)
        value = traded[:, :, at].reshape(every, chunk).astype(F32) - changed(slice_top, slice_both, source)
        if j == 0:
            value = jnp.concatenate([value[:, :LANE] - begin_change, value[:, LANE:]], axis=1)
        held[:, at] = value
        rounded[:, at] = value.astype(BF16)
        if j == 2:
            pump(1)
    pump(CHUNKS)

    piece = work.shape[2]
    per_block = BLOCK // piece

    def piece_of(place):
        return jnp.minimum((place * 5 + 7) // 8, owners - 1)

    def owns(place):
        return (((place * 5 + 7) // 8) * 8) // 5 == place

    def put(p):
        blocks = (
            acc[every : every + BLOCK, :BLOCK],
            acc[every + BLOCK :, :BLOCK],
            acc[every + BLOCK :, BLOCK:],
            acc[:every, :BLOCK],
            acc[:every, BLOCK:],
        )
        for place, block in enumerate(blocks):
            value = block.astype(BF16)
            for k in range(per_block):
                work[p, place * per_block + k] = value[k * piece : (k + 1) * piece]

    def scatter(p, k):
        target = (me + k) % peers
        return pltpu.make_async_remote_copy(
            src_ref=work.at[p, piece_of(target)],
            dst_ref=slots.at[p, k - 1],
            send_sem=send_rs.at[p],
            recv_sem=recv_rs.at[p],
            device_id=device(target),
            device_id_type=mesh,
        )

    def gather(p, k):
        place = piece_of(me)
        return pltpu.make_async_remote_copy(
            src_ref=whole.at[p, place],
            dst_ref=whole.at[p, place],
            send_sem=send_ag.at[p],
            recv_sem=recv_ag.at[p],
            device_id=device((me + k) % peers),
            device_id_type=mesh,
        )

    def start_reduce(p):
        put(p)
        for k in range(1, peers):
            pl.when(owns((me + k) % peers))(scatter(p, k).start)

    def finish_reduce(p):
        @pl.when(owns(me))
        def _():
            sized(slots.at[p], send_rs.at[p], recv_rs.at[p]).wait_recv()
            value = work[p, piece_of(me)].astype(F32)
            for k in range(1, peers):
                value = value + slots[p, k - 1].astype(F32)
            whole[p, piece_of(me)] = value.astype(BF16)
            for k in range(1, peers):
                gather(p, k).start()

    def finish_gather(p):
        pl.when(owns(me))(sized(whole.at[p, pl.ds(0, owners - 1)], send_ag.at[p], recv_ag.at[p]).wait_recv)
        pl.when(jnp.logical_not(owns(me)))(sized(whole.at[p], send_ag.at[p], recv_ag.at[p]).wait_recv)

    def panel_solve(p, between):
        def got(place):
            return jnp.concatenate(
                [whole[p, place * per_block + k].astype(F32) for k in range(per_block)], axis=0
            )

        gram = {(0, 0): got(0), (1, 0): got(1), (1, 1): got(2)}
        picked = [jnp.where(diag, gram[t, t], 0.0) for t in range(2)]
        down = [2.0 / jnp.sum(v, axis=1, keepdims=True) for v in picked]
        beside = [2.0 / jnp.sum(v, axis=0, keepdims=True) for v in picked]
        below = [jnp.where(bp > bq, gram[t, t] * down[t], 0.0) for t in range(2)]
        inverses = tile_inverses(below, between)
        second = dot3(got(4), inverses[1])
        first = dot3(got(3) - dot3(second, gram[1, 0] * down[1]), inverses[0])
        return jnp.concatenate([(first * beside[0]).astype(BF16), (second * beside[1]).astype(BF16)], axis=1)

    start_reduce(0)
    lax.fori_loop(steps // 4, steps // 2, keep_step, 0)
    pump(2)
    lax.fori_loop(steps // 2, 3 * steps // 4, keep_step, 0)
    pump(1)
    lax.fori_loop(3 * steps // 4, steps, keep_step, 0)
    kept_copy = pltpu.make_async_copy(kept, kept_hbm, load.at[2])
    kept_copy.start()
    pump(4)
    finish_reduce(0)
    pump(5)
    finish_gather(0)
    coeffs = panel_solve(0, lambda size: pump(1) if size in (2, 8, 32) else None)
    for j in range(CHUNKS):
        at = slice(j * chunk, (j + 1) * chunk)
        value = mxu(coeffs, reflect(0, at))
        delta[:, at] = value
        rounded[:, at] = (held[:, at] - value).astype(BF16)
    pump(len(queue))
    start_reduce(1)
    finish_reduce(1)
    finish_gather(1)
    coeffs = panel_solve(1, None)

    def back(j, k):
        target = (cx + k) % NX
        return pltpu.make_async_remote_copy(
            src_ref=change.at[target, :, pl.ds(j * chunk, chunk)],
            dst_ref=home.at[:, pl.ds(pl.multiple_of(cx * part + j * chunk, LANE), chunk)],
            send_sem=send_h.at[0],
            recv_sem=recv_h.at[0],
            device_id={"cx": target},
            device_id_type=mesh,
        )

    for j in range(CHUNKS):
        at = slice(j * chunk, (j + 1) * chunk)
        value = (delta[:, at] + mxu(coeffs, reflect(1, at))).astype(BF16)
        for x in range(NX):
            change[x, :, at] = value[x * rows : (x + 1) * rows]
        for k in (2, 1, 3):
            back(j, k).start()
    keep_home = pltpu.make_async_copy(
        change.at[cx], home.at[:, pl.ds(pl.multiple_of(cx * part, LANE), part)], own_sem.at[0]
    )
    keep_home.start()

    sized(packs.at[pl.ds(0, n_row - 1)], send_p.at[0], recv_p.at[0]).wait_send()
    sized(inners.at[pl.ds(0, n_row - 1)], send_w.at[0], recv_w.at[0]).wait_send()
    sized(outgoing.at[pl.ds(0, NX - 1)], send_x.at[0], recv_x.at[0]).wait_send()
    sized(shared.at[pl.ds(0, NX - 1)], send_c.at[0], recv_c.at[0]).wait_send()
    sized(cut.at[pl.ds(0, NX - 1)], send_a.at[0], recv_a.at[0]).wait_send()
    sized(gathered.at[:, :, pl.ds(0, NZ - 1)], send_f.at[0], recv_f.at[0]).wait_send()
    for p in range(n_panel):
        less, full = work.at[p, pl.ds(0, owners - 1)], work.at[p]
        pl.when(owns(me))(sized(less, send_rs.at[p], recv_rs.at[p]).wait_send)
        pl.when(jnp.logical_not(owns(me)))(sized(full, send_rs.at[p], recv_rs.at[p]).wait_send)
        pl.when(owns(me))(sized(slots.at[p], send_ag.at[p], recv_ag.at[p]).wait_send)
    kept_copy.wait()
    keep_home.wait()
    sized(change.at[pl.ds(0, NX - 1)], send_h.at[0], recv_h.at[0]).wait_send()
    sized(home.at[:, pl.ds(0, (NX - 1) * part)], send_h.at[0], recv_h.at[0]).wait_recv()


def fused_step(offs, vectors, eigen, panels, n_row):
    rows, cols = eigen.shape
    n_panel, refl_dev, _ = panels.shape
    part = -(-(cols // LANE) // NX) * LANE
    per_dev, band = vectors.shape
    peers = n_row * NX
    owners, piece = 20, 32
    every = NX * rows
    dma = pltpu.SemaphoreType.DMA
    hbm = pl.BlockSpec(memory_space=pltpu.HBM)
    units = n_panel * (NZ // 2) * CHUNKS
    trade = (NX, rows, part)
    return pl.pallas_call(
        fused_kernel,
        out_shape=[jax.ShapeDtypeStruct((rows, cols), F32), jax.ShapeDtypeStruct((rows, NX * part), BF16)],
        in_specs=[hbm] * 4,
        out_specs=[hbm] * 2,
        scratch_shapes=[
            pltpu.VMEM((rows, cols), F32),
            pltpu.SMEM(offs.shape, jnp.int32),
            pltpu.VMEM((per_dev, band), F32),
            pltpu.VMEM((rows, cols), F32),
            pltpu.VMEM((NX, n_panel, refl_dev, part), BF16),
            pltpu.VMEM((n_panel, NX, NZ, refl_dev, part), BF16),
            pltpu.VMEM((n_row, per_dev + 8, band), F32),
            pltpu.VMEM((n_row, rows, LANE), F32),
            pltpu.VMEM((n_row * per_dev, 2 * LANE), F32),
            pltpu.VMEM((n_row * per_dev, LANE), F32),
            pltpu.VMEM((per_dev, NX * part), BF16),
            pltpu.VMEM((per_dev, NX * part), BF16),
            pltpu.VMEM(trade, BF16),
            pltpu.VMEM(trade, BF16),
            pltpu.VMEM((NX, rows, LANE), F32),
            pltpu.VMEM((every, part), F32),
            pltpu.VMEM((every, part), BF16),
            pltpu.VMEM((every, part), F32),
            pltpu.VMEM((every + 2 * BLOCK, 2 * BLOCK), F32),
            pltpu.VMEM((n_panel, owners, piece, BLOCK), BF16),
            pltpu.VMEM((n_panel, peers - 1, piece, BLOCK), BF16),
            pltpu.VMEM((n_panel, owners, piece, BLOCK), BF16),
            pltpu.VMEM(trade, BF16),
            dma((3 + NX,)),
            dma((1,)),
            dma((n_panel * CHUNKS,)),
            dma((1,)),
            dma((1,)),
            dma((1,)),
            dma((1,)),
            dma((1,)),
            dma((units,)),
            dma((1,)),
            dma((1,)),
            dma((1,)),
            dma((1,)),
            dma((n_panel,)),
            dma((n_panel,)),
            dma((n_panel,)),
            dma((n_panel,)),
            dma((1,)),
            dma((1,)),
            dma((2,)),
        ],
        compiler_params=pltpu.CompilerParams(
            collective_id=0, has_side_effects=True, vmem_limit_bytes=60 * 1024 * 1024
        ),
        cost_estimate=pl.CostEstimate(flops=20_000_000_000, bytes_accessed=8_000_000, transcendentals=0),
    )(offs, vectors, eigen, panels)


def local(eigvecs, span_vectors, span_offsets, panels):
    cols = eigvecs.shape[1]
    band = span_vectors.shape[3]
    n_row = lax.psum(1, "row")
    eigen, home = fused_step(span_offsets, span_vectors.reshape(-1, band), eigvecs, panels, n_row)
    return eigen - home[:, :cols].astype(F32)


def solution(mesh):
    finer = Mesh(mesh.devices.reshape(mesh.shape["row"], NX, NZ), ("row", "cx", "cz"))
    col = ("cx", "cz")
    placed = (P(col, "row"), P(None, "row", None, None), P(None, "row"), P(None, col, "row"))
    return jax.shard_map(local, mesh=finer, in_specs=placed, out_specs=P(col, "row"), check_vma=False)
```

```python
import functools

import jax
import jax.numpy as jnp
from jax import lax
from jax.experimental import pallas as pl
from jax.experimental.pallas import tpu as pltpu
from jax.sharding import Mesh
from jax.sharding import PartitionSpec as P

LANE = 128
BLOCK = 128
NX = 4
NZ = 8
CHUNKS = 5
F32 = jnp.float32
BF16 = jnp.bfloat16
NT = (((1,), (1,)), ((), ()))
NN = (((1,), (0,)), ((), ()))


def halves(a):
    top = a.astype(BF16)
    return top, (a - top.astype(F32)).astype(BF16)


def dot3(a, b):
    a_top, a_low = halves(a)
    b_top, b_low = halves(b)
    d = functools.partial(lax.dot_general, dimension_numbers=NN, preferred_element_type=F32)
    return d(a_top, b_top) + (d(a_top, b_low) + d(a_low, b_top))


GRAM_TILES = ((0, 0), (0, 2), (0, 3), (1, 0), (1, 1), (1, 2), (1, 3), (2, 2), (3, 2), (3, 3))


def dot3_nt(a, b):
    a_top, a_low = halves(a)
    b_top, b_low = halves(b)
    d = functools.partial(lax.dot_general, dimension_numbers=NT, preferred_element_type=F32)
    return d(a_top, b_top) + (d(a_top, b_low) + d(a_low, b_top))


def tile_inverses(tiles, between=None):
    bp = lax.broadcasted_iota(jnp.int32, (BLOCK, BLOCK), 0)
    bq = lax.broadcasted_iota(jnp.int32, (BLOCK, BLOCK), 1)
    eye = (bp == bq).astype(F32)
    inverse = [eye - jnp.where(bp // 2 == bq // 2, tile, 0.0) for tile in tiles]
    size = 2
    while size < BLOCK:
        joined = (bp // (2 * size) == bq // (2 * size)) & (bp // size != bq // size)
        left = [dot3(inv, jnp.where(joined, tile, 0.0)) for inv, tile in zip(inverse, tiles)]
        inverse = [inv - dot3(lhs, inv) for inv, lhs in zip(inverse, left)]
        if between is not None:
            between(size)
        size *= 2
    return inverse


def fused_kernel(offs_hbm, vectors_hbm, eigen_hbm, panels_hbm, kept_hbm, home, kept, offs, vectors, eigen, cut, gathered, packs,
                 inners, wide, tile_of, placed_top, placed_low, outgoing, traded, shared, rounded, acc_top, acc_low,
                 work, slots, whole, change, load, send_a, recv_a, send_p, recv_p, send_w, recv_w, send_f, recv_f,
                 send_x, recv_x, send_c, recv_c, send_rs, recv_rs, send_ag, recv_ag, send_h, recv_h,
                 own_sem):
    row, cx, cz = lax.axis_index("row"), lax.axis_index("cx"), lax.axis_index("cz")
    n_row = lax.axis_size("row")
    rows, cols = eigen.shape
    every = NX * rows
    tiles_dev = cols // LANE
    part = cut.shape[3]
    chunk = part // CHUNKS
    n_panel = cut.shape[1]
    per_dev = vectors.shape[0]
    half = per_dev // 2
    refl = 4
    spans = half // refl
    per_tile = BLOCK // half
    peers = n_row * NX
    me = row * NX + cx
    owners = work.shape[0]
    mesh = pl.DeviceIdType.MESH
    mxu_nt = functools.partial(lax.dot_general, dimension_numbers=NT, preferred_element_type=F32)
    mxu = functools.partial(lax.dot_general, dimension_numbers=NN, preferred_element_type=F32)

    def device(place):
        return {"row": place // NX, "cx": place % NX}

    loads = [
        pltpu.make_async_copy(offs_hbm, offs, load.at[0]),
        pltpu.make_async_copy(vectors_hbm, vectors, load.at[1]),
    ]
    eigen_load = pltpu.make_async_copy(eigen_hbm, eigen, load.at[2])
    for x in range(NX):
        size = min(part, cols - x * part)
        loads.append(
            pltpu.make_async_copy(
                panels_hbm.at[:, :, pl.ds(x * part, size)], cut.at[x, :, :, pl.ds(0, size)], load.at[3 + x]
            )
        )
        if size < part:
            cut[x, :, :, size:] = jnp.zeros((n_panel, cut.shape[2], part - size), BF16)
    for copy in loads:
        copy.start()
    eigen_load.start()
    barrier = pltpu.get_barrier_semaphore()
    for k in (1, NZ - 1):
        pl.semaphore_signal(barrier, inc=1, device_id={"cz": (cz + k) % NZ}, device_id_type=mesh)
    for k in range(1, peers):
        pl.semaphore_signal(barrier, inc=1, device_id=device((me + k) % peers), device_id_type=mesh)
    for copy in loads:
        copy.wait()

    lane8 = lax.broadcasted_iota(jnp.int32, (8, LANE), 1)
    line8 = lax.broadcasted_iota(jnp.int32, (8, LANE), 0)
    line64 = lax.broadcasted_iota(jnp.int32, (per_dev, LANE), 0) // refl
    meta = jnp.zeros((8, LANE), F32)
    own_tile = jnp.zeros((per_dev, LANE), F32)
    own_shift = jnp.zeros((per_dev, LANE), jnp.int32)
    for s in range(2):
        for b in range(spans):
            at = offs[s, b]
            tile_at = at >> 7
            shift_at = at & 127
            place = (row % per_tile) * half + b * refl
            mine = (lane8 >= place) & (lane8 < place + refl)
            line = s * 2 + row // per_tile
            meta = jnp.where(mine & (line8 == line), (tile_at + row * tiles_dev).astype(F32), meta)
            meta = jnp.where(mine & (line8 == line + 4), shift_at.astype(F32), meta)
            own_tile = jnp.where(line64 == s * spans + b, tile_at.astype(F32), own_tile)
            own_shift = jnp.where(line64 == s * spans + b, shift_at, own_shift)
    packs[row, :per_dev] = vectors[...]
    packs[row, per_dev:] = meta
    def sized(ref, send, recv):
        return pltpu.make_async_remote_copy(
            src_ref=ref, dst_ref=ref, send_sem=send, recv_sem=recv, device_id={"cx": (cx + 1) % NX}, device_id_type=mesh
        )

    def over_x(j, k):
        at = pl.ds(j * chunk, chunk)
        return pltpu.make_async_remote_copy(
            src_ref=cut.at[(cx + k) % NX, :, :, at],
            dst_ref=gathered.at[:, cx, cz, :, at],
            send_sem=send_a.at[0],
            recv_sem=recv_a.at[j],
            device_id={"cx": (cx + k) % NX},
            device_id_type=mesh,
        )

    def over_row(ref, sends, recvs, k):
        return pltpu.make_async_remote_copy(
            src_ref=ref.at[row],
            dst_ref=ref.at[row],
            send_sem=sends.at[0],
            recv_sem=recvs.at[0],
            device_id={"row": (row + k) % n_row},
            device_id_type=mesh,
        )

    def along_x(source_ref, target_ref, sends, recvs, k):
        target = (cx + k) % NX
        return pltpu.make_async_remote_copy(
            src_ref=source_ref.at[target] if source_ref is not target_ref else source_ref.at[cx],
            dst_ref=target_ref.at[cx],
            send_sem=sends.at[0],
            recv_sem=recvs.at[0],
            device_id={"cx": target},
            device_id_type=mesh,
        )

    last = NZ // 2 - 1

    def ring(ahead, d, j):
        step = 1 if ahead else NZ - 1
        at = pl.ds(j * chunk, chunk)
        panel = slice(None) if d < last else (pl.ds(0, 1) if ahead else pl.ds(1, 1))
        place = gathered.at[panel, :, (cz + NZ - d * step) % NZ if ahead else (cz + d) % NZ, :, at]
        return pltpu.make_async_remote_copy(
            src_ref=place,
            dst_ref=place,
            send_sem=send_f.at[0],
            recv_sem=recv_f.at[d * CHUNKS + j],
            device_id={"cz": (cz + step) % NZ},
            device_id_type=mesh,
        )

    def launch(j):
        at = pl.ds(j * chunk, chunk)
        sized(gathered.at[:, pl.ds(0, NX - 1), cz, :, at], send_a.at[0], recv_a.at[j]).wait_recv()
        for ahead in (True, False):
            ring(ahead, 0, j).start()

    def reflect(at, panel):
        return gathered[panel, :, :, :, at].reshape(-1, chunk)

    def product(j):
        at = slice(j * chunk, (j + 1) * chunk)
        upper, lower = reflect(at, 0), reflect(at, 1)
        top = jnp.concatenate([rounded[:, at], upper], axis=0)
        first = mxu_nt(top, jnp.concatenate([upper, lower], axis=0))
        second = mxu_nt(lower, lower)
        acc_top[...] = first if j == 0 else acc_top[...] + first
        acc_low[...] = second if j == 0 else acc_low[...] + second

    queue = [(d, j) for d in range(last + 1) for j in range(CHUNKS)]

    def pump(count):
        for _ in range(count):
            d, j = queue.pop(0)
            at = pl.ds(j * chunk, chunk)
            both = gathered.at[:, :, pl.ds(0, 2 if d < last else 1), :, at]
            sized(both, send_f.at[0], recv_f.at[d * CHUNKS + j]).wait_recv()
            if d < last:
                for ahead in (True, False):
                    ring(ahead, d + 1, j).start()
            else:
                product(j)

    def shifted(values, amount):
        both = jnp.concatenate([values, jnp.zeros_like(values)], axis=1)
        for bit in range(7):
            both = jnp.where(((amount >> bit) & 1) == 1, pltpu.roll(both, 1 << bit, 1), both)
        return both

    own_wide = shifted(vectors[...], jnp.concatenate([own_shift, own_shift], axis=1))
    low_top, low_low = [v.astype(F32) for v in halves(own_wide[:, :LANE])]
    high_top, high_low = [v.astype(F32) for v in halves(own_wide[:, LANE:])]
    group = 7

    def build(step, carry):
        for k in range(group):
            tile = (step * group + k).astype(F32)
            first, second = own_tile == tile, own_tile == tile - 1.0
            at = pl.ds(pl.multiple_of((step * group + k) * LANE, LANE), LANE)
            placed_top[:, at] = jnp.where(first, low_top, jnp.where(second, high_top, 0.0)).astype(BF16)
            placed_low[:, at] = jnp.where(first, low_low, jnp.where(second, high_low, 0.0)).astype(BF16)
        return carry

    lax.fori_loop(0, tiles_dev // group, build, 0)
    placed_top[:, cols:] = jnp.zeros((per_dev, NX * part - cols), BF16)
    placed_low[:, cols:] = jnp.zeros((per_dev, NX * part - cols), BF16)
    own_copy = pltpu.make_async_copy(cut.at[cx], gathered.at[:, cx, cz], own_sem.at[0])
    own_copy.start()
    own_copy.wait()

    pl.semaphore_wait(barrier, peers - 1 + 2)
    for j in range(CHUNKS):
        for k in (1, 3, 2):
            over_x(j, k).start()
    for k in range(1, n_row):
        over_row(packs, send_p, recv_p, k).start()
    eigen_load.wait()
    for x in range(NX):
        size = min(part, cols - x * part)
        outgoing[x, :, :size] = eigen[:, x * part : x * part + size].astype(BF16)
        if size < part:
            outgoing[x, :, size:] = jnp.zeros((rows, part - size), BF16)

    own_trade = pltpu.make_async_copy(outgoing.at[cx], traded.at[cx], own_sem.at[1])
    own_trade.start()
    for k in (1, 3, 2):
        along_x(outgoing, traded, send_x, recv_x, k).start()
    for j in range(CHUNKS):
        launch(j)

    def inner_step(step, total):
        at = pl.ds(pl.multiple_of(step * group * LANE, LANE), group * LANE)
        top, low = halves(eigen[:, at])
        first = mxu_nt(jnp.concatenate([top, low], axis=0), placed_top[:, at])
        return total + first[:rows] + first[rows:] + mxu_nt(top, placed_low[:, at])

    steps = tiles_dev // group
    total = lax.fori_loop(0, steps, inner_step, jnp.zeros((rows, per_dev), F32))
    pump(1)

    sized(packs.at[pl.ds(0, n_row - 1)], send_p.at[0], recv_p.at[0]).wait_recv()
    every_meta = packs[0, per_dev:]
    for r in range(1, n_row):
        every_meta = every_meta + packs[r, per_dev:]
    bp = lax.broadcasted_iota(jnp.int32, (BLOCK, BLOCK), 0)
    bq = lax.broadcasted_iota(jnp.int32, (BLOCK, BLOCK), 1)
    diag = bp == bq

    def turned(line):
        return jnp.sum(jnp.where(diag, line, 0.0), axis=1, keepdims=True)

    count = 2 * n_row * half // BLOCK
    across_tile = [every_meta[u : u + 1] for u in range(count)]
    down_tile = []
    for u in range(count):
        s, h = u // 2, u % 2
        low = jnp.concatenate(
            [packs[h * per_tile + k, s * half : (s + 1) * half] for k in range(per_tile)], axis=0
        )
        wide[u * BLOCK : (u + 1) * BLOCK] = shifted(low, turned(every_meta[u + 4 : u + 5]).astype(jnp.int32))
        down = turned(across_tile[u])
        down_tile.append(down)
        tile_of[u * BLOCK : (u + 1) * BLOCK] = jnp.broadcast_to(down, (BLOCK, LANE))

    def of_row(ref, r):
        return jnp.concatenate(
            [ref[pl.ds(pl.multiple_of(s * n_row * half + r * half, half), half)] for s in range(2)], axis=0
        )

    prev_row = jnp.maximum(row - 1, 0)
    prev_tile = of_row(tile_of, prev_row) - (row * tiles_dev).astype(F32)
    prev_high = jnp.where(prev_tile == -1.0, of_row(wide, prev_row)[:, LANE:], 0.0)
    behind = dot3_nt(eigen[:, :LANE], prev_high)
    inners[row] = jnp.concatenate([total, behind], axis=1)
    for k in range(1, n_row):
        over_row(inners, send_w, recv_w, k).start()
    pump(1)

    keep = (((bp // refl) == (bq // refl)) & (bp > bq)) | (((bp // refl) != (bq // refl)) & (bp < bq))
    strict, across = {}, []
    for u in range(count):
        mine = wide[u * BLOCK : (u + 1) * BLOCK]
        rest = wide[u * BLOCK :]
        level = dot3_nt(mine, rest)
        after = dot3_nt(mine[:, LANE:], rest[:, :LANE])
        before = dot3_nt(mine[:, :LANE], rest[:, LANE:])
        for t in range(u, count):
            cols_at = slice((t - u) * BLOCK, (t - u + 1) * BLOCK)
            gap = across_tile[t] - down_tile[u]
            tile = jnp.where(
                gap == 0.0,
                level[:, cols_at],
                jnp.where(gap == 1.0, after[:, cols_at], jnp.where(gap == -1.0, before[:, cols_at], 0.0)),
            )
            if t == u:
                picked = jnp.where(diag, tile, 0.0)
                scale = 2.0 / jnp.sum(picked, axis=1, keepdims=True)
                across.append(2.0 / jnp.sum(picked, axis=0, keepdims=True))
                tile = jnp.where(keep, tile, 0.0)
            strict[u, t] = tile * scale
        if u == 1:
            pump(1)
    inverse = tile_inverses([strict[t, t] for t in range(count)], lambda size: pump(1) if size == 8 else None)
    pump(1)

    sized(inners.at[pl.ds(0, n_row - 1)], send_w.at[0], recv_w.at[0]).wait_recv()
    lane = lax.broadcasted_iota(jnp.int32, (rows, LANE), 1) // half
    right = [jnp.zeros((rows, LANE), F32) for _ in range(count)]
    for r in range(n_row):
        values = inners[r]
        for s in range(2):
            u = s * 2 + r // per_tile
            moved = pltpu.roll(values, (half * (r % per_tile) - half * s) % LANE, 1)
            right[u] = right[u] + jnp.where(lane == r % per_tile, moved, 0.0)
            if r > 0:
                u = s * 2 + (r - 1) // per_tile
                moved = pltpu.roll(values, (half * ((r - 1) % per_tile) - per_dev - half * s) % LANE, 1)
                right[u] = right[u] + jnp.where(lane == (r - 1) % per_tile, moved, 0.0)
    found = []
    for t in range(count):
        value = right[t]
        for u in range(t):
            value = value - dot3(found[u], strict[u, t])
        found.append(dot3(value, inverse[t]))
    solved = [found[t] * across[t] for t in range(count)]

    def coeffs_of(r):
        result = jnp.zeros((rows, LANE), F32)
        for s in range(2):
            tile = jnp.where(r // per_tile == 0, solved[s * 2], solved[s * 2 + 1])
            moved = pltpu.roll(tile, (LANE - half * (r % per_tile) + half * s) % LANE, 1)
            result = jnp.where(lane == s, moved, result)
        return result[:, :per_dev]

    own_coeffs, prev_coeffs = coeffs_of(row), coeffs_of(prev_row)
    shared[cx] = jnp.concatenate([own_coeffs, prev_coeffs], axis=1)
    for k in (1, 3, 2):
        along_x(shared, shared, send_c, recv_c, k).start()
    pump(1)

    def both_halves(values):
        top, low = halves(values)
        return top, jnp.concatenate([top, low], axis=0)

    def changed(top, both, at):
        size = top.shape[0]
        first = mxu(both, placed_top[:, at])
        return first[:size] + first[size:] + mxu(top, placed_low[:, at])

    coeffs_top, coeffs_both = both_halves(own_coeffs)
    first_change = dot3(prev_coeffs, prev_high)

    def keep_step(step, carry):
        at = pl.ds(pl.multiple_of(step * group * LANE, LANE), group * LANE)
        kept[:, at] = eigen[:, at] - changed(coeffs_top, coeffs_both, at)
        return carry

    lax.fori_loop(0, steps // 4, keep_step, 0)
    pump(1)
    kept[:, :LANE] = kept[:, :LANE] - first_change

    own_trade.wait()
    sized(traded.at[pl.ds(0, NX - 1)], send_x.at[0], recv_x.at[0]).wait_recv()
    sized(shared.at[pl.ds(0, NX - 1)], send_c.at[0], recv_c.at[0]).wait_recv()
    all_shared = shared[...].reshape(every, LANE)
    slice_top, slice_both = both_halves(all_shared[:, :per_dev])
    begin_change = jnp.where(cx == 0, 1.0, 0.0).astype(F32) * dot3(all_shared[:, per_dev:], prev_high)
    for j in range(CHUNKS):
        at = slice(j * chunk, (j + 1) * chunk)
        source = pl.ds(pl.multiple_of(cx * part + j * chunk, LANE), chunk)
        value = traded[:, :, at].reshape(every, chunk).astype(F32) - changed(slice_top, slice_both, source)
        if j == 0:
            value = jnp.concatenate([value[:, :LANE] - begin_change, value[:, LANE:]], axis=1)
        rounded[:, at] = value.astype(BF16)
    pump(1)
    lax.fori_loop(steps // 4, steps // 2, keep_step, 0)
    pump(1)
    lax.fori_loop(steps // 2, 3 * steps // 4, keep_step, 0)
    pump(1)
    lax.fori_loop(3 * steps // 4, steps, keep_step, 0)
    kept_copy = pltpu.make_async_copy(kept, kept_hbm, load.at[2])
    kept_copy.start()
    pump(len(queue))

    piece = BLOCK // 2

    def put(place, value):
        rounded = value.astype(BF16)
        work[2 * place] = rounded[:piece]
        work[2 * place + 1] = rounded[piece:]

    for place, (u, t) in enumerate(GRAM_TILES):
        if u < 2:
            put(place, acc_top[(1 + u) * BLOCK : (2 + u) * BLOCK, t * BLOCK : (t + 1) * BLOCK])
        else:
            put(place, acc_low[(u - 2) * BLOCK : (u - 1) * BLOCK, (t - 2) * BLOCK : (t - 1) * BLOCK])
    for t in range(4):
        put(len(GRAM_TILES) + t, acc_top[:BLOCK, t * BLOCK : (t + 1) * BLOCK])

    def scatter(k):
        return pltpu.make_async_remote_copy(
            src_ref=work.at[lax.rem((me + k) % peers, owners)],
            dst_ref=slots.at[k - 1],
            send_sem=send_rs.at[0],
            recv_sem=recv_rs.at[0],
            device_id=device((me + k) % peers),
            device_id_type=mesh,
        )

    def gather(k):
        place = lax.rem(me, owners)
        return pltpu.make_async_remote_copy(
            src_ref=whole.at[place],
            dst_ref=whole.at[place],
            send_sem=send_ag.at[0],
            recv_sem=recv_ag.at[0],
            device_id=device((me + k) % peers),
            device_id_type=mesh,
        )

    for k in range(1, peers):
        pl.when((me + k) % peers < owners)(scatter(k).start)

    @pl.when(me < owners)
    def _():
        sized(slots, send_rs.at[0], recv_rs.at[0]).wait_recv()
        value = work[lax.rem(me, owners)].astype(F32)
        for k in range(1, peers):
            value = value + slots[k - 1].astype(F32)
        whole[lax.rem(me, owners)] = value.astype(BF16)
        for k in range(1, peers):
            gather(k).start()

    pl.when(me < owners)(sized(whole.at[pl.ds(0, owners - 1)], send_ag.at[0], recv_ag.at[0]).wait_recv)
    pl.when(me >= owners)(sized(whole, send_ag.at[0], recv_ag.at[0]).wait_recv)

    def got(place):
        return jnp.concatenate([whole[2 * place].astype(F32), whole[2 * place + 1].astype(F32)], axis=0)

    gram = {key: got(place) for place, key in enumerate(GRAM_TILES)}
    picked = [jnp.where(diag, gram[t, t], 0.0) for t in range(4)]
    down = [2.0 / jnp.sum(p, axis=1, keepdims=True) for p in picked]
    beside = [2.0 / jnp.sum(p, axis=0, keepdims=True) for p in picked]
    panel_strict = {(u, t): gram[u, t] * down[u] for u, t in GRAM_TILES}
    for t in range(4):
        panel_strict[t, t] = jnp.where(bp > bq, panel_strict[t, t], 0.0)
    panel_inverse = tile_inverses([panel_strict[t, t] for t in range(4)])
    answer = {}
    for t in (1, 0, 3, 2):
        value = got(len(GRAM_TILES) + t)
        for u in tuple(answer):
            value = value - dot3(answer[u], panel_strict[u, t])
        answer[t] = dot3(value, panel_inverse[t])
    coeffs = jnp.concatenate([(answer[t] * beside[t]).astype(BF16) for t in range(4)], axis=1)

    def back(j, k):
        target = (cx + k) % NX
        return pltpu.make_async_remote_copy(
            src_ref=change.at[target, :, pl.ds(j * chunk, chunk)],
            dst_ref=home.at[:, pl.ds(pl.multiple_of(cx * part + j * chunk, LANE), chunk)],
            send_sem=send_h.at[0],
            recv_sem=recv_h.at[0],
            device_id={"cx": target},
            device_id_type=mesh,
        )

    for j in range(CHUNKS):
        at = slice(j * chunk, (j + 1) * chunk)
        value = mxu(coeffs, jnp.concatenate([reflect(at, 0), reflect(at, 1)], axis=0)).astype(BF16)
        for x in range(NX):
            change[x, :, at] = value[x * rows : (x + 1) * rows]
        for k in (2, 1, 3):
            back(j, k).start()
    keep_home = pltpu.make_async_copy(
        change.at[cx], home.at[:, pl.ds(pl.multiple_of(cx * part, LANE), part)], own_sem.at[0]
    )
    keep_home.start()

    sized(packs.at[pl.ds(0, n_row - 1)], send_p.at[0], recv_p.at[0]).wait_send()
    sized(inners.at[pl.ds(0, n_row - 1)], send_w.at[0], recv_w.at[0]).wait_send()
    sized(outgoing.at[pl.ds(0, NX - 1)], send_x.at[0], recv_x.at[0]).wait_send()
    sized(shared.at[pl.ds(0, NX - 1)], send_c.at[0], recv_c.at[0]).wait_send()
    sized(cut.at[pl.ds(0, NX - 1)], send_a.at[0], recv_a.at[0]).wait_send()
    sized(gathered.at[:, :, pl.ds(0, NZ - 1)], send_f.at[0], recv_f.at[0]).wait_send()
    pl.when(me < owners)(sized(work.at[pl.ds(0, owners - 1)], send_rs.at[0], recv_rs.at[0]).wait_send)
    pl.when(me >= owners)(sized(work, send_rs.at[0], recv_rs.at[0]).wait_send)
    pl.when(me < owners)(sized(slots, send_ag.at[0], recv_ag.at[0]).wait_send)
    kept_copy.wait()
    keep_home.wait()
    sized(change.at[pl.ds(0, NX - 1)], send_h.at[0], recv_h.at[0]).wait_send()
    sized(home.at[:, pl.ds(0, (NX - 1) * part)], send_h.at[0], recv_h.at[0]).wait_recv()


def fused_step(offs, vectors, eigen, panels, n_row):
    rows, cols = eigen.shape
    n_panel, refl_dev, _ = panels.shape
    part = -(-(cols // LANE) // NX) * LANE
    per_dev, band = vectors.shape
    peers = n_row * NX
    owners, piece = 2 * (len(GRAM_TILES) + 4), BLOCK // 2
    every = NX * rows
    dma = pltpu.SemaphoreType.DMA
    hbm = pl.BlockSpec(memory_space=pltpu.HBM)
    units = (NZ // 2) * CHUNKS
    trade = (NX, rows, part)
    return pl.pallas_call(
        fused_kernel,
        out_shape=[jax.ShapeDtypeStruct((rows, cols), F32), jax.ShapeDtypeStruct((rows, NX * part), BF16)],
        in_specs=[hbm] * 4,
        out_specs=[hbm] * 2,
        scratch_shapes=[
            pltpu.VMEM((rows, cols), F32),
            pltpu.SMEM(offs.shape, jnp.int32),
            pltpu.VMEM((per_dev, band), F32),
            pltpu.VMEM((rows, cols), F32),
            pltpu.VMEM((NX, n_panel, refl_dev, part), BF16),
            pltpu.VMEM((n_panel, NX, NZ, refl_dev, part), BF16),
            pltpu.VMEM((n_row, per_dev + 8, band), F32),
            pltpu.VMEM((n_row, rows, LANE), F32),
            pltpu.VMEM((n_row * per_dev, 2 * LANE), F32),
            pltpu.VMEM((n_row * per_dev, LANE), F32),
            pltpu.VMEM((per_dev, NX * part), BF16),
            pltpu.VMEM((per_dev, NX * part), BF16),
            pltpu.VMEM(trade, BF16),
            pltpu.VMEM(trade, BF16),
            pltpu.VMEM((NX, rows, LANE), F32),
            pltpu.VMEM((every, part), BF16),
            pltpu.VMEM((every + 2 * BLOCK, 4 * BLOCK), F32),
            pltpu.VMEM((2 * BLOCK, 2 * BLOCK), F32),
            pltpu.VMEM((owners, piece, BLOCK), BF16),
            pltpu.VMEM((peers - 1, piece, BLOCK), BF16),
            pltpu.VMEM((owners, piece, BLOCK), BF16),
            pltpu.VMEM(trade, BF16),
            dma((3 + NX,)),
            dma((1,)),
            dma((CHUNKS,)),
            dma((1,)),
            dma((1,)),
            dma((1,)),
            dma((1,)),
            dma((1,)),
            dma((units,)),
            dma((1,)),
            dma((1,)),
            dma((1,)),
            dma((1,)),
            dma((1,)),
            dma((1,)),
            dma((1,)),
            dma((1,)),
            dma((1,)),
            dma((1,)),
            dma((2,)),
        ],
        compiler_params=pltpu.CompilerParams(
            collective_id=0, has_side_effects=True, vmem_limit_bytes=60 * 1024 * 1024
        ),
        cost_estimate=pl.CostEstimate(flops=20_000_000_000, bytes_accessed=8_000_000, transcendentals=0),
    )(offs, vectors, eigen, panels)


def local(eigvecs, span_vectors, span_offsets, panels):
    cols = eigvecs.shape[1]
    band = span_vectors.shape[3]
    n_row = lax.psum(1, "row")
    eigen, home = fused_step(span_offsets, span_vectors.reshape(-1, band), eigvecs, panels, n_row)
    return eigen - home[:, :cols].astype(F32)


def solution(mesh):
    finer = Mesh(mesh.devices.reshape(mesh.shape["row"], NX, NZ), ("row", "cx", "cz"))
    col = ("cx", "cz")
    placed = (P(col, "row"), P(None, "row", None, None), P(None, "row"), P(None, col, "row"))
    return jax.shard_map(local, mesh=finer, in_specs=placed, out_specs=P(col, "row"), check_vma=False)
```

```python
import functools

import jax
import jax.numpy as jnp
from jax import lax
from jax.experimental import pallas as pl
from jax.experimental.pallas import tpu as pltpu
from jax.sharding import Mesh
from jax.sharding import PartitionSpec as P

LANE = 128
BLOCK = 128
NX = 4
NZ = 8
CHUNKS = 5
F32 = jnp.float32
BF16 = jnp.bfloat16
NT = (((1,), (1,)), ((), ()))
NN = (((1,), (0,)), ((), ()))


def halves(a):
    top = a.astype(BF16)
    return top, (a - top.astype(F32)).astype(BF16)


def dot3(a, b):
    a_top, a_low = halves(a)
    b_top, b_low = halves(b)
    d = functools.partial(lax.dot_general, dimension_numbers=NN, preferred_element_type=F32)
    return d(a_top, b_top) + (d(a_top, b_low) + d(a_low, b_top))


GRAM_TILES = ((0, 0), (0, 2), (0, 3), (1, 0), (1, 1), (1, 2), (1, 3), (2, 2), (3, 2), (3, 3))


def dot3_nt(a, b):
    a_top, a_low = halves(a)
    b_top, b_low = halves(b)
    d = functools.partial(lax.dot_general, dimension_numbers=NT, preferred_element_type=F32)
    return d(a_top, b_top) + (d(a_top, b_low) + d(a_low, b_top))


def tile_inverses(tiles, between=None):
    bp = lax.broadcasted_iota(jnp.int32, (BLOCK, BLOCK), 0)
    bq = lax.broadcasted_iota(jnp.int32, (BLOCK, BLOCK), 1)
    eye = (bp == bq).astype(F32)
    inverse = [eye - jnp.where(bp // 2 == bq // 2, tile, 0.0) for tile in tiles]
    size = 2
    while size < BLOCK:
        joined = (bp // (2 * size) == bq // (2 * size)) & (bp // size != bq // size)
        left = [dot3(inv, jnp.where(joined, tile, 0.0)) for inv, tile in zip(inverse, tiles)]
        inverse = [inv - dot3(lhs, inv) for inv, lhs in zip(inverse, left)]
        if between is not None:
            between(size)
        size *= 2
    return inverse


def fused_kernel(offs_hbm, vectors_hbm, eigen_hbm, panels_hbm, kept_hbm, home, kept, offs, vectors, eigen, cut, gathered, packs,
                 inners, wide, tile_of, placed_top, placed_low, outgoing, traded, shared, rounded, acc_top, acc_low,
                 work, joined, slots, whole, change, load, send_a, recv_a, send_p, recv_p, send_w, recv_w, send_f, recv_f,
                 send_x, recv_x, send_c, recv_c, send_d, recv_d, send_rs, recv_rs, send_ag, recv_ag, send_h, recv_h,
                 own_sem):
    row, cx, cz = lax.axis_index("row"), lax.axis_index("cx"), lax.axis_index("cz")
    n_row = lax.axis_size("row")
    rows, cols = eigen.shape
    every = NX * rows
    tiles_dev = cols // LANE
    part = cut.shape[3]
    chunk = part // CHUNKS
    n_panel = cut.shape[1]
    per_dev = vectors.shape[0]
    half = per_dev // 2
    refl = 4
    spans = half // refl
    per_tile = BLOCK // half
    peers = n_row * NX
    me = row * NX + cx
    owners = joined.shape[0]
    mesh = pl.DeviceIdType.MESH
    mxu_nt = functools.partial(lax.dot_general, dimension_numbers=NT, preferred_element_type=F32)
    mxu = functools.partial(lax.dot_general, dimension_numbers=NN, preferred_element_type=F32)

    def device(place):
        return {"row": place // NX, "cx": place % NX}

    loads = [
        pltpu.make_async_copy(offs_hbm, offs, load.at[0]),
        pltpu.make_async_copy(vectors_hbm, vectors, load.at[1]),
    ]
    eigen_load = pltpu.make_async_copy(eigen_hbm, eigen, load.at[2])
    for x in range(NX):
        size = min(part, cols - x * part)
        loads.append(
            pltpu.make_async_copy(
                panels_hbm.at[:, :, pl.ds(x * part, size)], cut.at[x, :, :, pl.ds(0, size)], load.at[3 + x]
            )
        )
        if size < part:
            cut[x, :, :, size:] = jnp.zeros((n_panel, cut.shape[2], part - size), BF16)
    for copy in loads:
        copy.start()
    eigen_load.start()
    barrier = pltpu.get_barrier_semaphore()
    for k in (1, NZ - 1):
        pl.semaphore_signal(barrier, inc=1, device_id={"cz": (cz + k) % NZ}, device_id_type=mesh)
    for k in range(1, peers):
        pl.semaphore_signal(barrier, inc=1, device_id=device((me + k) % peers), device_id_type=mesh)
    for copy in loads:
        copy.wait()

    lane8 = lax.broadcasted_iota(jnp.int32, (8, LANE), 1)
    line8 = lax.broadcasted_iota(jnp.int32, (8, LANE), 0)
    line64 = lax.broadcasted_iota(jnp.int32, (per_dev, LANE), 0) // refl
    meta = jnp.zeros((8, LANE), F32)
    own_tile = jnp.zeros((per_dev, LANE), F32)
    own_shift = jnp.zeros((per_dev, LANE), jnp.int32)
    for s in range(2):
        for b in range(spans):
            at = offs[s, b]
            tile_at = at >> 7
            shift_at = at & 127
            place = (row % per_tile) * half + b * refl
            mine = (lane8 >= place) & (lane8 < place + refl)
            line = s * 2 + row // per_tile
            meta = jnp.where(mine & (line8 == line), (tile_at + row * tiles_dev).astype(F32), meta)
            meta = jnp.where(mine & (line8 == line + 4), shift_at.astype(F32), meta)
            own_tile = jnp.where(line64 == s * spans + b, tile_at.astype(F32), own_tile)
            own_shift = jnp.where(line64 == s * spans + b, shift_at, own_shift)
    packs[row, :per_dev] = vectors[...]
    packs[row, per_dev:] = meta
    def sized(ref, send, recv):
        return pltpu.make_async_remote_copy(
            src_ref=ref, dst_ref=ref, send_sem=send, recv_sem=recv, device_id={"cx": (cx + 1) % NX}, device_id_type=mesh
        )

    def over_x(j, k):
        at = pl.ds(j * chunk, chunk)
        return pltpu.make_async_remote_copy(
            src_ref=cut.at[(cx + k) % NX, :, :, at],
            dst_ref=gathered.at[:, cx, cz, :, at],
            send_sem=send_a.at[0],
            recv_sem=recv_a.at[j],
            device_id={"cx": (cx + k) % NX},
            device_id_type=mesh,
        )

    def over_row(ref, sends, recvs, k):
        return pltpu.make_async_remote_copy(
            src_ref=ref.at[row],
            dst_ref=ref.at[row],
            send_sem=sends.at[0],
            recv_sem=recvs.at[0],
            device_id={"row": (row + k) % n_row},
            device_id_type=mesh,
        )

    def along_x(source_ref, target_ref, sends, recvs, k):
        target = (cx + k) % NX
        return pltpu.make_async_remote_copy(
            src_ref=source_ref.at[target] if source_ref is not target_ref else source_ref.at[cx],
            dst_ref=target_ref.at[cx],
            send_sem=sends.at[0],
            recv_sem=recvs.at[0],
            device_id={"cx": target},
            device_id_type=mesh,
        )

    last = NZ // 2 - 1

    def ring(ahead, d, j):
        step = 1 if ahead else NZ - 1
        at = pl.ds(j * chunk, chunk)
        panel = slice(None) if d < last else (pl.ds(0, 1) if ahead else pl.ds(1, 1))
        place = gathered.at[panel, :, (cz + NZ - d * step) % NZ if ahead else (cz + d) % NZ, :, at]
        return pltpu.make_async_remote_copy(
            src_ref=place,
            dst_ref=place,
            send_sem=send_f.at[0],
            recv_sem=recv_f.at[d * CHUNKS + j],
            device_id={"cz": (cz + step) % NZ},
            device_id_type=mesh,
        )

    def own_block(ahead, j, k):
        at = pl.ds(j * chunk, chunk)
        place = gathered.at[:, (cx + NX - k) % NX, cz, :, at]
        return pltpu.make_async_remote_copy(
            src_ref=cut.at[cx, :, :, at] if k == 0 else place,
            dst_ref=place,
            send_sem=send_f.at[0],
            recv_sem=recv_f.at[j],
            device_id={"cz": (cz + (1 if ahead else NZ - 1)) % NZ},
            device_id_type=mesh,
        )

    def launch(j):
        at = pl.ds(j * chunk, chunk)
        sized(gathered.at[:, pl.ds(0, NX - 1), cz, :, at], send_a.at[0], recv_a.at[j]).wait_recv()
        for k in range(1, NX):
            for ahead in (True, False):
                own_block(ahead, j, k).start()

    def reflect(at, panel):
        return gathered[panel, :, :, :, at].reshape(-1, chunk)

    def product(j):
        at = slice(j * chunk, (j + 1) * chunk)
        upper, lower = reflect(at, 0), reflect(at, 1)
        top = jnp.concatenate([rounded[:, at], upper], axis=0)
        first = mxu_nt(top, jnp.concatenate([upper, lower], axis=0))
        second = mxu_nt(lower, lower)
        acc_top[...] = first if j == 0 else acc_top[...] + first
        acc_low[...] = second if j == 0 else acc_low[...] + second

    queue = [(d, j) for d in range(last + 1) for j in range(CHUNKS)]

    def pump(count):
        for _ in range(count):
            d, j = queue.pop(0)
            at = pl.ds(j * chunk, chunk)
            both = gathered.at[:, :, pl.ds(0, 2 if d < last else 1), :, at]
            sized(both, send_f.at[0], recv_f.at[d * CHUNKS + j]).wait_recv()
            if d < last:
                for ahead in (True, False):
                    ring(ahead, d + 1, j).start()
            else:
                product(j)

    def shifted(values, amount):
        both = jnp.concatenate([values, jnp.zeros_like(values)], axis=1)
        for bit in range(7):
            both = jnp.where(((amount >> bit) & 1) == 1, pltpu.roll(both, 1 << bit, 1), both)
        return both

    own_copy = pltpu.make_async_copy(cut.at[cx], gathered.at[:, cx, cz], own_sem.at[0])
    own_copy.start()

    pl.semaphore_wait(barrier, peers - 1 + 2)
    for j in range(3):
        for k in (1, 3, 2):
            over_x(j, k).start()
        if j == 0:
            for i in range(CHUNKS):
                for ahead in (True, False):
                    own_block(ahead, i, 0).start()
    for k in range(1, n_row):
        over_row(packs, send_p, recv_p, k).start()
    own_wide = shifted(vectors[...], jnp.concatenate([own_shift, own_shift], axis=1))
    low_top, low_low = [v.astype(F32) for v in halves(own_wide[:, :LANE])]
    high_top, high_low = [v.astype(F32) for v in halves(own_wide[:, LANE:])]
    group = 7

    def build(step, carry):
        for k in range(group):
            tile = (step * group + k).astype(F32)
            first, second = own_tile == tile, own_tile == tile - 1.0
            at = pl.ds(pl.multiple_of((step * group + k) * LANE, LANE), LANE)
            placed_top[:, at] = jnp.where(first, low_top, jnp.where(second, high_top, 0.0)).astype(BF16)
            placed_low[:, at] = jnp.where(first, low_low, jnp.where(second, high_low, 0.0)).astype(BF16)
        return carry

    lax.fori_loop(0, tiles_dev // group, build, 0)
    placed_top[:, cols:] = jnp.zeros((per_dev, NX * part - cols), BF16)
    placed_low[:, cols:] = jnp.zeros((per_dev, NX * part - cols), BF16)
    eigen_load.wait()
    for x in range(NX):
        size = min(part, cols - x * part)
        outgoing[x, :, :size] = eigen[:, x * part : x * part + size].astype(BF16)
        if size < part:
            outgoing[x, :, size:] = jnp.zeros((rows, part - size), BF16)

    own_trade = pltpu.make_async_copy(outgoing.at[cx], traded.at[cx], own_sem.at[1])
    own_trade.start()
    def inner_step(step, total):
        at = pl.ds(pl.multiple_of(step * group * LANE, LANE), group * LANE)
        top, low = halves(eigen[:, at])
        first = mxu_nt(jnp.concatenate([top, low], axis=0), placed_top[:, at])
        return total + first[:rows] + first[rows:] + mxu_nt(top, placed_low[:, at])

    steps = tiles_dev // group
    for j in range(2):
        launch(j)
        for k in (1, 3, 2):
            over_x(j + 3, k).start()
    for k in (1, 3, 2):
        along_x(outgoing, traded, send_x, recv_x, k).start()
    total = lax.fori_loop(0, steps // 2, inner_step, jnp.zeros((rows, per_dev), F32))
    launch(2)
    launch(3)
    total = lax.fori_loop(steps // 2, steps, inner_step, total)
    launch(4)
    pump(1)

    sized(packs.at[pl.ds(0, n_row - 1)], send_p.at[0], recv_p.at[0]).wait_recv()
    every_meta = packs[0, per_dev:]
    for r in range(1, n_row):
        every_meta = every_meta + packs[r, per_dev:]
    bp = lax.broadcasted_iota(jnp.int32, (BLOCK, BLOCK), 0)
    bq = lax.broadcasted_iota(jnp.int32, (BLOCK, BLOCK), 1)
    diag = bp == bq

    def turned(line):
        return jnp.sum(jnp.where(diag, line, 0.0), axis=1, keepdims=True)

    count = 2 * n_row * half // BLOCK
    across_tile = [every_meta[u : u + 1] for u in range(count)]
    down_tile = []
    for u in range(count):
        s, h = u // 2, u % 2
        low = jnp.concatenate(
            [packs[h * per_tile + k, s * half : (s + 1) * half] for k in range(per_tile)], axis=0
        )
        wide[u * BLOCK : (u + 1) * BLOCK] = shifted(low, turned(every_meta[u + 4 : u + 5]).astype(jnp.int32))
        down = turned(across_tile[u])
        down_tile.append(down)
        tile_of[u * BLOCK : (u + 1) * BLOCK] = jnp.broadcast_to(down, (BLOCK, LANE))

    def of_row(ref, r):
        return jnp.concatenate(
            [ref[pl.ds(pl.multiple_of(s * n_row * half + r * half, half), half)] for s in range(2)], axis=0
        )

    prev_row = jnp.maximum(row - 1, 0)
    prev_tile = of_row(tile_of, prev_row) - (row * tiles_dev).astype(F32)
    prev_high = jnp.where(prev_tile == -1.0, of_row(wide, prev_row)[:, LANE:], 0.0)
    behind = dot3_nt(eigen[:, :LANE], prev_high)
    inners[row] = jnp.concatenate([total, behind], axis=1)
    for k in range(1, n_row):
        over_row(inners, send_w, recv_w, k).start()
    pump(1)

    keep = (((bp // refl) == (bq // refl)) & (bp > bq)) | (((bp // refl) != (bq // refl)) & (bp < bq))
    strict, across = {}, []
    for u in range(count):
        mine = wide[u * BLOCK : (u + 1) * BLOCK]
        rest = wide[u * BLOCK :]
        level = dot3_nt(mine, rest)
        after = dot3_nt(mine[:, LANE:], rest[:, :LANE])
        before = dot3_nt(mine[:, :LANE], rest[:, LANE:])
        for t in range(u, count):
            cols_at = slice((t - u) * BLOCK, (t - u + 1) * BLOCK)
            gap = across_tile[t] - down_tile[u]
            tile = jnp.where(
                gap == 0.0,
                level[:, cols_at],
                jnp.where(gap == 1.0, after[:, cols_at], jnp.where(gap == -1.0, before[:, cols_at], 0.0)),
            )
            if t == u:
                picked = jnp.where(diag, tile, 0.0)
                scale = 2.0 / jnp.sum(picked, axis=1, keepdims=True)
                across.append(2.0 / jnp.sum(picked, axis=0, keepdims=True))
                tile = jnp.where(keep, tile, 0.0)
            strict[u, t] = tile * scale
        if u == 1:
            pump(1)
    inverse = tile_inverses([strict[t, t] for t in range(count)], lambda size: pump(1) if size == 8 else None)
    pump(1)

    sized(inners.at[pl.ds(0, n_row - 1)], send_w.at[0], recv_w.at[0]).wait_recv()
    lane = lax.broadcasted_iota(jnp.int32, (rows, LANE), 1) // half
    right = [jnp.zeros((rows, LANE), F32) for _ in range(count)]
    for r in range(n_row):
        values = inners[r]
        for s in range(2):
            u = s * 2 + r // per_tile
            moved = pltpu.roll(values, (half * (r % per_tile) - half * s) % LANE, 1)
            right[u] = right[u] + jnp.where(lane == r % per_tile, moved, 0.0)
            if r > 0:
                u = s * 2 + (r - 1) // per_tile
                moved = pltpu.roll(values, (half * ((r - 1) % per_tile) - per_dev - half * s) % LANE, 1)
                right[u] = right[u] + jnp.where(lane == (r - 1) % per_tile, moved, 0.0)
    found = []
    for t in range(count):
        value = right[t]
        for u in range(t):
            value = value - dot3(found[u], strict[u, t])
        found.append(dot3(value, inverse[t]))
    solved = [found[t] * across[t] for t in range(count)]

    def coeffs_of(r):
        result = jnp.zeros((rows, LANE), F32)
        for s in range(2):
            tile = jnp.where(r // per_tile == 0, solved[s * 2], solved[s * 2 + 1])
            moved = pltpu.roll(tile, (LANE - half * (r % per_tile) + half * s) % LANE, 1)
            result = jnp.where(lane == s, moved, result)
        return result[:, :per_dev]

    own_coeffs, prev_coeffs = coeffs_of(row), coeffs_of(prev_row)
    shared[cx] = jnp.concatenate([own_coeffs, prev_coeffs], axis=1)
    for k in (1, 3, 2):
        along_x(shared, shared, send_c, recv_c, k).start()
    pump(1)

    def both_halves(values):
        top, low = halves(values)
        return top, jnp.concatenate([top, low], axis=0)

    def changed(top, both, at):
        size = top.shape[0]
        first = mxu(both, placed_top[:, at])
        return first[:size] + first[size:] + mxu(top, placed_low[:, at])

    coeffs_top, coeffs_both = both_halves(own_coeffs)
    first_change = dot3(prev_coeffs, prev_high)

    def keep_step(step, carry):
        at = pl.ds(pl.multiple_of(step * group * LANE, LANE), group * LANE)
        kept[:, at] = eigen[:, at] - changed(coeffs_top, coeffs_both, at)
        return carry

    lax.fori_loop(0, steps // 4, keep_step, 0)
    pump(1)
    kept[:, :LANE] = kept[:, :LANE] - first_change

    pump(1)
    lax.fori_loop(steps // 4, steps // 2, keep_step, 0)
    pump(1)
    lax.fori_loop(steps // 2, 3 * steps // 4, keep_step, 0)
    pump(1)
    lax.fori_loop(3 * steps // 4, steps, keep_step, 0)
    kept_copy = pltpu.make_async_copy(kept, kept_hbm, load.at[2])
    kept_copy.start()
    own_copy.wait()
    own_trade.wait()
    sized(traded.at[pl.ds(0, NX - 1)], send_x.at[0], recv_x.at[0]).wait_recv()
    sized(shared.at[pl.ds(0, NX - 1)], send_c.at[0], recv_c.at[0]).wait_recv()
    all_shared = shared[...].reshape(every, LANE)
    slice_top, slice_both = both_halves(all_shared[:, :per_dev])
    begin_change = jnp.where(cx == 0, 1.0, 0.0).astype(F32) * dot3(all_shared[:, per_dev:], prev_high)
    for j in range(CHUNKS):
        at = slice(j * chunk, (j + 1) * chunk)
        source = pl.ds(pl.multiple_of(cx * part + j * chunk, LANE), chunk)
        value = traded[:, :, at].reshape(every, chunk).astype(F32) - changed(slice_top, slice_both, source)
        if j == 0:
            value = jnp.concatenate([value[:, :LANE] - begin_change, value[:, LANE:]], axis=1)
        rounded[:, at] = value.astype(BF16)
    pump(len(queue))

    piece = BLOCK // 2

    def put(place, value):
        rounded = value.astype(BF16)
        work[2 * place] = rounded[:piece]
        work[2 * place + 1] = rounded[piece:]

    for place, (u, t) in enumerate(GRAM_TILES):
        if u < 2:
            put(place, acc_top[(1 + u) * BLOCK : (2 + u) * BLOCK, t * BLOCK : (t + 1) * BLOCK])
        else:
            put(place, acc_low[(u - 2) * BLOCK : (u - 1) * BLOCK, (t - 2) * BLOCK : (t - 1) * BLOCK])
    for t in range(4):
        put(len(GRAM_TILES) + t, acc_top[:BLOCK, t * BLOCK : (t + 1) * BLOCK])

    core, chip = row % 2, (row // 2) * NX + cx
    chips = peers // 2

    def across(source, target, send, recv):
        return pltpu.make_async_remote_copy(
            src_ref=source,
            dst_ref=target,
            send_sem=send,
            recv_sem=recv,
            device_id={"row": row + 1 - 2 * core},
            device_id_type=mesh,
        )

    def on_chip(place):
        return {"row": (place // NX) * 2 + core, "cx": place % NX}

    def scatter(k):
        target = (chip + k) % chips
        return pltpu.make_async_remote_copy(
            src_ref=joined.at[lax.rem(target, owners)],
            dst_ref=slots.at[k - 1],
            send_sem=send_rs.at[0],
            recv_sem=recv_rs.at[0],
            device_id=on_chip(target),
            device_id_type=mesh,
        )

    mine = core * owners + lax.rem(chip, owners)

    def gather(k):
        return pltpu.make_async_remote_copy(
            src_ref=whole.at[mine],
            dst_ref=whole.at[mine],
            send_sem=send_ag.at[0],
            recv_sem=recv_ag.at[0],
            device_id=on_chip((chip + k) % chips),
            device_id_type=mesh,
        )

    first_swap = across(work.at[pl.ds((1 - core) * owners, owners)], joined, send_d.at[0], recv_d.at[0])
    first_swap.start()
    first_swap.wait_recv()
    for place in range(owners):
        joined[place] = (joined[place].astype(F32) + work[core * owners + place].astype(F32)).astype(BF16)
    for k in range(1, chips):
        pl.when((chip + k) % chips < owners)(scatter(k).start)

    @pl.when(chip < owners)
    def _():
        sized(slots, send_rs.at[0], recv_rs.at[0]).wait_recv()
        value = joined[lax.rem(chip, owners)].astype(F32)
        for k in range(1, chips):
            value = value + slots[k - 1].astype(F32)
        whole[mine] = value.astype(BF16)
        for k in range(1, chips):
            gather(k).start()

    pl.when(chip < owners)(sized(whole.at[pl.ds(0, owners - 1)], send_ag.at[0], recv_ag.at[0]).wait_recv)
    pl.when(chip >= owners)(sized(whole.at[pl.ds(0, owners)], send_ag.at[0], recv_ag.at[0]).wait_recv)
    half_whole = whole.at[pl.ds(core * owners, owners)]
    second_swap = across(half_whole, half_whole, send_d.at[1], recv_d.at[1])
    second_swap.start()
    second_swap.wait_recv()

    def got(place):
        return jnp.concatenate([whole[2 * place].astype(F32), whole[2 * place + 1].astype(F32)], axis=0)

    gram = {key: got(place) for place, key in enumerate(GRAM_TILES)}
    picked = [jnp.where(diag, gram[t, t], 0.0) for t in range(4)]
    down = [2.0 / jnp.sum(p, axis=1, keepdims=True) for p in picked]
    beside = [2.0 / jnp.sum(p, axis=0, keepdims=True) for p in picked]
    panel_strict = {(u, t): gram[u, t] * down[u] for u, t in GRAM_TILES}
    for t in range(4):
        panel_strict[t, t] = jnp.where(bp > bq, panel_strict[t, t], 0.0)
    panel_inverse = tile_inverses([panel_strict[t, t] for t in range(4)])
    answer = {}
    for t in (1, 0, 3, 2):
        value = got(len(GRAM_TILES) + t)
        for u in tuple(answer):
            value = value - dot3(answer[u], panel_strict[u, t])
        answer[t] = dot3(value, panel_inverse[t])
    coeffs = jnp.concatenate([(answer[t] * beside[t]).astype(BF16) for t in range(4)], axis=1)

    def back(j, k):
        target = (cx + k) % NX
        return pltpu.make_async_remote_copy(
            src_ref=change.at[target, :, pl.ds(j * chunk, chunk)],
            dst_ref=home.at[:, pl.ds(pl.multiple_of(cx * part + j * chunk, LANE), chunk)],
            send_sem=send_h.at[0],
            recv_sem=recv_h.at[0],
            device_id={"cx": target},
            device_id_type=mesh,
        )

    for j in range(CHUNKS):
        at = slice(j * chunk, (j + 1) * chunk)
        value = mxu(coeffs, jnp.concatenate([reflect(at, 0), reflect(at, 1)], axis=0)).astype(BF16)
        for x in range(NX):
            change[x, :, at] = value[x * rows : (x + 1) * rows]
        for k in (2, 1, 3):
            back(j, k).start()
    keep_home = pltpu.make_async_copy(
        change.at[cx], home.at[:, pl.ds(pl.multiple_of(cx * part, LANE), part)], own_sem.at[0]
    )
    keep_home.start()

    sized(packs.at[pl.ds(0, n_row - 1)], send_p.at[0], recv_p.at[0]).wait_send()
    sized(inners.at[pl.ds(0, n_row - 1)], send_w.at[0], recv_w.at[0]).wait_send()
    sized(outgoing.at[pl.ds(0, NX - 1)], send_x.at[0], recv_x.at[0]).wait_send()
    sized(shared.at[pl.ds(0, NX - 1)], send_c.at[0], recv_c.at[0]).wait_send()
    sized(cut.at[pl.ds(0, NX - 1)], send_a.at[0], recv_a.at[0]).wait_send()
    sized(gathered.at[:, :, pl.ds(0, NZ - 1)], send_f.at[0], recv_f.at[0]).wait_send()
    first_swap.wait_send()
    second_swap.wait_send()
    pl.when(chip < owners)(sized(joined.at[pl.ds(0, owners - 1)], send_rs.at[0], recv_rs.at[0]).wait_send)
    pl.when(chip >= owners)(sized(joined, send_rs.at[0], recv_rs.at[0]).wait_send)
    pl.when(chip < owners)(sized(slots, send_ag.at[0], recv_ag.at[0]).wait_send)
    kept_copy.wait()
    keep_home.wait()
    sized(change.at[pl.ds(0, NX - 1)], send_h.at[0], recv_h.at[0]).wait_send()
    sized(home.at[:, pl.ds(0, (NX - 1) * part)], send_h.at[0], recv_h.at[0]).wait_recv()


def fused_step(offs, vectors, eigen, panels, n_row):
    rows, cols = eigen.shape
    n_panel, refl_dev, _ = panels.shape
    part = -(-(cols // LANE) // NX) * LANE
    per_dev, band = vectors.shape
    owners, piece = 2 * (len(GRAM_TILES) + 4), BLOCK // 2
    every = NX * rows
    dma = pltpu.SemaphoreType.DMA
    hbm = pl.BlockSpec(memory_space=pltpu.HBM)
    units = (NZ // 2) * CHUNKS
    trade = (NX, rows, part)
    return pl.pallas_call(
        fused_kernel,
        out_shape=[jax.ShapeDtypeStruct((rows, cols), F32), jax.ShapeDtypeStruct((rows, NX * part), BF16)],
        in_specs=[hbm] * 4,
        out_specs=[hbm] * 2,
        scratch_shapes=[
            pltpu.VMEM((rows, cols), F32),
            pltpu.SMEM(offs.shape, jnp.int32),
            pltpu.VMEM((per_dev, band), F32),
            pltpu.VMEM((rows, cols), F32),
            pltpu.VMEM((NX, n_panel, refl_dev, part), BF16),
            pltpu.VMEM((n_panel, NX, NZ, refl_dev, part), BF16),
            pltpu.VMEM((n_row, per_dev + 8, band), F32),
            pltpu.VMEM((n_row, rows, LANE), F32),
            pltpu.VMEM((n_row * per_dev, 2 * LANE), F32),
            pltpu.VMEM((n_row * per_dev, LANE), F32),
            pltpu.VMEM((per_dev, NX * part), BF16),
            pltpu.VMEM((per_dev, NX * part), BF16),
            pltpu.VMEM(trade, BF16),
            pltpu.VMEM(trade, BF16),
            pltpu.VMEM((NX, rows, LANE), F32),
            pltpu.VMEM((every, part), BF16),
            pltpu.VMEM((every + 2 * BLOCK, 4 * BLOCK), F32),
            pltpu.VMEM((2 * BLOCK, 2 * BLOCK), F32),
            pltpu.VMEM((owners, piece, BLOCK), BF16),
            pltpu.VMEM((owners // 2, piece, BLOCK), BF16),
            pltpu.VMEM((n_row * NX // 2 - 1, piece, BLOCK), BF16),
            pltpu.VMEM((owners, piece, BLOCK), BF16),
            pltpu.VMEM(trade, BF16),
            dma((3 + NX,)),
            dma((1,)),
            dma((CHUNKS,)),
            dma((1,)),
            dma((1,)),
            dma((1,)),
            dma((1,)),
            dma((1,)),
            dma((units,)),
            dma((1,)),
            dma((1,)),
            dma((1,)),
            dma((1,)),
            dma((2,)),
            dma((2,)),
            dma((1,)),
            dma((1,)),
            dma((1,)),
            dma((1,)),
            dma((1,)),
            dma((1,)),
            dma((2,)),
        ],
        compiler_params=pltpu.CompilerParams(
            collective_id=0, has_side_effects=True, vmem_limit_bytes=60 * 1024 * 1024
        ),
        cost_estimate=pl.CostEstimate(flops=20_000_000_000, bytes_accessed=8_000_000, transcendentals=0),
    )(offs, vectors, eigen, panels)


def local(eigvecs, span_vectors, span_offsets, panels):
    cols = eigvecs.shape[1]
    band = span_vectors.shape[3]
    n_row = lax.psum(1, "row")
    eigen, home = fused_step(span_offsets, span_vectors.reshape(-1, band), eigvecs, panels, n_row)
    return eigen - home[:, :cols].astype(F32)


def solution(mesh):
    finer = Mesh(mesh.devices.reshape(mesh.shape["row"], NX, NZ), ("row", "cx", "cz"))
    col = ("cx", "cz")
    placed = (P(col, "row"), P(None, "row", None, None), P(None, "row"), P(None, col, "row"))
    return jax.shard_map(local, mesh=finer, in_specs=placed, out_specs=P(col, "row"), check_vma=False)
```

```python
import functools

import jax
import jax.numpy as jnp
from jax import lax
from jax.experimental import pallas as pl
from jax.experimental.pallas import tpu as pltpu
from jax.sharding import Mesh
from jax.sharding import PartitionSpec as P

LANE = 128
BLOCK = 128
NX = 4
NZ = 8
CHUNKS = 5
F32 = jnp.float32
BF16 = jnp.bfloat16
NT = (((1,), (1,)), ((), ()))
NN = (((1,), (0,)), ((), ()))


def halves(a):
    top = a.astype(BF16)
    return top, (a - top.astype(F32)).astype(BF16)


def dot3(a, b):
    a_top, a_low = halves(a)
    b_top, b_low = halves(b)
    d = functools.partial(lax.dot_general, dimension_numbers=NN, preferred_element_type=F32)
    return d(a_top, b_top) + (d(a_top, b_low) + d(a_low, b_top))


GRAM_TILES = ((0, 0), (0, 2), (0, 3), (1, 0), (1, 1), (1, 2), (1, 3), (2, 2), (3, 2), (3, 3))


def dot3_nt(a, b):
    a_top, a_low = halves(a)
    b_top, b_low = halves(b)
    d = functools.partial(lax.dot_general, dimension_numbers=NT, preferred_element_type=F32)
    return d(a_top, b_top) + (d(a_top, b_low) + d(a_low, b_top))


def tile_inverses(tiles, between=None):
    bp = lax.broadcasted_iota(jnp.int32, (BLOCK, BLOCK), 0)
    bq = lax.broadcasted_iota(jnp.int32, (BLOCK, BLOCK), 1)
    eye = (bp == bq).astype(F32)
    inverse = [eye - jnp.where(bp // 2 == bq // 2, tile, 0.0) for tile in tiles]
    size = 2
    while size < BLOCK:
        joined = (bp // (2 * size) == bq // (2 * size)) & (bp // size != bq // size)
        left = [dot3(inv, jnp.where(joined, tile, 0.0)) for inv, tile in zip(inverse, tiles)]
        inverse = [inv - dot3(lhs, inv) for inv, lhs in zip(inverse, left)]
        if between is not None:
            between(size)
        size *= 2
    return inverse


def fused_kernel(offs_hbm, vectors_hbm, eigen_hbm, panels_hbm, kept_hbm, home, kept, offs, vectors, eigen, cut, gathered, packs,
                 inners, wide, tile_of, placed_top, placed_low, outgoing, traded, shared, rounded, acc_top, acc_low,
                 work, joined, slots, whole, change, load, send_a, recv_a, send_p, recv_p, send_w, recv_w, send_f, recv_f,
                 send_x, recv_x, send_c, recv_c, send_d, recv_d, send_rs, recv_rs, send_ag, recv_ag, send_h, recv_h,
                 own_sem):
    row, cx, cz = lax.axis_index("row"), lax.axis_index("cx"), lax.axis_index("cz")
    n_row = lax.axis_size("row")
    rows, cols = eigen.shape
    every = NX * rows
    tiles_dev = cols // LANE
    part = cut.shape[3]
    chunk = part // CHUNKS
    n_panel = cut.shape[1]
    per_dev = vectors.shape[0]
    half = per_dev // 2
    refl = 4
    spans = half // refl
    per_tile = BLOCK // half
    peers = n_row * NX
    owners = joined.shape[0]
    mesh = pl.DeviceIdType.MESH
    mxu_nt = functools.partial(lax.dot_general, dimension_numbers=NT, preferred_element_type=F32)
    mxu = functools.partial(lax.dot_general, dimension_numbers=NN, preferred_element_type=F32)

    loads = [
        pltpu.make_async_copy(offs_hbm, offs, load.at[0]),
        pltpu.make_async_copy(vectors_hbm, vectors, load.at[1]),
    ]
    eigen_load = pltpu.make_async_copy(eigen_hbm, eigen, load.at[2])
    for x in range(NX):
        size = min(part, cols - x * part)
        loads.append(
            pltpu.make_async_copy(
                panels_hbm.at[:, :, pl.ds(x * part, size)], cut.at[x, :, :, pl.ds(0, size)], load.at[3 + x]
            )
        )
        if size < part:
            cut[x, :, :, size:] = jnp.zeros((n_panel, cut.shape[2], part - size), BF16)
    for copy in loads:
        copy.start()
    eigen_load.start()
    barrier = pltpu.get_barrier_semaphore()
    for k in (1, NZ - 1):
        pl.semaphore_signal(barrier, inc=1, device_id={"cz": (cz + k) % NZ}, device_id_type=mesh)
    for k in range(1, NX):
        pl.semaphore_signal(barrier, inc=1, device_id={"cx": (cx + k) % NX}, device_id_type=mesh)
    for k in range(1, n_row):
        pl.semaphore_signal(barrier, inc=1, device_id={"row": (row + k) % n_row}, device_id_type=mesh)
    for i in range(1, n_row // 2):
        for k in range(1, NX):
            there = {"row": (row + 2 * i) % n_row, "cx": (cx + k) % NX}
            pl.semaphore_signal(barrier, inc=1, device_id=there, device_id_type=mesh)
    for copy in loads:
        copy.wait()

    lane8 = lax.broadcasted_iota(jnp.int32, (8, LANE), 1)
    line8 = lax.broadcasted_iota(jnp.int32, (8, LANE), 0)
    line64 = lax.broadcasted_iota(jnp.int32, (per_dev, LANE), 0) // refl
    meta = jnp.zeros((8, LANE), F32)
    own_tile = jnp.zeros((per_dev, LANE), F32)
    own_shift = jnp.zeros((per_dev, LANE), jnp.int32)
    for s in range(2):
        for b in range(spans):
            at = offs[s, b]
            tile_at = at >> 7
            shift_at = at & 127
            place = (row % per_tile) * half + b * refl
            mine = (lane8 >= place) & (lane8 < place + refl)
            line = s * 2 + row // per_tile
            meta = jnp.where(mine & (line8 == line), (tile_at + row * tiles_dev).astype(F32), meta)
            meta = jnp.where(mine & (line8 == line + 4), shift_at.astype(F32), meta)
            own_tile = jnp.where(line64 == s * spans + b, tile_at.astype(F32), own_tile)
            own_shift = jnp.where(line64 == s * spans + b, shift_at, own_shift)
    packs[row, :per_dev] = vectors[...]
    packs[row, per_dev:] = meta
    def sized(ref, send, recv):
        return pltpu.make_async_remote_copy(
            src_ref=ref, dst_ref=ref, send_sem=send, recv_sem=recv, device_id={"cx": (cx + 1) % NX}, device_id_type=mesh
        )

    def over_x(j, k):
        at = pl.ds(j * chunk, chunk)
        return pltpu.make_async_remote_copy(
            src_ref=cut.at[(cx + k) % NX, :, :, at],
            dst_ref=gathered.at[:, cx, cz, :, at],
            send_sem=send_a.at[0],
            recv_sem=recv_a.at[j],
            device_id={"cx": (cx + k) % NX},
            device_id_type=mesh,
        )

    def over_row(ref, sends, recvs, k):
        return pltpu.make_async_remote_copy(
            src_ref=ref.at[row],
            dst_ref=ref.at[row],
            send_sem=sends.at[0],
            recv_sem=recvs.at[0],
            device_id={"row": (row + k) % n_row},
            device_id_type=mesh,
        )

    def along_x(source_ref, target_ref, sends, recvs, k):
        target = (cx + k) % NX
        return pltpu.make_async_remote_copy(
            src_ref=source_ref.at[target] if source_ref is not target_ref else source_ref.at[cx],
            dst_ref=target_ref.at[cx],
            send_sem=sends.at[0],
            recv_sem=recvs.at[0],
            device_id={"cx": target},
            device_id_type=mesh,
        )

    last = NZ // 2 - 1

    def ring(ahead, d, j):
        step = 1 if ahead else NZ - 1
        at = pl.ds(j * chunk, chunk)
        panel = slice(None) if d < last else (pl.ds(0, 1) if ahead else pl.ds(1, 1))
        place = gathered.at[panel, :, (cz + NZ - d * step) % NZ if ahead else (cz + d) % NZ, :, at]
        return pltpu.make_async_remote_copy(
            src_ref=place,
            dst_ref=place,
            send_sem=send_f.at[0],
            recv_sem=recv_f.at[d * CHUNKS + j],
            device_id={"cz": (cz + step) % NZ},
            device_id_type=mesh,
        )

    def own_block(ahead, j, k):
        at = pl.ds(j * chunk, chunk)
        place = gathered.at[:, (cx + NX - k) % NX, cz, :, at]
        return pltpu.make_async_remote_copy(
            src_ref=cut.at[cx, :, :, at] if k == 0 else place,
            dst_ref=place,
            send_sem=send_f.at[0],
            recv_sem=recv_f.at[j],
            device_id={"cz": (cz + (1 if ahead else NZ - 1)) % NZ},
            device_id_type=mesh,
        )

    def launch(j):
        at = pl.ds(j * chunk, chunk)
        sized(gathered.at[:, pl.ds(0, NX - 1), cz, :, at], send_a.at[0], recv_a.at[j]).wait_recv()
        for k in range(1, NX):
            for ahead in (True, False):
                own_block(ahead, j, k).start()

    def reflect(at, panel):
        return gathered[panel, :, :, :, at].reshape(-1, chunk)

    def product(j):
        at = slice(j * chunk, (j + 1) * chunk)
        upper, lower = reflect(at, 0), reflect(at, 1)
        top = jnp.concatenate([rounded[:, at], upper], axis=0)
        first = mxu_nt(top, jnp.concatenate([upper, lower], axis=0))
        second = mxu_nt(lower, lower)
        acc_top[...] = first if j == 0 else acc_top[...] + first
        acc_low[...] = second if j == 0 else acc_low[...] + second

    queue = [(d, j) for d in range(last + 1) for j in range(CHUNKS)]

    def pump(count):
        for _ in range(count):
            d, j = queue.pop(0)
            at = pl.ds(j * chunk, chunk)
            both = gathered.at[:, :, pl.ds(0, 2 if d < last else 1), :, at]
            sized(both, send_f.at[0], recv_f.at[d * CHUNKS + j]).wait_recv()
            if d < last:
                for ahead in (True, False):
                    ring(ahead, d + 1, j).start()
            else:
                product(j)

    def shifted(values, amount):
        both = jnp.concatenate([values, jnp.zeros_like(values)], axis=1)
        for bit in range(7):
            both = jnp.where(((amount >> bit) & 1) == 1, pltpu.roll(both, 1 << bit, 1), both)
        return both

    own_copy = pltpu.make_async_copy(cut.at[cx], gathered.at[:, cx, cz], own_sem.at[0])
    own_copy.start()

    pl.semaphore_wait(barrier, 2 + NX - 1 + n_row - 1 + (n_row // 2 - 1) * (NX - 1))
    for j in range(3):
        for k in (1, 3, 2):
            over_x(j, k).start()
        if j == 0:
            for i in range(CHUNKS):
                for ahead in (True, False):
                    own_block(ahead, i, 0).start()
    for k in range(1, n_row):
        over_row(packs, send_p, recv_p, k).start()
    own_wide = shifted(vectors[...], jnp.concatenate([own_shift, own_shift], axis=1))
    low_top, low_low = [v.astype(F32) for v in halves(own_wide[:, :LANE])]
    high_top, high_low = [v.astype(F32) for v in halves(own_wide[:, LANE:])]
    group = 7

    def build(step, carry):
        for k in range(group):
            tile = (step * group + k).astype(F32)
            first, second = own_tile == tile, own_tile == tile - 1.0
            at = pl.ds(pl.multiple_of((step * group + k) * LANE, LANE), LANE)
            placed_top[:, at] = jnp.where(first, low_top, jnp.where(second, high_top, 0.0)).astype(BF16)
            placed_low[:, at] = jnp.where(first, low_low, jnp.where(second, high_low, 0.0)).astype(BF16)
        return carry

    lax.fori_loop(0, tiles_dev // group, build, 0)
    placed_top[:, cols:] = jnp.zeros((per_dev, NX * part - cols), BF16)
    placed_low[:, cols:] = jnp.zeros((per_dev, NX * part - cols), BF16)
    eigen_load.wait()
    for x in range(NX):
        size = min(part, cols - x * part)
        outgoing[x, :, :size] = eigen[:, x * part : x * part + size].astype(BF16)
        if size < part:
            outgoing[x, :, size:] = jnp.zeros((rows, part - size), BF16)

    own_trade = pltpu.make_async_copy(outgoing.at[cx], traded.at[cx], own_sem.at[1])
    own_trade.start()
    def inner_step(step, total):
        at = pl.ds(pl.multiple_of(step * group * LANE, LANE), group * LANE)
        top, low = halves(eigen[:, at])
        first = mxu_nt(jnp.concatenate([top, low], axis=0), placed_top[:, at])
        return total + first[:rows] + first[rows:] + mxu_nt(top, placed_low[:, at])

    steps = tiles_dev // group
    for j in range(2):
        launch(j)
        for k in (1, 3, 2):
            over_x(j + 3, k).start()
    for k in (1, 3, 2):
        along_x(outgoing, traded, send_x, recv_x, k).start()
    total = lax.fori_loop(0, steps // 2, inner_step, jnp.zeros((rows, per_dev), F32))
    launch(2)
    launch(3)
    total = lax.fori_loop(steps // 2, steps, inner_step, total)
    launch(4)
    pump(1)

    sized(packs.at[pl.ds(0, n_row - 1)], send_p.at[0], recv_p.at[0]).wait_recv()
    every_meta = packs[0, per_dev:]
    for r in range(1, n_row):
        every_meta = every_meta + packs[r, per_dev:]
    bp = lax.broadcasted_iota(jnp.int32, (BLOCK, BLOCK), 0)
    bq = lax.broadcasted_iota(jnp.int32, (BLOCK, BLOCK), 1)
    diag = bp == bq

    def turned(line):
        return jnp.sum(jnp.where(diag, line, 0.0), axis=1, keepdims=True)

    count = 2 * n_row * half // BLOCK
    across_tile = [every_meta[u : u + 1] for u in range(count)]
    down_tile = []
    for u in range(count):
        s, h = u // 2, u % 2
        low = jnp.concatenate(
            [packs[h * per_tile + k, s * half : (s + 1) * half] for k in range(per_tile)], axis=0
        )
        wide[u * BLOCK : (u + 1) * BLOCK] = shifted(low, turned(every_meta[u + 4 : u + 5]).astype(jnp.int32))
        down = turned(across_tile[u])
        down_tile.append(down)
        tile_of[u * BLOCK : (u + 1) * BLOCK] = jnp.broadcast_to(down, (BLOCK, LANE))

    def of_row(ref, r):
        return jnp.concatenate(
            [ref[pl.ds(pl.multiple_of(s * n_row * half + r * half, half), half)] for s in range(2)], axis=0
        )

    prev_row = jnp.maximum(row - 1, 0)
    prev_tile = of_row(tile_of, prev_row) - (row * tiles_dev).astype(F32)
    prev_high = jnp.where(prev_tile == -1.0, of_row(wide, prev_row)[:, LANE:], 0.0)
    behind = dot3_nt(eigen[:, :LANE], prev_high)
    inners[row] = jnp.concatenate([total, behind], axis=1)
    for k in range(1, n_row):
        over_row(inners, send_w, recv_w, k).start()
    pump(1)

    keep = (((bp // refl) == (bq // refl)) & (bp > bq)) | (((bp // refl) != (bq // refl)) & (bp < bq))
    strict, across = {}, []
    for u in range(count):
        mine = wide[u * BLOCK : (u + 1) * BLOCK]
        rest = wide[u * BLOCK :]
        level = dot3_nt(mine, rest)
        after = dot3_nt(mine[:, LANE:], rest[:, :LANE])
        before = dot3_nt(mine[:, :LANE], rest[:, LANE:])
        for t in range(u, count):
            cols_at = slice((t - u) * BLOCK, (t - u + 1) * BLOCK)
            gap = across_tile[t] - down_tile[u]
            tile = jnp.where(
                gap == 0.0,
                level[:, cols_at],
                jnp.where(gap == 1.0, after[:, cols_at], jnp.where(gap == -1.0, before[:, cols_at], 0.0)),
            )
            if t == u:
                picked = jnp.where(diag, tile, 0.0)
                scale = 2.0 / jnp.sum(picked, axis=1, keepdims=True)
                across.append(2.0 / jnp.sum(picked, axis=0, keepdims=True))
                tile = jnp.where(keep, tile, 0.0)
            strict[u, t] = tile * scale
        if u == 1:
            pump(1)
    inverse = tile_inverses([strict[t, t] for t in range(count)], lambda size: pump(1) if size == 8 else None)
    pump(1)

    sized(inners.at[pl.ds(0, n_row - 1)], send_w.at[0], recv_w.at[0]).wait_recv()
    lane = lax.broadcasted_iota(jnp.int32, (rows, LANE), 1) // half
    right = [jnp.zeros((rows, LANE), F32) for _ in range(count)]
    for r in range(n_row):
        values = inners[r]
        for s in range(2):
            u = s * 2 + r // per_tile
            moved = pltpu.roll(values, (half * (r % per_tile) - half * s) % LANE, 1)
            right[u] = right[u] + jnp.where(lane == r % per_tile, moved, 0.0)
            if r > 0:
                u = s * 2 + (r - 1) // per_tile
                moved = pltpu.roll(values, (half * ((r - 1) % per_tile) - per_dev - half * s) % LANE, 1)
                right[u] = right[u] + jnp.where(lane == (r - 1) % per_tile, moved, 0.0)
    found = []
    for t in range(count):
        value = right[t]
        for u in range(t):
            value = value - dot3(found[u], strict[u, t])
        found.append(dot3(value, inverse[t]))
    solved = [found[t] * across[t] for t in range(count)]

    def coeffs_of(r):
        result = jnp.zeros((rows, LANE), F32)
        for s in range(2):
            tile = jnp.where(r // per_tile == 0, solved[s * 2], solved[s * 2 + 1])
            moved = pltpu.roll(tile, (LANE - half * (r % per_tile) + half * s) % LANE, 1)
            result = jnp.where(lane == s, moved, result)
        return result[:, :per_dev]

    own_coeffs, prev_coeffs = coeffs_of(row), coeffs_of(prev_row)
    shared[cx] = jnp.concatenate([own_coeffs, prev_coeffs], axis=1)
    for k in (1, 3, 2):
        along_x(shared, shared, send_c, recv_c, k).start()
    pump(1)

    def both_halves(values):
        top, low = halves(values)
        return top, jnp.concatenate([top, low], axis=0)

    def changed(top, both, at):
        size = top.shape[0]
        first = mxu(both, placed_top[:, at])
        return first[:size] + first[size:] + mxu(top, placed_low[:, at])

    coeffs_top, coeffs_both = both_halves(own_coeffs)
    first_change = dot3(prev_coeffs, prev_high)

    def keep_step(step, carry):
        at = pl.ds(pl.multiple_of(step * group * LANE, LANE), group * LANE)
        kept[:, at] = eigen[:, at] - changed(coeffs_top, coeffs_both, at)
        return carry

    lax.fori_loop(0, steps // 4, keep_step, 0)
    pump(1)
    kept[:, :LANE] = kept[:, :LANE] - first_change

    pump(1)
    lax.fori_loop(steps // 4, steps // 2, keep_step, 0)
    pump(1)
    lax.fori_loop(steps // 2, 3 * steps // 4, keep_step, 0)
    pump(1)
    lax.fori_loop(3 * steps // 4, steps, keep_step, 0)
    kept_copy = pltpu.make_async_copy(kept, kept_hbm, load.at[2])
    kept_copy.start()
    own_copy.wait()
    own_trade.wait()
    sized(traded.at[pl.ds(0, NX - 1)], send_x.at[0], recv_x.at[0]).wait_recv()
    sized(shared.at[pl.ds(0, NX - 1)], send_c.at[0], recv_c.at[0]).wait_recv()
    all_shared = shared[...].reshape(every, LANE)
    slice_top, slice_both = both_halves(all_shared[:, :per_dev])
    begin_change = jnp.where(cx == 0, 1.0, 0.0).astype(F32) * dot3(all_shared[:, per_dev:], prev_high)
    for j in range(CHUNKS):
        at = slice(j * chunk, (j + 1) * chunk)
        source = pl.ds(pl.multiple_of(cx * part + j * chunk, LANE), chunk)
        value = traded[:, :, at].reshape(every, chunk).astype(F32) - changed(slice_top, slice_both, source)
        if j == 0:
            value = jnp.concatenate([value[:, :LANE] - begin_change, value[:, LANE:]], axis=1)
        rounded[:, at] = value.astype(BF16)
    pump(len(queue))

    piece = BLOCK // 2

    def put(place, value):
        rounded = value.astype(BF16)
        work[2 * place] = rounded[:piece]
        work[2 * place + 1] = rounded[piece:]

    for place, (u, t) in enumerate(GRAM_TILES):
        if u < 2:
            put(place, acc_top[(1 + u) * BLOCK : (2 + u) * BLOCK, t * BLOCK : (t + 1) * BLOCK])
        else:
            put(place, acc_low[(u - 2) * BLOCK : (u - 1) * BLOCK, (t - 2) * BLOCK : (t - 1) * BLOCK])
    for t in range(4):
        put(len(GRAM_TILES) + t, acc_top[:BLOCK, t * BLOCK : (t + 1) * BLOCK])

    core, chip = row % 2, (row // 2) * NX + cx
    chips = peers // 2
    ys = n_row // 2
    far_first = sorted(
        ((i, k) for i in range(ys) for k in range(NX) if i or k),
        key=lambda pair: -min(pair[0], ys - pair[0]) - min(pair[1], NX - pair[1]),
    )

    def chip_at(k):
        i, shift = far_first[k - 1]
        return ((row // 2 + i) % ys) * NX + (cx + shift) % NX

    def across(source, target, send, recv):
        return pltpu.make_async_remote_copy(
            src_ref=source,
            dst_ref=target,
            send_sem=send,
            recv_sem=recv,
            device_id={"row": row + 1 - 2 * core},
            device_id_type=mesh,
        )

    def on_chip(place):
        return {"row": (place // NX) * 2 + core, "cx": place % NX}

    def scatter(k):
        target = chip_at(k)
        return pltpu.make_async_remote_copy(
            src_ref=joined.at[lax.rem(target, owners)],
            dst_ref=slots.at[k - 1],
            send_sem=send_rs.at[0],
            recv_sem=recv_rs.at[0],
            device_id=on_chip(target),
            device_id_type=mesh,
        )

    mine = core * owners + lax.rem(chip, owners)

    def gather(k):
        return pltpu.make_async_remote_copy(
            src_ref=whole.at[mine],
            dst_ref=whole.at[mine],
            send_sem=send_ag.at[0],
            recv_sem=recv_ag.at[0],
            device_id=on_chip(chip_at(k)),
            device_id_type=mesh,
        )

    first_swap = across(work.at[pl.ds((1 - core) * owners, owners)], joined, send_d.at[0], recv_d.at[0])
    first_swap.start()
    first_swap.wait_recv()
    for place in range(owners):
        joined[place] = (joined[place].astype(F32) + work[core * owners + place].astype(F32)).astype(BF16)
    for k in range(1, chips):
        pl.when(chip_at(k) < owners)(scatter(k).start)

    @pl.when(chip < owners)
    def _():
        sized(slots, send_rs.at[0], recv_rs.at[0]).wait_recv()
        value = joined[lax.rem(chip, owners)].astype(F32)
        for k in range(1, chips):
            value = value + slots[k - 1].astype(F32)
        whole[mine] = value.astype(BF16)
        for k in range(1, chips):
            gather(k).start()

    pl.when(chip < owners)(sized(whole.at[pl.ds(0, owners - 1)], send_ag.at[0], recv_ag.at[0]).wait_recv)
    pl.when(chip >= owners)(sized(whole.at[pl.ds(0, owners)], send_ag.at[0], recv_ag.at[0]).wait_recv)
    half_whole = whole.at[pl.ds(core * owners, owners)]
    second_swap = across(half_whole, half_whole, send_d.at[1], recv_d.at[1])
    second_swap.start()
    second_swap.wait_recv()

    def got(place):
        return jnp.concatenate([whole[2 * place].astype(F32), whole[2 * place + 1].astype(F32)], axis=0)

    gram = {key: got(place) for place, key in enumerate(GRAM_TILES)}
    picked = [jnp.where(diag, gram[t, t], 0.0) for t in range(4)]
    down = [2.0 / jnp.sum(p, axis=1, keepdims=True) for p in picked]
    beside = [2.0 / jnp.sum(p, axis=0, keepdims=True) for p in picked]
    panel_strict = {(u, t): gram[u, t] * down[u] for u, t in GRAM_TILES}
    for t in range(4):
        panel_strict[t, t] = jnp.where(bp > bq, panel_strict[t, t], 0.0)
    panel_inverse = tile_inverses([panel_strict[t, t] for t in range(4)])
    answer = {}
    for t in (1, 0, 3, 2):
        value = got(len(GRAM_TILES) + t)
        for u in tuple(answer):
            value = value - dot3(answer[u], panel_strict[u, t])
        answer[t] = dot3(value, panel_inverse[t])
    coeffs = jnp.concatenate([(answer[t] * beside[t]).astype(BF16) for t in range(4)], axis=1)

    def back(j, k):
        target = (cx + k) % NX
        return pltpu.make_async_remote_copy(
            src_ref=change.at[target, :, pl.ds(j * chunk, chunk)],
            dst_ref=home.at[:, pl.ds(pl.multiple_of(cx * part + j * chunk, LANE), chunk)],
            send_sem=send_h.at[0],
            recv_sem=recv_h.at[0],
            device_id={"cx": target},
            device_id_type=mesh,
        )

    for j in range(CHUNKS):
        at = slice(j * chunk, (j + 1) * chunk)
        value = mxu(coeffs, jnp.concatenate([reflect(at, 0), reflect(at, 1)], axis=0)).astype(BF16)
        for x in range(NX):
            change[x, :, at] = value[x * rows : (x + 1) * rows]
        for k in (1, 3, 2):
            back(j, k).start()
    keep_home = pltpu.make_async_copy(
        change.at[cx], home.at[:, pl.ds(pl.multiple_of(cx * part, LANE), part)], own_sem.at[0]
    )
    keep_home.start()

    sized(packs.at[pl.ds(0, n_row - 1)], send_p.at[0], recv_p.at[0]).wait_send()
    sized(inners.at[pl.ds(0, n_row - 1)], send_w.at[0], recv_w.at[0]).wait_send()
    sized(outgoing.at[pl.ds(0, NX - 1)], send_x.at[0], recv_x.at[0]).wait_send()
    sized(shared.at[pl.ds(0, NX - 1)], send_c.at[0], recv_c.at[0]).wait_send()
    sized(cut.at[pl.ds(0, NX - 1)], send_a.at[0], recv_a.at[0]).wait_send()
    sized(gathered.at[:, :, pl.ds(0, NZ - 1)], send_f.at[0], recv_f.at[0]).wait_send()
    first_swap.wait_send()
    second_swap.wait_send()
    pl.when(chip < owners)(sized(joined.at[pl.ds(0, owners - 1)], send_rs.at[0], recv_rs.at[0]).wait_send)
    pl.when(chip >= owners)(sized(joined, send_rs.at[0], recv_rs.at[0]).wait_send)
    pl.when(chip < owners)(sized(slots, send_ag.at[0], recv_ag.at[0]).wait_send)
    kept_copy.wait()
    keep_home.wait()
    sized(change.at[pl.ds(0, NX - 1)], send_h.at[0], recv_h.at[0]).wait_send()
    sized(home.at[:, pl.ds(0, (NX - 1) * part)], send_h.at[0], recv_h.at[0]).wait_recv()


def fused_step(offs, vectors, eigen, panels, n_row):
    rows, cols = eigen.shape
    n_panel, refl_dev, _ = panels.shape
    part = -(-(cols // LANE) // NX) * LANE
    per_dev, band = vectors.shape
    owners, piece = 2 * (len(GRAM_TILES) + 4), BLOCK // 2
    every = NX * rows
    dma = pltpu.SemaphoreType.DMA
    hbm = pl.BlockSpec(memory_space=pltpu.HBM)
    units = (NZ // 2) * CHUNKS
    trade = (NX, rows, part)
    return pl.pallas_call(
        fused_kernel,
        out_shape=[jax.ShapeDtypeStruct((rows, cols), F32), jax.ShapeDtypeStruct((rows, NX * part), BF16)],
        in_specs=[hbm] * 4,
        out_specs=[hbm] * 2,
        scratch_shapes=[
            pltpu.VMEM((rows, cols), F32),
            pltpu.SMEM(offs.shape, jnp.int32),
            pltpu.VMEM((per_dev, band), F32),
            pltpu.VMEM((rows, cols), F32),
            pltpu.VMEM((NX, n_panel, refl_dev, part), BF16),
            pltpu.VMEM((n_panel, NX, NZ, refl_dev, part), BF16),
            pltpu.VMEM((n_row, per_dev + 8, band), F32),
            pltpu.VMEM((n_row, rows, LANE), F32),
            pltpu.VMEM((n_row * per_dev, 2 * LANE), F32),
            pltpu.VMEM((n_row * per_dev, LANE), F32),
            pltpu.VMEM((per_dev, NX * part), BF16),
            pltpu.VMEM((per_dev, NX * part), BF16),
            pltpu.VMEM(trade, BF16),
            pltpu.VMEM(trade, BF16),
            pltpu.VMEM((NX, rows, LANE), F32),
            pltpu.VMEM((every, part), BF16),
            pltpu.VMEM((every + 2 * BLOCK, 4 * BLOCK), F32),
            pltpu.VMEM((2 * BLOCK, 2 * BLOCK), F32),
            pltpu.VMEM((owners, piece, BLOCK), BF16),
            pltpu.VMEM((owners // 2, piece, BLOCK), BF16),
            pltpu.VMEM((n_row * NX // 2 - 1, piece, BLOCK), BF16),
            pltpu.VMEM((owners, piece, BLOCK), BF16),
            pltpu.VMEM(trade, BF16),
            dma((3 + NX,)),
            dma((1,)),
            dma((CHUNKS,)),
            dma((1,)),
            dma((1,)),
            dma((1,)),
            dma((1,)),
            dma((1,)),
            dma((units,)),
            dma((1,)),
            dma((1,)),
            dma((1,)),
            dma((1,)),
            dma((2,)),
            dma((2,)),
            dma((1,)),
            dma((1,)),
            dma((1,)),
            dma((1,)),
            dma((1,)),
            dma((1,)),
            dma((2,)),
        ],
        compiler_params=pltpu.CompilerParams(
            collective_id=0, has_side_effects=True, vmem_limit_bytes=60 * 1024 * 1024
        ),
        cost_estimate=pl.CostEstimate(flops=20_000_000_000, bytes_accessed=8_000_000, transcendentals=0),
    )(offs, vectors, eigen, panels)


def local(eigvecs, span_vectors, span_offsets, panels):
    cols = eigvecs.shape[1]
    band = span_vectors.shape[3]
    n_row = lax.psum(1, "row")
    eigen, home = fused_step(span_offsets, span_vectors.reshape(-1, band), eigvecs, panels, n_row)
    return eigen - home[:, :cols].astype(F32)


def solution(mesh):
    finer = Mesh(mesh.devices.reshape(mesh.shape["row"], NX, NZ), ("row", "cx", "cz"))
    col = ("cx", "cz")
    placed = (P(col, "row"), P(None, "row", None, None), P(None, "row"), P(None, col, "row"))
    return jax.shard_map(local, mesh=finer, in_specs=placed, out_specs=P(col, "row"), check_vma=False)
```

```python
import functools

import jax
import jax.numpy as jnp
from jax import lax
from jax.experimental import pallas as pl
from jax.experimental.pallas import tpu as pltpu
from jax.sharding import Mesh
from jax.sharding import PartitionSpec as P

LANE = 128
BLOCK = 128
NX = 4
NZ = 8
CHUNKS = 5
F32 = jnp.float32
BF16 = jnp.bfloat16
NT = (((1,), (1,)), ((), ()))
NN = (((1,), (0,)), ((), ()))


def halves(a):
    top = a.astype(BF16)
    return top, (a - top.astype(F32)).astype(BF16)


def dot3(a, b):
    a_top, a_low = halves(a)
    b_top, b_low = halves(b)
    d = functools.partial(lax.dot_general, dimension_numbers=NN, preferred_element_type=F32)
    return d(a_top, b_top) + (d(a_top, b_low) + d(a_low, b_top))


GRAM_TILES = ((0, 0), (0, 2), (0, 3), (1, 0), (1, 1), (1, 2), (1, 3), (2, 2), (3, 2), (3, 3))


def dot3_nt(a, b):
    a_top, a_low = halves(a)
    b_top, b_low = halves(b)
    d = functools.partial(lax.dot_general, dimension_numbers=NT, preferred_element_type=F32)
    return d(a_top, b_top) + (d(a_top, b_low) + d(a_low, b_top))


def tile_inverses(tiles, between=None):
    bp = lax.broadcasted_iota(jnp.int32, (BLOCK, BLOCK), 0)
    bq = lax.broadcasted_iota(jnp.int32, (BLOCK, BLOCK), 1)
    eye = (bp == bq).astype(F32)
    inverse = [eye - jnp.where(bp // 2 == bq // 2, tile, 0.0) for tile in tiles]
    size = 2
    while size < BLOCK:
        joined = (bp // (2 * size) == bq // (2 * size)) & (bp // size != bq // size)
        left = [dot3(inv, jnp.where(joined, tile, 0.0)) for inv, tile in zip(inverse, tiles)]
        inverse = [inv - dot3(lhs, inv) for inv, lhs in zip(inverse, left)]
        if between is not None:
            between(size)
        size *= 2
    return inverse


def fused_kernel(offs_hbm, vectors_hbm, eigen_hbm, panels_hbm, kept_hbm, home, kept, offs, vectors, eigen, cut, gathered, packs,
                 inners, wide, tile_of, placed_top, placed_low, outgoing, traded, shared, rounded, acc_top, acc_low,
                 work, joined, slots, whole, change, load, send_a, recv_a, send_p, recv_p, send_w, recv_w, send_f, recv_f,
                 send_x, recv_x, send_c, recv_c, send_d, recv_d, send_rs, recv_rs, send_ag, recv_ag, send_h, recv_h,
                 own_sem):
    row, cx, cz = lax.axis_index("row"), lax.axis_index("cx"), lax.axis_index("cz")
    n_row = lax.axis_size("row")
    rows, cols = eigen.shape
    every = NX * rows
    tiles_dev = cols // LANE
    part = cut.shape[3]
    chunk = part // CHUNKS
    n_panel = cut.shape[1]
    per_dev = vectors.shape[0]
    half = per_dev // 2
    refl = 4
    spans = half // refl
    per_tile = BLOCK // half
    peers = n_row * NX
    owners = joined.shape[0]
    mesh = pl.DeviceIdType.MESH
    mxu_nt = functools.partial(lax.dot_general, dimension_numbers=NT, preferred_element_type=F32)
    mxu = functools.partial(lax.dot_general, dimension_numbers=NN, preferred_element_type=F32)

    loads = [
        pltpu.make_async_copy(offs_hbm, offs, load.at[0]),
        pltpu.make_async_copy(vectors_hbm, vectors, load.at[1]),
    ]
    eigen_load = pltpu.make_async_copy(eigen_hbm, eigen, load.at[2])
    for x in range(NX):
        size = min(part, cols - x * part)
        loads.append(
            pltpu.make_async_copy(
                panels_hbm.at[:, :, pl.ds(x * part, size)], cut.at[x, :, :, pl.ds(0, size)], load.at[3 + x]
            )
        )
        if size < part:
            cut[x, :, :, size:] = jnp.zeros((n_panel, cut.shape[2], part - size), BF16)
    for copy in loads:
        copy.start()
    eigen_load.start()
    barrier = pltpu.get_barrier_semaphore()
    for k in (1, NZ - 1):
        pl.semaphore_signal(barrier, inc=1, device_id={"cz": (cz + k) % NZ}, device_id_type=mesh)
    for k in range(1, NX):
        pl.semaphore_signal(barrier, inc=1, device_id={"cx": (cx + k) % NX}, device_id_type=mesh)
    for k in range(1, n_row):
        pl.semaphore_signal(barrier, inc=1, device_id={"row": (row + k) % n_row}, device_id_type=mesh)
    for i in range(1, n_row // 2):
        for k in range(1, NX):
            there = {"row": (row + 2 * i) % n_row, "cx": (cx + k) % NX}
            pl.semaphore_signal(barrier, inc=1, device_id=there, device_id_type=mesh)
    for copy in loads:
        copy.wait()

    lane8 = lax.broadcasted_iota(jnp.int32, (8, LANE), 1)
    line8 = lax.broadcasted_iota(jnp.int32, (8, LANE), 0)
    line64 = lax.broadcasted_iota(jnp.int32, (per_dev, LANE), 0) // refl
    meta = jnp.zeros((8, LANE), F32)
    own_tile = jnp.zeros((per_dev, LANE), F32)
    own_shift = jnp.zeros((per_dev, LANE), jnp.int32)
    for s in range(2):
        for b in range(spans):
            at = offs[s, b]
            tile_at = at >> 7
            shift_at = at & 127
            place = (row % per_tile) * half + b * refl
            mine = (lane8 >= place) & (lane8 < place + refl)
            line = s * 2 + row // per_tile
            meta = jnp.where(mine & (line8 == line), (tile_at + row * tiles_dev).astype(F32), meta)
            meta = jnp.where(mine & (line8 == line + 4), shift_at.astype(F32), meta)
            own_tile = jnp.where(line64 == s * spans + b, tile_at.astype(F32), own_tile)
            own_shift = jnp.where(line64 == s * spans + b, shift_at, own_shift)
    packs[row, :per_dev] = vectors[...]
    packs[row, per_dev:] = meta
    def sized(ref, send, recv):
        return pltpu.make_async_remote_copy(
            src_ref=ref, dst_ref=ref, send_sem=send, recv_sem=recv, device_id={"cx": (cx + 1) % NX}, device_id_type=mesh
        )

    def over_x(j, k):
        at = pl.ds(j * chunk, chunk)
        return pltpu.make_async_remote_copy(
            src_ref=cut.at[(cx + k) % NX, :, :, at],
            dst_ref=gathered.at[:, cx, cz, :, at],
            send_sem=send_a.at[0],
            recv_sem=recv_a.at[j],
            device_id={"cx": (cx + k) % NX},
            device_id_type=mesh,
        )

    def over_row(ref, sends, recvs, k):
        return pltpu.make_async_remote_copy(
            src_ref=ref.at[row],
            dst_ref=ref.at[row],
            send_sem=sends.at[0],
            recv_sem=recvs.at[0],
            device_id={"row": (row + k) % n_row},
            device_id_type=mesh,
        )

    def along_x(source_ref, target_ref, sends, recvs, k):
        target = (cx + k) % NX
        return pltpu.make_async_remote_copy(
            src_ref=source_ref.at[target] if source_ref is not target_ref else source_ref.at[cx],
            dst_ref=target_ref.at[cx],
            send_sem=sends.at[0],
            recv_sem=recvs.at[0],
            device_id={"cx": target},
            device_id_type=mesh,
        )

    last = NZ // 2 - 1

    def ring(ahead, d, j):
        step = 1 if ahead else NZ - 1
        at = pl.ds(j * chunk, chunk)
        panel = slice(None) if d < last else (pl.ds(0, 1) if ahead else pl.ds(1, 1))
        place = gathered.at[panel, :, (cz + NZ - d * step) % NZ if ahead else (cz + d) % NZ, :, at]
        return pltpu.make_async_remote_copy(
            src_ref=place,
            dst_ref=place,
            send_sem=send_f.at[0],
            recv_sem=recv_f.at[d * CHUNKS + j],
            device_id={"cz": (cz + step) % NZ},
            device_id_type=mesh,
        )

    def own_block(ahead, j, k):
        at = pl.ds(j * chunk, chunk)
        place = gathered.at[:, (cx + NX - k) % NX, cz, :, at]
        return pltpu.make_async_remote_copy(
            src_ref=cut.at[cx, :, :, at] if k == 0 else place,
            dst_ref=place,
            send_sem=send_f.at[0],
            recv_sem=recv_f.at[j],
            device_id={"cz": (cz + (1 if ahead else NZ - 1)) % NZ},
            device_id_type=mesh,
        )

    def launch(j):
        at = pl.ds(j * chunk, chunk)
        sized(gathered.at[:, pl.ds(0, NX - 1), cz, :, at], send_a.at[0], recv_a.at[j]).wait_recv()
        for k in range(1, NX):
            for ahead in (True, False):
                own_block(ahead, j, k).start()

    def reflect(at, panel):
        return gathered[panel, :, :, :, at].reshape(-1, chunk)

    def product(j):
        at = slice(j * chunk, (j + 1) * chunk)
        upper, lower = reflect(at, 0), reflect(at, 1)
        top = jnp.concatenate([rounded[:, at], upper], axis=0)
        first = mxu_nt(top, jnp.concatenate([upper, lower], axis=0))
        second = mxu_nt(lower, lower)
        acc_top[...] = first if j == 0 else acc_top[...] + first
        acc_low[...] = second if j == 0 else acc_low[...] + second

    queue = [(d, j) for d in range(last + 1) for j in range(CHUNKS)]

    def pump(count):
        for _ in range(count):
            d, j = queue.pop(0)
            at = pl.ds(j * chunk, chunk)
            both = gathered.at[:, :, pl.ds(0, 2 if d < last else 1), :, at]
            sized(both, send_f.at[0], recv_f.at[d * CHUNKS + j]).wait_recv()
            if d < last:
                for ahead in (True, False):
                    ring(ahead, d + 1, j).start()
            else:
                product(j)

    def shifted(values, amount):
        both = jnp.concatenate([values, jnp.zeros_like(values)], axis=1)
        for bit in range(7):
            both = jnp.where(((amount >> bit) & 1) == 1, pltpu.roll(both, 1 << bit, 1), both)
        return both

    own_copy = pltpu.make_async_copy(cut.at[cx], gathered.at[:, cx, cz], own_sem.at[0])
    own_copy.start()

    pl.semaphore_wait(barrier, 2 + NX - 1 + n_row - 1 + (n_row // 2 - 1) * (NX - 1))
    for j in range(3):
        for k in (1, 3, 2):
            over_x(j, k).start()
        if j == 0:
            for i in range(CHUNKS):
                for ahead in (True, False):
                    own_block(ahead, i, 0).start()
    for k in range(1, n_row):
        over_row(packs, send_p, recv_p, k).start()
    own_wide = shifted(vectors[...], jnp.concatenate([own_shift, own_shift], axis=1))
    low_top, low_low = [v.astype(F32) for v in halves(own_wide[:, :LANE])]
    high_top, high_low = [v.astype(F32) for v in halves(own_wide[:, LANE:])]
    group = 7

    def build(step, carry):
        for k in range(group):
            tile = (step * group + k).astype(F32)
            first, second = own_tile == tile, own_tile == tile - 1.0
            at = pl.ds(pl.multiple_of((step * group + k) * LANE, LANE), LANE)
            placed_top[:, at] = jnp.where(first, low_top, jnp.where(second, high_top, 0.0)).astype(BF16)
            placed_low[:, at] = jnp.where(first, low_low, jnp.where(second, high_low, 0.0)).astype(BF16)
        return carry

    lax.fori_loop(0, tiles_dev // group, build, 0)
    placed_top[:, cols:] = jnp.zeros((per_dev, NX * part - cols), BF16)
    placed_low[:, cols:] = jnp.zeros((per_dev, NX * part - cols), BF16)
    eigen_load.wait()
    for x in range(NX):
        size = min(part, cols - x * part)
        outgoing[x, :, :size] = eigen[:, x * part : x * part + size].astype(BF16)
        if size < part:
            outgoing[x, :, size:] = jnp.zeros((rows, part - size), BF16)

    own_trade = pltpu.make_async_copy(outgoing.at[cx], traded.at[cx], own_sem.at[1])
    own_trade.start()
    def inner_step(step, total):
        at = pl.ds(pl.multiple_of(step * group * LANE, LANE), group * LANE)
        top, low = halves(eigen[:, at])
        first = mxu_nt(jnp.concatenate([top, low], axis=0), placed_top[:, at])
        return total + first[:rows] + first[rows:] + mxu_nt(top, placed_low[:, at])

    steps = tiles_dev // group
    for j in range(2):
        launch(j)
        for k in (1, 3, 2):
            over_x(j + 3, k).start()
    for k in (1, 3, 2):
        along_x(outgoing, traded, send_x, recv_x, k).start()
    for j in range(2, CHUNKS):
        launch(j)
    total = lax.fori_loop(0, steps // 2, inner_step, jnp.zeros((rows, per_dev), F32))
    pump(1)
    total = lax.fori_loop(steps // 2, steps, inner_step, total)
    pump(1)

    sized(packs.at[pl.ds(0, n_row - 1)], send_p.at[0], recv_p.at[0]).wait_recv()
    every_meta = packs[0, per_dev:]
    for r in range(1, n_row):
        every_meta = every_meta + packs[r, per_dev:]
    bp = lax.broadcasted_iota(jnp.int32, (BLOCK, BLOCK), 0)
    bq = lax.broadcasted_iota(jnp.int32, (BLOCK, BLOCK), 1)
    diag = bp == bq

    def turned(line):
        return jnp.sum(jnp.where(diag, line, 0.0), axis=1, keepdims=True)

    count = 2 * n_row * half // BLOCK
    across_tile = [every_meta[u : u + 1] for u in range(count)]
    down_tile = []
    for u in range(count):
        s, h = u // 2, u % 2
        low = jnp.concatenate(
            [packs[h * per_tile + k, s * half : (s + 1) * half] for k in range(per_tile)], axis=0
        )
        wide[u * BLOCK : (u + 1) * BLOCK] = shifted(low, turned(every_meta[u + 4 : u + 5]).astype(jnp.int32))
        down = turned(across_tile[u])
        down_tile.append(down)
        tile_of[u * BLOCK : (u + 1) * BLOCK] = jnp.broadcast_to(down, (BLOCK, LANE))

    def of_row(ref, r):
        return jnp.concatenate(
            [ref[pl.ds(pl.multiple_of(s * n_row * half + r * half, half), half)] for s in range(2)], axis=0
        )

    prev_row = jnp.maximum(row - 1, 0)
    prev_tile = of_row(tile_of, prev_row) - (row * tiles_dev).astype(F32)
    prev_high = jnp.where(prev_tile == -1.0, of_row(wide, prev_row)[:, LANE:], 0.0)
    behind = dot3_nt(eigen[:, :LANE], prev_high)
    inners[row] = jnp.concatenate([total, behind], axis=1)
    for k in range(1, n_row):
        over_row(inners, send_w, recv_w, k).start()
    pump(1)

    keep = (((bp // refl) == (bq // refl)) & (bp > bq)) | (((bp // refl) != (bq // refl)) & (bp < bq))
    strict, across = {}, []
    for u in range(count):
        mine = wide[u * BLOCK : (u + 1) * BLOCK]
        rest = wide[u * BLOCK :]
        level = dot3_nt(mine, rest)
        after = dot3_nt(mine[:, LANE:], rest[:, :LANE])
        before = dot3_nt(mine[:, :LANE], rest[:, LANE:])
        for t in range(u, count):
            cols_at = slice((t - u) * BLOCK, (t - u + 1) * BLOCK)
            gap = across_tile[t] - down_tile[u]
            tile = jnp.where(
                gap == 0.0,
                level[:, cols_at],
                jnp.where(gap == 1.0, after[:, cols_at], jnp.where(gap == -1.0, before[:, cols_at], 0.0)),
            )
            if t == u:
                picked = jnp.where(diag, tile, 0.0)
                scale = 2.0 / jnp.sum(picked, axis=1, keepdims=True)
                across.append(2.0 / jnp.sum(picked, axis=0, keepdims=True))
                tile = jnp.where(keep, tile, 0.0)
            strict[u, t] = tile * scale
        if u == 1:
            pump(1)
    inverse = tile_inverses([strict[t, t] for t in range(count)], lambda size: pump(1) if size == 8 else None)
    pump(1)

    sized(inners.at[pl.ds(0, n_row - 1)], send_w.at[0], recv_w.at[0]).wait_recv()
    lane = lax.broadcasted_iota(jnp.int32, (rows, LANE), 1) // half
    right = [jnp.zeros((rows, LANE), F32) for _ in range(count)]
    for r in range(n_row):
        values = inners[r]
        for s in range(2):
            u = s * 2 + r // per_tile
            moved = pltpu.roll(values, (half * (r % per_tile) - half * s) % LANE, 1)
            right[u] = right[u] + jnp.where(lane == r % per_tile, moved, 0.0)
            if r > 0:
                u = s * 2 + (r - 1) // per_tile
                moved = pltpu.roll(values, (half * ((r - 1) % per_tile) - per_dev - half * s) % LANE, 1)
                right[u] = right[u] + jnp.where(lane == (r - 1) % per_tile, moved, 0.0)
    found = []
    for t in range(count):
        value = right[t]
        for u in range(t):
            value = value - dot3(found[u], strict[u, t])
        found.append(dot3(value, inverse[t]))
    solved = [found[t] * across[t] for t in range(count)]

    def coeffs_of(r):
        result = jnp.zeros((rows, LANE), F32)
        for s in range(2):
            tile = jnp.where(r // per_tile == 0, solved[s * 2], solved[s * 2 + 1])
            moved = pltpu.roll(tile, (LANE - half * (r % per_tile) + half * s) % LANE, 1)
            result = jnp.where(lane == s, moved, result)
        return result[:, :per_dev]

    own_coeffs, prev_coeffs = coeffs_of(row), coeffs_of(prev_row)
    shared[cx] = jnp.concatenate([own_coeffs, prev_coeffs], axis=1)
    for k in (1, 3, 2):
        along_x(shared, shared, send_c, recv_c, k).start()
    pump(1)

    def both_halves(values):
        top, low = halves(values)
        return top, jnp.concatenate([top, low], axis=0)

    def changed(top, both, at):
        size = top.shape[0]
        first = mxu(both, placed_top[:, at])
        return first[:size] + first[size:] + mxu(top, placed_low[:, at])

    coeffs_top, coeffs_both = both_halves(own_coeffs)
    first_change = dot3(prev_coeffs, prev_high)

    def keep_step(step, carry):
        at = pl.ds(pl.multiple_of(step * group * LANE, LANE), group * LANE)
        kept[:, at] = eigen[:, at] - changed(coeffs_top, coeffs_both, at)
        return carry

    lax.fori_loop(0, steps // 4, keep_step, 0)
    pump(1)
    kept[:, :LANE] = kept[:, :LANE] - first_change

    pump(1)
    lax.fori_loop(steps // 4, steps // 2, keep_step, 0)
    pump(1)
    lax.fori_loop(steps // 2, 3 * steps // 4, keep_step, 0)
    pump(1)
    lax.fori_loop(3 * steps // 4, steps, keep_step, 0)
    kept_copy = pltpu.make_async_copy(kept, kept_hbm, load.at[2])
    kept_copy.start()
    own_copy.wait()
    own_trade.wait()
    sized(traded.at[pl.ds(0, NX - 1)], send_x.at[0], recv_x.at[0]).wait_recv()
    sized(shared.at[pl.ds(0, NX - 1)], send_c.at[0], recv_c.at[0]).wait_recv()
    all_shared = shared[...].reshape(every, LANE)
    slice_top, slice_both = both_halves(all_shared[:, :per_dev])
    begin_change = jnp.where(cx == 0, 1.0, 0.0).astype(F32) * dot3(all_shared[:, per_dev:], prev_high)
    for j in range(CHUNKS):
        at = slice(j * chunk, (j + 1) * chunk)
        source = pl.ds(pl.multiple_of(cx * part + j * chunk, LANE), chunk)
        value = traded[:, :, at].reshape(every, chunk).astype(F32) - changed(slice_top, slice_both, source)
        if j == 0:
            value = jnp.concatenate([value[:, :LANE] - begin_change, value[:, LANE:]], axis=1)
        rounded[:, at] = value.astype(BF16)
    pump(len(queue))

    piece = BLOCK // 2

    def put(place, value):
        rounded = value.astype(BF16)
        work[2 * place] = rounded[:piece]
        work[2 * place + 1] = rounded[piece:]

    for place, (u, t) in enumerate(GRAM_TILES):
        if u < 2:
            put(place, acc_top[(1 + u) * BLOCK : (2 + u) * BLOCK, t * BLOCK : (t + 1) * BLOCK])
        else:
            put(place, acc_low[(u - 2) * BLOCK : (u - 1) * BLOCK, (t - 2) * BLOCK : (t - 1) * BLOCK])
    for t in range(4):
        put(len(GRAM_TILES) + t, acc_top[:BLOCK, t * BLOCK : (t + 1) * BLOCK])

    core, chip = row % 2, (row // 2) * NX + cx
    chips = peers // 2
    ys = n_row // 2
    far_first = sorted(
        ((i, k) for i in range(ys) for k in range(NX) if i or k),
        key=lambda pair: -min(pair[0], ys - pair[0]) - min(pair[1], NX - pair[1]),
    )

    def chip_at(k):
        i, shift = far_first[k - 1]
        return ((row // 2 + i) % ys) * NX + (cx + shift) % NX

    def across(source, target, send, recv):
        return pltpu.make_async_remote_copy(
            src_ref=source,
            dst_ref=target,
            send_sem=send,
            recv_sem=recv,
            device_id={"row": row + 1 - 2 * core},
            device_id_type=mesh,
        )

    def on_chip(place):
        return {"row": (place // NX) * 2 + core, "cx": place % NX}

    def scatter(k):
        target = chip_at(k)
        return pltpu.make_async_remote_copy(
            src_ref=joined.at[lax.rem(target, owners)],
            dst_ref=slots.at[k - 1],
            send_sem=send_rs.at[0],
            recv_sem=recv_rs.at[0],
            device_id=on_chip(target),
            device_id_type=mesh,
        )

    mine = core * owners + lax.rem(chip, owners)

    def gather(k):
        return pltpu.make_async_remote_copy(
            src_ref=whole.at[mine],
            dst_ref=whole.at[mine],
            send_sem=send_ag.at[0],
            recv_sem=recv_ag.at[0],
            device_id=on_chip(chip_at(k)),
            device_id_type=mesh,
        )

    first_swap = across(work.at[pl.ds((1 - core) * owners, owners)], joined, send_d.at[0], recv_d.at[0])
    first_swap.start()
    first_swap.wait_recv()
    for place in range(owners):
        joined[place] = (joined[place].astype(F32) + work[core * owners + place].astype(F32)).astype(BF16)
    for k in range(1, chips):
        pl.when(chip_at(k) < owners)(scatter(k).start)

    @pl.when(chip < owners)
    def _():
        sized(slots, send_rs.at[0], recv_rs.at[0]).wait_recv()
        value = joined[lax.rem(chip, owners)].astype(F32)
        for k in range(1, chips):
            value = value + slots[k - 1].astype(F32)
        whole[mine] = value.astype(BF16)
        for k in range(1, chips):
            gather(k).start()

    pl.when(chip < owners)(sized(whole.at[pl.ds(0, owners - 1)], send_ag.at[0], recv_ag.at[0]).wait_recv)
    pl.when(chip >= owners)(sized(whole.at[pl.ds(0, owners)], send_ag.at[0], recv_ag.at[0]).wait_recv)
    half_whole = whole.at[pl.ds(core * owners, owners)]
    second_swap = across(half_whole, half_whole, send_d.at[1], recv_d.at[1])
    second_swap.start()
    second_swap.wait_recv()

    def got(place):
        return jnp.concatenate([whole[2 * place].astype(F32), whole[2 * place + 1].astype(F32)], axis=0)

    gram = {key: got(place) for place, key in enumerate(GRAM_TILES)}
    picked = [jnp.where(diag, gram[t, t], 0.0) for t in range(4)]
    down = [2.0 / jnp.sum(p, axis=1, keepdims=True) for p in picked]
    beside = [2.0 / jnp.sum(p, axis=0, keepdims=True) for p in picked]
    panel_strict = {(u, t): gram[u, t] * down[u] for u, t in GRAM_TILES}
    for t in range(4):
        panel_strict[t, t] = jnp.where(bp > bq, panel_strict[t, t], 0.0)
    panel_inverse = tile_inverses([panel_strict[t, t] for t in range(4)])
    answer = {}
    for t in (1, 0, 3, 2):
        value = got(len(GRAM_TILES) + t)
        for u in tuple(answer):
            value = value - dot3(answer[u], panel_strict[u, t])
        answer[t] = dot3(value, panel_inverse[t])
    coeffs = jnp.concatenate([(answer[t] * beside[t]).astype(BF16) for t in range(4)], axis=1)

    def back(j, k):
        target = (cx + k) % NX
        return pltpu.make_async_remote_copy(
            src_ref=change.at[target, :, pl.ds(j * chunk, chunk)],
            dst_ref=home.at[:, pl.ds(pl.multiple_of(cx * part + j * chunk, LANE), chunk)],
            send_sem=send_h.at[0],
            recv_sem=recv_h.at[0],
            device_id={"cx": target},
            device_id_type=mesh,
        )

    for j in range(CHUNKS):
        at = slice(j * chunk, (j + 1) * chunk)
        value = mxu(coeffs, jnp.concatenate([reflect(at, 0), reflect(at, 1)], axis=0)).astype(BF16)
        for x in range(NX):
            change[x, :, at] = value[x * rows : (x + 1) * rows]
        for k in (1, 3, 2):
            back(j, k).start()
    keep_home = pltpu.make_async_copy(
        change.at[cx], home.at[:, pl.ds(pl.multiple_of(cx * part, LANE), part)], own_sem.at[0]
    )
    keep_home.start()

    sized(packs.at[pl.ds(0, n_row - 1)], send_p.at[0], recv_p.at[0]).wait_send()
    sized(inners.at[pl.ds(0, n_row - 1)], send_w.at[0], recv_w.at[0]).wait_send()
    sized(outgoing.at[pl.ds(0, NX - 1)], send_x.at[0], recv_x.at[0]).wait_send()
    sized(shared.at[pl.ds(0, NX - 1)], send_c.at[0], recv_c.at[0]).wait_send()
    sized(cut.at[pl.ds(0, NX - 1)], send_a.at[0], recv_a.at[0]).wait_send()
    sized(gathered.at[:, :, pl.ds(0, NZ - 1)], send_f.at[0], recv_f.at[0]).wait_send()
    first_swap.wait_send()
    second_swap.wait_send()
    pl.when(chip < owners)(sized(joined.at[pl.ds(0, owners - 1)], send_rs.at[0], recv_rs.at[0]).wait_send)
    pl.when(chip >= owners)(sized(joined, send_rs.at[0], recv_rs.at[0]).wait_send)
    pl.when(chip < owners)(sized(slots, send_ag.at[0], recv_ag.at[0]).wait_send)
    kept_copy.wait()
    keep_home.wait()
    sized(change.at[pl.ds(0, NX - 1)], send_h.at[0], recv_h.at[0]).wait_send()
    sized(home.at[:, pl.ds(0, (NX - 1) * part)], send_h.at[0], recv_h.at[0]).wait_recv()


def fused_step(offs, vectors, eigen, panels, n_row):
    rows, cols = eigen.shape
    n_panel, refl_dev, _ = panels.shape
    part = -(-(cols // LANE) // NX) * LANE
    per_dev, band = vectors.shape
    owners, piece = 2 * (len(GRAM_TILES) + 4), BLOCK // 2
    every = NX * rows
    dma = pltpu.SemaphoreType.DMA
    hbm = pl.BlockSpec(memory_space=pltpu.HBM)
    units = (NZ // 2) * CHUNKS
    trade = (NX, rows, part)
    return pl.pallas_call(
        fused_kernel,
        out_shape=[jax.ShapeDtypeStruct((rows, cols), F32), jax.ShapeDtypeStruct((rows, NX * part), BF16)],
        in_specs=[hbm] * 4,
        out_specs=[hbm] * 2,
        scratch_shapes=[
            pltpu.VMEM((rows, cols), F32),
            pltpu.SMEM(offs.shape, jnp.int32),
            pltpu.VMEM((per_dev, band), F32),
            pltpu.VMEM((rows, cols), F32),
            pltpu.VMEM((NX, n_panel, refl_dev, part), BF16),
            pltpu.VMEM((n_panel, NX, NZ, refl_dev, part), BF16),
            pltpu.VMEM((n_row, per_dev + 8, band), F32),
            pltpu.VMEM((n_row, rows, LANE), F32),
            pltpu.VMEM((n_row * per_dev, 2 * LANE), F32),
            pltpu.VMEM((n_row * per_dev, LANE), F32),
            pltpu.VMEM((per_dev, NX * part), BF16),
            pltpu.VMEM((per_dev, NX * part), BF16),
            pltpu.VMEM(trade, BF16),
            pltpu.VMEM(trade, BF16),
            pltpu.VMEM((NX, rows, LANE), F32),
            pltpu.VMEM((every, part), BF16),
            pltpu.VMEM((every + 2 * BLOCK, 4 * BLOCK), F32),
            pltpu.VMEM((2 * BLOCK, 2 * BLOCK), F32),
            pltpu.VMEM((owners, piece, BLOCK), BF16),
            pltpu.VMEM((owners // 2, piece, BLOCK), BF16),
            pltpu.VMEM((n_row * NX // 2 - 1, piece, BLOCK), BF16),
            pltpu.VMEM((owners, piece, BLOCK), BF16),
            pltpu.VMEM(trade, BF16),
            dma((3 + NX,)),
            dma((1,)),
            dma((CHUNKS,)),
            dma((1,)),
            dma((1,)),
            dma((1,)),
            dma((1,)),
            dma((1,)),
            dma((units,)),
            dma((1,)),
            dma((1,)),
            dma((1,)),
            dma((1,)),
            dma((2,)),
            dma((2,)),
            dma((1,)),
            dma((1,)),
            dma((1,)),
            dma((1,)),
            dma((1,)),
            dma((1,)),
            dma((2,)),
        ],
        compiler_params=pltpu.CompilerParams(
            collective_id=0, has_side_effects=True, vmem_limit_bytes=60 * 1024 * 1024
        ),
        cost_estimate=pl.CostEstimate(flops=20_000_000_000, bytes_accessed=8_000_000, transcendentals=0),
    )(offs, vectors, eigen, panels)


def local(eigvecs, span_vectors, span_offsets, panels):
    cols = eigvecs.shape[1]
    band = span_vectors.shape[3]
    n_row = lax.psum(1, "row")
    eigen, home = fused_step(span_offsets, span_vectors.reshape(-1, band), eigvecs, panels, n_row)
    return eigen - home[:, :cols].astype(F32)


def solution(mesh):
    finer = Mesh(mesh.devices.reshape(mesh.shape["row"], NX, NZ), ("row", "cx", "cz"))
    col = ("cx", "cz")
    placed = (P(col, "row"), P(None, "row", None, None), P(None, "row"), P(None, col, "row"))
    return jax.shard_map(local, mesh=finer, in_specs=placed, out_specs=P(col, "row"), check_vma=False)
```
